32 devices in a mesh: gx: 4 (over z), gy: 8 (over y, x, core).
Axes of the slice: x: 2, y: 2, z: 4, core: 2. Of those that a mesh axis runs over, the one named last changes fastest.
Arguments:
- hidden: bfloat16 [4, 16384], replicated, may hold values from -6 to 6
- norm_gain: float32 [16384], replicated, may hold values from 0.5 to 1.5
- q_codes: int32 [16384, 8192], P('gx', 'gy'), may hold values from 0 to 255, as said below
- q_absmax: float32 [256, 16384], P('gx', 'gy'), may hold values from 0.0046875 to 0.046875
- kv_codes: int32 [16384, 1024], P('gx', 'gy'), may hold values from 0 to 255
- kv_absmax: float32 [256, 2048], P('gx', 'gy'), may hold values from 0.015625 to 0.15625
- o_codes: int32 [16384, 8192], P('gx', 'gy'), may hold values from 0 to 255, as said below
- o_absmax: float32 [256, 16384], P('gx', 'gy'), may hold values from 0.0046875 to 0.046875
- q_down: bfloat16 [8, 16384, 16], P(None, 'gx'), may hold values from -0.140625 to 0.140625
- q_up: bfloat16 [8, 16, 16384], P(None, None, 'gy'), may hold values from -1.5 to 1.5
- q_magnitude: float32 [8, 16384], P(None, 'gy'), may hold values from 0.25 to 1.75
- o_down: bfloat16 [8, 16384, 16], P(None, 'gx'), may hold values from -0.140625 to 0.140625
- o_up: bfloat16 [8, 16, 16384], P(None, None, 'gy'), may hold values from -1.5 to 1.5
- o_magnitude: float32 [8, 16384], P(None, 'gy'), may hold values from 0.25 to 1.75
- tenant: int32 [4], replicated, may hold values from 0 to 7
- lengths: int32 [4], replicated, may hold values from 1 to 24576, as said below
- page_table: int32 [4, 96], replicated, may hold values from 0 to 287, as said below
- kv_cache: bfloat16 [288, 2, 256, 1024], P(('gx', 'gy')), may hold values from -1080 to 1080, as said below
Outputs:
- layer_out: bfloat16 [4, 16384], P('gx', 'gy')
The draws below stay inside these ranges and needn't reach their ends.
Inputs may be any that keep to these rules, and one draw needn't show every extreme that they name: `q_codes`: each word holds two 4-bit codes: word % 16 for the even column and word // 16 for the odd one. `kv_codes`: each word holds two 4-bit codes: word % 16 for the even column and word // 16 for the odd one. `o_codes`: each word holds two 4-bit codes: word % 16 for the even column and word // 16 for the odd one. `lengths`: one row holds exactly 24576 tokens; every other row fewer than 16384. `page_table`: for j below ceil(lengths[r] / 256), entry [r, j] is the global slot of page j of row r: device index along gx+gy times 9 plus the slot on that device; no slot holds two pages; other entries are 0 and are not read. On every device the used slots are its first ones; no device holds more than 9 pages and some device holds exactly 9. `kv_cache`: row d * 9 + s holds slot s of device d; unused slots hold finite values.
All inputs are finite; a program needn't handle non-finite values.
Results may differ from the reference program's by a relative error of at most 0.01.
The reference program's roundings to bfloat16 on the way (of `normed`, `query` and `attended`) count: a program that leaves them out, or rounds other values in their place, can miss the bound.
Values may be sent and summed in bfloat16 or wider, within the bound.
No kernel may reach another device: no remote copies, remote signals or barrier semaphores. Data moves between devices by JAX's collectives and lax.ppermute only.
A program may use at most 384 MiB of HBM per device.

```python
import math
import jax
import jax.numpy as jnp
from jax import lax

D = 16384
HEADS = 128
KV_HEADS = 8
HEAD_DIM = 128
RANK = 16
TENANTS = 8
QBLOCK = 64
PAGE = 256
MAXLEN = 24576
MEAN_LEN = 8192
ROWS = 4
QWIDTH = 16384
KVWIDTH = 2048
MAX_PAGES = 96
SLOTS = 9
ALL_SLOTS = 288
HOT = 2
N_GY = 8


def layout(key):
    root_key = jax.random.fold_in(key, 1234)
    pick_key, length_key, order_key = jax.random.split(root_key, 3)
    longest = jax.random.randint(pick_key, (), 0, ROWS)
    others = jax.random.randint(length_key, (ROWS,), 1, 2 * MEAN_LEN)
    row_lengths = jnp.where(jnp.arange(ROWS) == longest, MAXLEN, others).astype(jnp.int32)
    page_need = (row_lengths + PAGE - 1) // PAGE
    live_mask = jnp.arange(MAX_PAGES)[None, :] < page_need[:, None]
    live_rank = jnp.cumsum(live_mask.reshape(-1).astype(jnp.int32)) - 1
    device_total = ALL_SLOTS // SLOTS
    device_rank = jax.random.permutation(order_key, device_total)
    slot_ids = jnp.arange(ALL_SLOTS)
    device_of = slot_ids // SLOTS
    slot_of = slot_ids % SLOTS
    rank_of = device_rank[device_of]
    priority = jnp.where(rank_of < HOT, rank_of * SLOTS + slot_of, HOT * SLOTS + slot_of * device_total + rank_of)
    slot_order = jnp.argsort(priority, stable=True)
    chosen = slot_order[jnp.clip(live_rank, 0, ALL_SLOTS - 1)].reshape(ROWS, MAX_PAGES)
    table = jnp.where(live_mask, chosen, 0).astype(jnp.int32)
    return (row_lengths, table)


def draw_lengths(key, part):
    return layout(key)[0]


def draw_page_table(key, part):
    return layout(key)[1]


def draw_kv_cache(key, part):
    full_shape = (ALL_SLOTS, 2, PAGE, KV_HEADS * HEAD_DIM)
    normal_key = jax.random.fold_in(key, 99)
    values = jnp.clip(jax.random.normal(normal_key, full_shape, jnp.float32), -6.0, 6.0)
    is_key = jnp.arange(2)[None, :, None, None] == 0
    values = values * jnp.where(is_key, 2.5, 1.0)
    return values.astype(jnp.bfloat16)


def sign_matrix(key, sign_salt, row_count):
    return 2 * jax.random.randint(jax.random.fold_in(key, sign_salt), (TENANTS * RANK, row_count), 0, 2) - 1


def amplitude_level(key, sign_salt, row_count):
    offsets = jax.random.randint(jax.random.fold_in(key, sign_salt + 7), (2,), 0, 6)
    row_ids = jnp.arange(row_count)
    parity_low = ((row_ids + offsets[0]) % 2 == 0).astype(jnp.int32)
    third_low = ((row_ids + offsets[1]) % 3 == 0).astype(jnp.int32)
    return parity_low + third_low


def shrink_codes(codes, levels):
    return jnp.where(levels == 0, codes, jnp.where(levels == 1, 4 + codes // 2, 6 + codes // 4))


def signed_words(key, sign_salt, own_salt, row_count, word_count):
    signs = sign_matrix(key, sign_salt, row_count)
    group_of = jnp.arange(word_count) * (TENANTS * RANK) // word_count
    row_sign = jnp.take(signs, group_of, axis=0).T
    levels = amplitude_level(key, sign_salt, row_count)[:, None]
    drawn_words = jax.random.randint(jax.random.fold_in(key, own_salt), (row_count, word_count), 0, 65536)
    nibble_one = drawn_words % 16
    nibble_two = drawn_words // 16 % 16
    nibble_three = drawn_words // 256 % 16
    nibble_four = drawn_words // 4096
    low_code = jnp.where(row_sign > 0, jnp.maximum(nibble_one, nibble_two), jnp.minimum(nibble_one, nibble_two))
    high_code = jnp.where(row_sign > 0, jnp.maximum(nibble_three, nibble_four), jnp.minimum(nibble_three, nibble_four))
    low_code = shrink_codes(low_code, levels)
    high_code = shrink_codes(high_code, levels)
    return (low_code + 16 * high_code).astype(jnp.int32)


def drawn_down(key, sign_salt, own_salt, row_count):
    signs = sign_matrix(key, sign_salt, row_count).astype(jnp.float32).reshape(TENANTS, RANK, row_count)
    signs = jnp.transpose(signs, (0, 2, 1))
    noise_part = jnp.clip(jax.random.normal(jax.random.fold_in(key, own_salt), (TENANTS, row_count, RANK), jnp.float32), -6.0, 6.0)
    lean_size = jax.random.uniform(jax.random.fold_in(key, own_salt + 50), (TENANTS, 1, RANK), jnp.float32, 0.6, 1.2)
    lean_sign = (2 * jax.random.randint(jax.random.fold_in(key, own_salt + 51), (TENANTS, 1, RANK), 0, 2) - 1).astype(jnp.float32)
    position = jnp.arange(row_count, dtype=jnp.float32) / row_count
    row_factor = (10.0 ** (position - 0.5) / 1.47)[None, :, None]
    return ((noise_part + lean_size * lean_sign * signs) * row_factor * row_count ** (-0.5)).astype(jnp.bfloat16)


def draw_q_codes(key, part):
    return signed_words(key, 501, 601, D, QWIDTH // 2)


def draw_q_down(key, part):
    return drawn_down(key, 501, 602, D)


def draw_o_codes(key, part):
    return signed_words(key, 511, 611, QWIDTH, D // 2)


def draw_o_down(key, part):
    return drawn_down(key, 511, 612, QWIDTH)


def with_ends(drawn, stream_key, low, top_value):
    place = [jax.random.randint(jax.random.fold_in(stream_key, axis), (), 0, length) for axis, length in enumerate(drawn.shape)]
    main_axis = drawn.shape.index(max(drawn.shape))
    next_to = place[:main_axis] + [(place[main_axis] + 1) % drawn.shape[main_axis]] + place[main_axis + 1:]
    return drawn.at[tuple(place)].set(low).at[tuple(next_to)].set(top_value)


def steps_of(key, extent, cuts, smallest, high):
    def one(axis_at, shards_of):
        heights = jax.random.uniform(jax.random.fold_in(jax.random.fold_in(key, 6), axis_at), (shards_of,), jnp.float32, smallest / len(cuts), high / len(cuts))
        return jnp.repeat(jnp.exp(heights), extent[axis_at] // shards_of).reshape((-1,) + (1,) * (len(extent) - axis_at - 1))

    factor_of = one(*cuts[0])
    for cut in cuts[1:]:
        factor_of = factor_of * one(*cut)
    return factor_of


def bell_draw(rng, dims, scale, bound, shards=(), kind=jnp.bfloat16):
    drawn = jax.random.normal(rng, dims, jnp.float32) * scale
    if len(shards) > 0:
        drawn = steps_of(rng, dims, shards, -0.22, 0.18) * drawn
    return jnp.clip(drawn, min=-bound, max=bound).astype(kind)


def setup_inputs(seed: int = 0) -> dict:
    keys = jax.random.split(jax.random.key(seed), 19)
    return {
        "hidden": bell_draw(keys[0], (ROWS, D), 1.0, 6.0),
        "norm_gain": jnp.clip(1.0 + 0.1 * jax.random.normal(keys[1], (D,), jnp.float32), 0.5, 1.5),
        "q_codes": draw_q_codes(jax.random.fold_in(keys[18], 71), 0),
        "q_absmax": jnp.clip(jnp.exp(math.log(0.046875) - 2.3025851 * jax.random.uniform(keys[3], (D // QBLOCK, QWIDTH), jnp.float32) ** steps_of(keys[3], (D // QBLOCK, QWIDTH), ((0, 4), (1, 8)), -0.2, 0.2)), 0.0046875, 0.046875),
        "kv_codes": with_ends(jax.random.randint(keys[4], (D, KVWIDTH // 2), 0, 256), jax.random.fold_in(keys[4], 1), 0, 255).astype(jnp.int32),
        "kv_absmax": jnp.clip(jnp.exp(math.log(0.15625) - 2.3025851 * jax.random.uniform(keys[5], (D // QBLOCK, KVWIDTH), jnp.float32) ** steps_of(keys[5], (D // QBLOCK, KVWIDTH), ((0, 4), (1, 8)), -0.2, 0.2)), 0.015625, 0.15625),
        "o_codes": draw_o_codes(jax.random.fold_in(keys[18], 71), 0),
        "o_absmax": jnp.clip(jnp.exp(math.log(0.046875) - 2.3025851 * jax.random.uniform(keys[7], (QWIDTH // QBLOCK, D), jnp.float32) ** steps_of(keys[7], (QWIDTH // QBLOCK, D), ((0, 4), (1, 8)), -0.2, 0.2)), 0.0046875, 0.046875),
        "q_down": draw_q_down(jax.random.fold_in(keys[18], 71), 0),
        "q_up": bell_draw(keys[9], (TENANTS, RANK, QWIDTH), RANK ** -0.5, 1.5, ((2, 8),)),
        "q_magnitude": jnp.clip(1.0 + 0.15 * jax.random.normal(keys[10], (TENANTS, QWIDTH), jnp.float32), 0.25, 1.75),
        "o_down": draw_o_down(jax.random.fold_in(keys[18], 71), 0),
        "o_up": bell_draw(keys[12], (TENANTS, RANK, D), RANK ** -0.5, 1.5, ((2, 8),)),
        "o_magnitude": jnp.clip(1.0 + 0.15 * jax.random.normal(keys[13], (TENANTS, D), jnp.float32), 0.25, 1.75),
        "tenant": with_ends(jax.random.randint(keys[14], (ROWS,), 0, TENANTS), jax.random.fold_in(keys[14], 1), 0, TENANTS - 1).astype(jnp.int32),
        "lengths": draw_lengths(jax.random.fold_in(keys[18], 71), 0),
        "page_table": draw_page_table(jax.random.fold_in(keys[18], 71), 0),
        "kv_cache": draw_kv_cache(jax.random.fold_in(keys[18], 71), 0),
    }


NF4_LEVELS = (-1.0, -0.6961928009986877, -0.5250730514526367, -0.39491748809814453, -0.28444138169288635, -0.18477343022823334, -0.09105003625154495, 0.0, 0.07958029955625534, 0.16093020141124725, 0.24611230194568634, 0.33791524171829224, 0.44070982933044434, 0.5626170039176941, 0.7229568362236023, 1.0)
NORM_EPS = 1e-05
NEG_FILL = -1e+30
ROPE_BASE = 500000.0
PRECISE = lax.Precision.HIGHEST

def nf4_value(code_array):
    level_list = [jnp.float32(level_value) for level_value in NF4_LEVELS]
    for bit_place in range(4):
        bit_set = code_array // 2 ** bit_place % 2 == 1
        level_list = [jnp.where(bit_set, level_list[2 * pair_index + 1], level_list[2 * pair_index]) for pair_index in range(len(level_list) // 2)]
    return level_list[0]

def dequantize(packed, absmax):
    low_levels = nf4_value(packed % 16)
    high_levels = nf4_value(packed // 16)
    in_count, half_cols = packed.shape
    levels = jnp.stack([low_levels, high_levels], axis=-1).reshape(in_count // QBLOCK, QBLOCK, 2 * half_cols)
    return (levels * absmax[:, None, :]).reshape(in_count, 2 * half_cols).astype(jnp.bfloat16)

def rotate(values, positions):
    row_count = values.shape[0]
    half_dim = HEAD_DIM // 2
    frequency = ROPE_BASE ** (-2.0 * jnp.arange(half_dim, dtype=jnp.float32) / HEAD_DIM)
    angles = positions.astype(jnp.float32)[:, None, None] * frequency[None, None, :]
    cosine = jnp.cos(angles)
    sine_part = jnp.sin(angles)
    head_view = values.reshape(row_count, -1, HEAD_DIM)
    front_half = head_view[..., :half_dim]
    back_half = head_view[..., half_dim:]
    turned = jnp.concatenate([front_half * cosine - back_half * sine_part, back_half * cosine + front_half * sine_part], axis=-1)
    return turned.reshape(row_count, -1)

def weight_terms(inputs, down):
    down_float = down.astype(jnp.float32)

    def piece_terms(weight):
        weight_float = weight.astype(jnp.float32)
        product = jnp.dot(inputs, weight, preferred_element_type=jnp.float32)
        cross_terms = jnp.einsum('tdk,dc->tkc', down_float, weight_float, precision=PRECISE)
        squares = lax.optimization_barrier(jnp.sum(weight_float * weight_float, axis=0))
        return (product, cross_terms, squares)
    return piece_terms

def column_pieces(packed, absmax, piece_fn, piece_count):
    half_cols = packed.shape[1] // piece_count

    def one_piece(piece_index):
        codes_part = lax.dynamic_slice_in_dim(packed, piece_index * half_cols, half_cols, 1)
        absmax_part = lax.dynamic_slice_in_dim(absmax, piece_index * 2 * half_cols, 2 * half_cols, 1)
        return piece_fn(dequantize(codes_part, absmax_part))
    return lax.map(one_piece, jnp.arange(piece_count, dtype=jnp.int32))

def join_columns(stacked_part):
    moved = jnp.moveaxis(stacked_part, 0, -2)
    return moved.reshape(moved.shape[:-2] + (-1,))

def gram_terms(down):
    down_float = down.astype(jnp.float32)
    return jnp.einsum('tdk,tdl->tkl', down_float, down_float, precision=PRECISE)

def column_scale(cross_terms, squares, gram_matrix, up, magnitude):
    up_float = up.astype(jnp.float32)
    quadratic = jnp.einsum('tkc,tkl,tlc->tc', up_float, gram_matrix, up_float, precision=PRECISE)
    linear = lax.optimization_barrier(jnp.sum(up_float * cross_terms, axis=1))
    return magnitude.astype(jnp.float32) * lax.rsqrt(squares[None, :] + 2.0 * linear + quadratic)

def adapter_term(inputs, down, up, onehot):
    middle = jnp.einsum('rd,tdk->rtk', inputs.astype(jnp.float32), down.astype(jnp.float32), precision=PRECISE) * onehot[:, :, None]
    return jnp.dot(middle.reshape(middle.shape[0], -1), up.astype(jnp.float32).reshape(-1, up.shape[2]), precision=PRECISE)

def reference(hidden, norm_gain, q_codes, q_absmax, kv_codes, kv_absmax, o_codes, o_absmax, q_down, q_up, q_magnitude, o_down, o_up, o_magnitude, tenant, lengths, page_table, kv_cache):
    states = hidden.astype(jnp.float32)
    mean_square = lax.optimization_barrier(jnp.mean(states * states, axis=1, keepdims=True))
    normed = (states * lax.rsqrt(mean_square + NORM_EPS) * norm_gain.astype(jnp.float32)[None, :]).astype(jnp.bfloat16)
    onehot = (tenant[:, None] == jnp.arange(TENANTS, dtype=jnp.int32)[None, :]).astype(jnp.float32)
    q_parts = column_pieces(q_codes, q_absmax, weight_terms(normed, q_down), N_GY)
    query_base, q_cross, q_squares = [join_columns(stacked_part) for stacked_part in q_parts]
    q_scale = column_scale(q_cross, q_squares, gram_terms(q_down), q_up, q_magnitude)
    query_num = query_base + adapter_term(normed, q_down, q_up, onehot)
    row_scale = jnp.dot(onehot, q_scale, precision=PRECISE)
    query = rotate(query_num * row_scale, lengths).astype(jnp.bfloat16)
    w_keyval = dequantize(kv_codes, kv_absmax)
    keyval = jnp.dot(normed, w_keyval, preferred_element_type=jnp.float32)
    key_width = KV_HEADS * HEAD_DIM
    new_keys = rotate(keyval[:, :key_width], lengths).astype(jnp.bfloat16)
    new_values = keyval[:, key_width:].astype(jnp.bfloat16)
    group = HEADS // KV_HEADS
    inv_root = 1.0 / math.sqrt(HEAD_DIM)
    token_total = MAX_PAGES * PAGE

    def one_row(row_id):
        query_row = query[row_id].astype(jnp.float32).reshape(KV_HEADS, group, HEAD_DIM)
        pages = kv_cache[page_table[row_id]]
        key_rows = pages[:, 0].reshape(token_total, KV_HEADS, HEAD_DIM).astype(jnp.float32)
        value_rows = pages[:, 1].reshape(token_total, KV_HEADS, HEAD_DIM).astype(jnp.float32)
        scores = jnp.einsum('ghd,tgd->ght', query_row, key_rows, precision=PRECISE) * inv_root
        inside = jnp.arange(token_total, dtype=jnp.int32) < lengths[row_id]
        scores = jnp.where(inside[None, None, :], scores, NEG_FILL)
        own_key = new_keys[row_id].astype(jnp.float32).reshape(KV_HEADS, 1, HEAD_DIM)
        own_score = lax.optimization_barrier(jnp.sum(query_row * own_key, axis=-1)) * inv_root
        peak_score = jnp.maximum(lax.optimization_barrier(jnp.max(scores, axis=-1)), own_score)
        weights = jnp.where(inside[None, None, :], jnp.exp(scores - peak_score[..., None]), 0.0)
        own_weight = jnp.exp(own_score - peak_score)
        denominator = lax.optimization_barrier(jnp.sum(weights, axis=-1)) + own_weight
        own_value = new_values[row_id].astype(jnp.float32).reshape(KV_HEADS, 1, HEAD_DIM)
        numerator = jnp.einsum('ght,tgd->ghd', weights, value_rows, precision=PRECISE) + own_weight[..., None] * own_value
        return (numerator / denominator[..., None]).reshape(QWIDTH)
    attended = lax.map(one_row, jnp.arange(ROWS, dtype=jnp.int32)).astype(jnp.bfloat16)
    o_parts = column_pieces(o_codes, o_absmax, weight_terms(attended, o_down), N_GY)
    out_base, o_cross, o_squares = [join_columns(stacked_part) for stacked_part in o_parts]
    o_scale = column_scale(o_cross, o_squares, gram_terms(o_down), o_up, o_magnitude)
    out_num = out_base + adapter_term(attended, o_down, o_up, onehot)
    layer_out = states + out_num * jnp.dot(onehot, o_scale, precision=PRECISE)
    return layer_out.astype(jnp.bfloat16)
```

```python
import functools
import math

import jax
import jax.numpy as jnp
import numpy as np
from jax import lax
from jax.experimental import pallas as pl
from jax.experimental.pallas import tpu as pltpu
from jax.sharding import PartitionSpec as P

HEADS = 128
KV_HEADS = 8
HEAD_DIM = 128
TENANTS = 8
RANK = 16
QBLOCK = 64
PAGE = 256

NF4_LEVELS = (
    -1.0,
    -0.6961928009986877,
    -0.5250730514526367,
    -0.39491748809814453,
    -0.28444138169288635,
    -0.18477343022833234,
    -0.09105003625154495,
    0.0,
    0.07958029955625534,
    0.16093020141124725,
    0.24611230194568634,
    0.33791524171829224,
    0.44070982933044434,
    0.5626170039176941,
    0.7229568362236023,
    1.0,
)
NORM_EPS = 1e-05
NEG_FILL = -1e30
ROPE_BASE = 500000.0
WORDS = 128
COLS = 2 * WORDS
CHUNK = 512
PAD_ROWS = 16
F32 = jnp.float32
BF16 = jnp.bfloat16
GATHER_ROWS = lax.GatherDimensionNumbers(
    offset_dims=(),
    collapsed_slice_dims=(0,),
    start_index_map=(0,),
    operand_batching_dims=(1,),
    start_indices_batching_dims=(1,),
)


def level_table():
    return np.broadcast_to(np.asarray(NF4_LEVELS, np.float32)[:, None], (16, WORDS)).copy()


def split_columns():
    matrix = np.zeros((COLS, COLS), np.float32)
    for column in range(COLS):
        matrix[column, column // 2 + WORDS * (column % 2)] = 1.0
    return matrix


def keyval_order(kv_columns, size_x):
    step = HEAD_DIM // 2 // size_x
    matrix = np.zeros((COLS, size_x * HEAD_DIM), np.float32)
    for column in range(kv_columns):
        head, inner = divmod(column, HEAD_DIM)
        half, turn = divmod(inner, HEAD_DIM // 2)
        piece, spot = divmod(turn, step)
        place = piece * HEAD_DIM + head * 2 * step + half * step + spot
        matrix[column, place] = 1.0
    return matrix


def dot(left, right):
    return jnp.dot(left, right, preferred_element_type=F32)


def dot_rows(left, right):
    return lax.dot_general(left, right, (((1,), (1,)), ((), ())), preferred_element_type=F32)


def three_parts(values):
    first = values.astype(BF16)
    rest = values - first.astype(F32)
    second = rest.astype(BF16)
    third = (rest - second.astype(F32)).astype(BF16)
    return first, second, third


def wide_dot(left, right):
    first, second, third = three_parts(left)
    return (dot(first, right) + dot(second, right)) + dot(third, right)


def pick_rows(table, index):
    return lax.gather(
        table,
        index[..., None],
        GATHER_ROWS,
        slice_sizes=(1, 1),
        mode=lax.GatherScatterMode.PROMISE_IN_BOUNDS,
    )


def weight_tile(codes_ref, scale_ref, level_ref, left_ref, store_ref):
    in_rows = codes_ref.shape[0]
    chunk = min(CHUNK, in_rows)
    blocks = chunk // QBLOCK

    def visit(step, carry):
        total, even_square, odd_square = carry
        even_list = []
        odd_list = []
        for block in range(blocks):
            scale_row = scale_ref[pl.ds(step * blocks + block, 1), :]
            tables = [
                (level_ref[8 * half : 8 * half + 8, :] * scale_row[:, WORDS * side : WORDS * side + WORDS])
                .astype(BF16)
                .astype(F32)
                for side in range(2)
                for half in range(2)
            ]
            for row in range(0, QBLOCK, 8):
                word = codes_ref[pl.ds(step * chunk + block * QBLOCK + row, 8), :]
                low = word & 7
                even = jnp.where(
                    (word & 8) != 0, pick_rows(tables[1], low), pick_rows(tables[0], low)
                )
                high = lax.shift_right_logical(word, 4) & 7
                odd = jnp.where(
                    word >= 128, pick_rows(tables[3], high), pick_rows(tables[2], high)
                )
                even_square = even_square + even * even
                odd_square = odd_square + odd * odd
                even_list.append(even)
                odd_list.append(odd)
        weight = jnp.concatenate(
            [jnp.concatenate(even_list, 0), jnp.concatenate(odd_list, 0)], 1
        ).astype(BF16)
        start = pl.multiple_of(step * chunk, chunk)
        if store_ref is not None:
            store_ref[pl.ds(start, chunk), :] = weight
        total = total + dot(left_ref[:, pl.ds(start, chunk)], weight)
        return (total, even_square, odd_square)

    zero = jnp.zeros((8, WORDS), F32)
    total, even_square, odd_square = lax.fori_loop(
        0,
        in_rows // chunk,
        visit,
        (jnp.zeros((left_ref.shape[0], COLS), F32), zero, zero),
    )
    squares = jnp.concatenate(
        [jnp.sum(even_square, 0, keepdims=True), jnp.sum(odd_square, 0, keepdims=True)], 1
    )
    return total, squares


def block_mask(rows, columns, lead):
    row_id = lax.broadcasted_iota(jnp.int32, (rows, columns), 0)
    column_id = lax.broadcasted_iota(jnp.int32, (rows, columns), 1)
    owner = jnp.where(row_id < lead, row_id, lax.shift_right_logical(row_id - lead, 4))
    return owner == lax.shift_right_logical(column_id, 4)


def norm_terms(cross, gram, up_split, squares, row_count):
    inner = up_split * (2.0 * cross + gram)
    return squares + jnp.sum(inner.reshape(row_count, RANK, COLS), axis=1)


def query_kernel(
    row_count,
    size_x,
    scalar_ref,
    hidden_ref,
    part_ref,
    gain_ref,
    codes_ref,
    absmax_ref,
    kv_codes_ref,
    kv_absmax_ref,
    level_ref,
    split_ref,
    join_ref,
    kv_join_ref,
    *refs,
):
    downs = refs[:row_count]
    ups = refs[row_count : 2 * row_count]
    outs = refs[2 * row_count : 2 * row_count + size_x]
    left_ref, gram_ref, scale_ref, chunk_ref = refs[2 * row_count + size_x :]
    tile = pl.program_id(0)
    tiles = pl.num_programs(0) - 1
    share = chunk_ref.shape[2] - HEAD_DIM

    @pl.when(tile == 0)
    def _():
        states = hidden_ref[...].astype(F32)
        mean_square = jnp.mean(states * states, axis=1, keepdims=True)
        normed = part_ref[...].astype(F32) * lax.rsqrt(mean_square + NORM_EPS) * gain_ref[...]
        lead = jnp.concatenate(
            [normed, jnp.zeros((PAD_ROWS - row_count, normed.shape[1]), F32)], 0
        ).astype(BF16)
        left_ref[0:PAD_ROWS, :] = lead
        for row in range(row_count):
            left_ref[PAD_ROWS + RANK * row : PAD_ROWS + RANK * (row + 1), :] = downs[row][0]
        gram = dot_rows(left_ref[...], left_ref[PAD_ROWS:, :])
        gram_ref[...] = jnp.where(block_mask(*gram.shape, PAD_ROWS), gram, 0.0)

    @pl.when(tile < tiles)
    def _():
        scale_ref[...] = wide_dot(absmax_ref[...], split_ref[...])
        total, squares = weight_tile(codes_ref, scale_ref, level_ref, left_ref, None)
        up_split = dot(jnp.concatenate([up[0] for up in ups], 0), split_ref[...])
        extra = wide_dot(gram_ref[...], up_split.astype(BF16))
        number = total[:row_count] + extra[:row_count]
        norms = norm_terms(total[PAD_ROWS:], extra[PAD_ROWS:], up_split, squares, row_count)
        joined = wide_dot(jnp.concatenate([number, norms], 0), join_ref[...])
        piece = min(COLS, share)
        for part in range(COLS // piece):
            column = tile * COLS + part * piece
            owner = column // share
            chunk_ref[owner, :, pl.ds(pl.multiple_of(column % share, 128), piece)] = joined[
                :, part * piece : (part + 1) * piece
            ]

    @pl.when(tile == tiles)
    def _():
        scale_ref[...] = wide_dot(kv_absmax_ref[...], split_ref[...])
        total, _ = weight_tile(
            kv_codes_ref, scale_ref, level_ref, left_ref.at[0:PAD_ROWS, :], None
        )
        joined = wide_dot(total[: 2 * row_count], kv_join_ref[...])
        for owner in range(size_x):
            chunk_ref[owner, :, share:] = joined[:, owner * HEAD_DIM : (owner + 1) * HEAD_DIM]
        here = scalar_ref[row_count]
        for shift in range(size_x):
            outs[shift][...] = chunk_ref[lax.rem(here + shift, size_x)]


def output_scale_kernel(row_count, scalar_ref, codes_ref, absmax_ref, level_ref, split_ref, join_ref, *refs):
    downs = refs[:row_count]
    ups = refs[row_count : 2 * row_count]
    norm_ref, weight_ref, left_ref, gram_ref, scale_ref = refs[2 * row_count :]

    @pl.when(pl.program_id(0) == 0)
    def _():
        for row in range(row_count):
            left_ref[RANK * row : RANK * (row + 1), :] = downs[row][0]
        gram = dot_rows(left_ref[...], left_ref[...])
        gram_ref[...] = jnp.where(block_mask(*gram.shape, 0), gram, 0.0)

    scale_ref[...] = wide_dot(absmax_ref[...], split_ref[...])
    total, squares = weight_tile(codes_ref, scale_ref, level_ref, left_ref, weight_ref)
    up_split = dot(jnp.concatenate([up[0] for up in ups], 0), split_ref[...])
    extra = wide_dot(gram_ref[...], up_split.astype(BF16))
    norms = norm_terms(total, extra, up_split, squares, row_count)
    norms = jnp.concatenate([norms, jnp.zeros((PAD_ROWS - row_count, COLS), F32)], 0)
    norm_ref[...] = wide_dot(norms, join_ref[...])[:row_count]


def rotate_kernel(row_count, size_x, step, scalar_ref, magnitude_ref, cos_ref, sin_ref, *refs):
    parts = refs[:size_x]
    out_ref = refs[size_x]
    share = cos_ref.shape[1] - HEAD_DIM
    total = parts[0][...]
    for part in parts[1:]:
        total = total + part[...]
    magnitude = jnp.concatenate(
        [
            magnitude_ref[pl.ds(scalar_ref[row], 1), :]
            for row in range(row_count)
        ],
        0,
    )
    query = total[:row_count, :share] * (
        magnitude * lax.rsqrt(total[row_count:, :share])
    )
    keyval = total[:row_count, share:]
    half = HEAD_DIM // 2
    pieces = []
    for head in range(share // HEAD_DIM):
        block = query[:, head * HEAD_DIM : (head + 1) * HEAD_DIM]
        pieces.append(pltpu.roll(block, half, 1))
    lane = lax.broadcasted_iota(jnp.int32, keyval.shape, 1)
    other = jnp.where(
        (lane & step) != 0, pltpu.roll(keyval, step, 1), pltpu.roll(keyval, HEAD_DIM - step, 1)
    )
    values = jnp.concatenate([query, keyval], 1)
    partner = jnp.concatenate(pieces + [other], 1)
    turned = (values * cos_ref[...] + partner * sin_ref[...]).astype(BF16)
    for target in range(out_ref.shape[0]):
        out_ref[target] = turned


def attend_kernel(
    row_count,
    size_x,
    size_y,
    info_ref,
    gathered_ref,
    kv_order_ref,
    page_ref,
    send_ref,
    query_ref,
    mixed_ref,
    best_ref,
    total_ref,
    value_ref,
):
    slot = pl.program_id(0)
    slots = pl.num_programs(0)
    devices = size_x * size_y
    per_target = HEADS // devices
    group = HEADS // KV_HEADS
    inv_root = 1.0 / math.sqrt(HEAD_DIM)
    used = info_ref[2 * slots]
    device = info_ref[2 * slots + 1]
    share = gathered_ref.shape[2] - HEAD_DIM

    @pl.when(slot == 0)
    def _():
        heads_here = share // HEAD_DIM
        for place_x in range(size_x):
            for place_y in range(size_y):
                block = gathered_ref[place_x * size_y + place_y].astype(F32)
                for head in range(heads_here):
                    first = (place_y * size_x + place_x) * heads_here + head
                    query_ref[pl.ds(first, row_count, stride=HEADS), :] = block[
                        :, head * HEAD_DIM : (head + 1) * HEAD_DIM
                    ]
                mixed_ref[place_x, place_y * row_count : (place_y + 1) * row_count, :] = block[
                    :, share:
                ]
        best_ref[...] = jnp.full(best_ref.shape, NEG_FILL, F32)
        total_ref[...] = jnp.zeros(total_ref.shape, F32)
        value_ref[...] = jnp.zeros(value_ref.shape, F32)

        @pl.when(device < row_count)
        def _():
            columns = kv_order_ref.shape[0]
            plain = jnp.zeros((size_y * row_count, columns), F32)
            for place_x in range(size_x):
                plain = plain + dot_rows(
                    mixed_ref[place_x].astype(BF16),
                    kv_order_ref[:, place_x * HEAD_DIM : (place_x + 1) * HEAD_DIM],
                )
            heads_each = 2 * KV_HEADS // size_y
            for row in range(row_count):

                @pl.when(device == row)
                def _():
                    rows = []
                    for head in range(2 * KV_HEADS):
                        place_y, inner = divmod(head, heads_each)
                        line = place_y * row_count + row
                        one = plain[line : line + 1, inner * HEAD_DIM : (inner + 1) * HEAD_DIM]
                        rows.append(jnp.broadcast_to(one, (group, HEAD_DIM)))
                    new_keys = jnp.concatenate(rows[:KV_HEADS], 0)
                    new_values = jnp.concatenate(rows[KV_HEADS:], 0)
                    span = slice(row * HEADS, (row + 1) * HEADS)
                    score = jnp.sum(query_ref[span, :] * new_keys, 1, keepdims=True) * inv_root
                    best_ref[span, :] = jnp.broadcast_to(score, (HEADS, HEAD_DIM))
                    total_ref[span, :] = jnp.ones((HEADS, HEAD_DIM), F32)
                    value_ref[span, :] = new_values

    @pl.when(slot < used)
    def _():
        start = pl.multiple_of(info_ref[slot] * HEADS, HEADS)
        count = info_ref[slots + slot]
        span = pl.ds(start, HEADS)
        query = query_ref[span, :].astype(BF16)
        scores = jnp.concatenate(
            [
                dot_rows(
                    query[group * head : group * (head + 1), :],
                    page_ref[0, 0, :, head * HEAD_DIM : (head + 1) * HEAD_DIM],
                )
                for head in range(KV_HEADS)
            ],
            0,
        )
        inside = lax.broadcasted_iota(jnp.int32, (HEADS, PAGE), 1) < count
        scores = jnp.where(inside, scores * inv_root, NEG_FILL)
        old_best = best_ref[span, :]
        best = jnp.maximum(old_best, jnp.max(scores, axis=1, keepdims=True))
        weights = jnp.where(inside, jnp.exp(scores - best[:, :1]), 0.0)
        keep = jnp.exp(old_best - best)
        best_ref[span, :] = best
        total_ref[span, :] = total_ref[span, :] * keep + jnp.sum(weights, axis=1, keepdims=True)
        coarse = weights.astype(BF16)
        fine = (weights - coarse.astype(F32)).astype(BF16)
        gains = []
        for head in range(KV_HEADS):
            rows = slice(group * head, group * (head + 1))
            both = dot(
                jnp.concatenate([coarse[rows], fine[rows]], 0),
                page_ref[0, 1, :, head * HEAD_DIM : (head + 1) * HEAD_DIM],
            )
            gains.append(both[:group] + both[group:])
        value_ref[span, :] = value_ref[span, :] * keep + jnp.concatenate(gains, 0)

    @pl.when(slot == slots - 1)
    def _():
        eye = lax.broadcasted_iota(jnp.int32, (HEADS, HEAD_DIM), 0) == lax.broadcasted_iota(
            jnp.int32, (HEADS, HEAD_DIM), 1
        )
        lines = []
        for source in (best_ref, total_ref):
            for row in range(row_count):
                block = source[row * HEADS : (row + 1) * HEADS, :]
                lines.append(jnp.sum(jnp.where(eye, block, 0.0), axis=0, keepdims=True))
        scalars = jnp.concatenate(lines, 0)
        for target in range(devices):
            for row in range(row_count):
                begin = row * HEADS + target * per_target
                send_ref[target, row * per_target : (row + 1) * per_target, :] = value_ref[
                    begin : begin + per_target, :
                ]
            send_ref[target, row_count * per_target :, :] = scalars


def merge_kernel(row_count, per_target, info_ref, parts_ref, out_ref):
    offset = info_ref[0] * per_target
    values = parts_ref[:, : row_count * per_target, :]
    scalars = parts_ref[:, row_count * per_target :, :]
    lane = lax.broadcasted_iota(jnp.int32, scalars.shape, 2)
    for row in range(row_count):
        for head in range(per_target):
            chosen = jnp.sum(jnp.where(lane == offset + head, scalars, 0.0), axis=2, keepdims=True)
            best = chosen[:, row : row + 1, :]
            total = chosen[:, row_count + row : row_count + row + 1, :]
            factor = jnp.exp(best - jnp.max(best, axis=0, keepdims=True))
            line = row * per_target + head
            top = jnp.sum(values[:, line : line + 1, :] * factor, axis=0)
            bottom = jnp.sum(total * factor, axis=0)
            out_ref[row : row + 1, head * HEAD_DIM : (head + 1) * HEAD_DIM] = (
                top / bottom
            ).astype(BF16)


def output_kernel(row_count, size_x, scalar_ref, attended_ref, weight_ref, norm_ref, split_ref, join_ref, *refs):
    downs = refs[:row_count]
    ups = refs[row_count : 2 * row_count]
    outs = refs[2 * row_count : 2 * row_count + size_x]
    left_ref, middle_ref, chunk_ref = refs[2 * row_count + size_x :]
    tile = pl.program_id(0)
    tiles = pl.num_programs(0)
    own = row_count // size_x

    @pl.when(tile == 0)
    def _():
        width = attended_ref.shape[2]
        for part in range(attended_ref.shape[0]):
            block = attended_ref[part].astype(F32)
            left_ref[:, part * width : (part + 1) * width] = jnp.concatenate(
                [block, jnp.zeros((PAD_ROWS - row_count, width), F32)], 0
            ).astype(BF16)
        down = jnp.concatenate([down[0] for down in downs], 0)
        middle = dot_rows(left_ref[...], down)
        middle_ref[...] = jnp.where(block_mask(*middle.shape, PAD_ROWS), middle, 0.0)

    up_split = dot(jnp.concatenate([up[0] for up in ups], 0), split_ref[...]).astype(BF16)
    total = dot(left_ref[...], weight_ref[...]) + wide_dot(middle_ref[...], up_split)
    joined = wide_dot(total, join_ref[...])
    columns = pl.ds(pl.multiple_of(tile * COLS, COLS), COLS)
    for owner in range(size_x):
        rows = slice(owner * own, (owner + 1) * own)
        chunk_ref[owner, 0:own, columns] = joined[rows]
        chunk_ref[owner, own : 2 * own, columns] = norm_ref[rows, :]

    @pl.when(tile == tiles - 1)
    def _():
        here = scalar_ref[row_count]
        for shift in range(size_x):
            outs[shift][...] = chunk_ref[lax.rem(here + shift, size_x)]


def finish_kernel(row_count, size_x, scalar_ref, hidden_ref, magnitude_ref, *refs):
    parts = refs[:size_x]
    out_ref = refs[size_x]
    own = row_count // size_x
    total = parts[0][...]
    for part in parts[1:]:
        total = total + part[...]
    here = scalar_ref[row_count]
    states = hidden_ref[...].astype(F32)
    row_id = lax.broadcasted_iota(jnp.int32, states.shape, 0)
    for line in range(own):
        row = here * own + line
        state = jnp.sum(jnp.where(row_id == row, states, 0.0), axis=0, keepdims=True)
        magnitude = magnitude_ref[pl.ds(scalar_ref[row], 1), :]
        scale = magnitude * lax.rsqrt(total[own + line : own + line + 1])
        out_ref[line : line + 1, :] = (state + total[line : line + 1] * scale).astype(BF16)


def slot_info(page_table, lengths, device, slot_count):
    row_count, page_limit = page_table.shape
    page_need = (lengths + PAGE - 1) // PAGE
    page_numbers = jnp.arange(page_limit, dtype=jnp.int32)
    live_mask = page_numbers[None, :] < page_need[:, None]
    wanted = device * slot_count + jnp.arange(slot_count, dtype=jnp.int32)
    hits = ((page_table[None, :, :] == wanted[:, None, None]) & live_mask[None, :, :]).astype(
        jnp.int32
    )
    owner_row = jnp.sum(hits * jnp.arange(row_count, dtype=jnp.int32)[None, :, None], axis=(1, 2))
    remaining = jnp.clip(lengths[:, None] - page_numbers[None, :] * PAGE, 0, PAGE)
    filled = jnp.sum(hits * remaining[None, :, :], axis=(1, 2))
    return owner_row, filled, jnp.sum(hits)


def exchange(parts, axis, size):
    received = [parts[0]]
    for shift in range(1, size):
        received.append(
            lax.ppermute(parts[shift], axis, [(spot, (spot + shift) % size) for spot in range(size)])
        )
    return received


def whole(shape):
    return pl.BlockSpec(shape, lambda *_: (0,) * len(shape))


def local(
    hidden,
    norm_gain,
    q_codes,
    q_absmax,
    kv_codes,
    kv_absmax,
    o_codes,
    o_absmax,
    q_down,
    q_up,
    q_magnitude,
    o_down,
    o_up,
    o_magnitude,
    tenant,
    lengths,
    page_table,
    kv_cache,
):
    row_count, width = hidden.shape
    row_x = lax.axis_index("gx").astype(jnp.int32)
    col_y = lax.axis_index("gy").astype(jnp.int32)
    size_x = lax.axis_size("gx")
    size_y = lax.axis_size("gy")
    devices = size_x * size_y
    device = row_x * size_y + col_y
    in_rows, q_words = q_codes.shape
    q_cols = 2 * q_words
    share = q_cols // size_x
    kv_cols = 2 * kv_codes.shape[1]
    if kv_cols < COLS:
        kv_codes = jnp.pad(kv_codes, ((0, 0), (0, WORDS - kv_codes.shape[1])))
        kv_absmax = jnp.pad(kv_absmax, ((0, 0), (0, COLS - kv_cols)))
    low_rank = row_count * RANK
    level = jnp.asarray(level_table())
    split_matrix = split_columns()
    split = jnp.asarray(split_matrix, BF16)
    join = jnp.asarray(split_matrix.T, BF16)
    order = keyval_order(kv_cols, size_x)
    kv_join = jnp.asarray(split_matrix.T @ order, BF16)
    kv_order = jnp.asarray(order, BF16)
    scalars = jnp.concatenate([tenant, row_x[None], col_y[None]])
    q_down = jnp.swapaxes(q_down, 1, 2)
    o_down = jnp.swapaxes(o_down, 1, 2)
    q_tiles = q_words // WORDS
    scale_rows = in_rows // QBLOCK

    def last(tile):
        return jnp.minimum(tile, q_tiles - 1)

    def down_spec(row):
        return pl.BlockSpec((1, RANK, in_rows), lambda tile, ref: (ref[row], 0, 0))

    def up_spec(row):
        return pl.BlockSpec((1, RANK, COLS), lambda tile, ref: (ref[row], 0, last(tile)))

    adapter_specs = [down_spec(row) for row in range(row_count)] + [
        up_spec(row) for row in range(row_count)
    ]
    chunk_shape = (2 * row_count, share + HEAD_DIM)
    q_parts = pl.pallas_call(
        functools.partial(query_kernel, row_count, size_x),
        grid_spec=pltpu.PrefetchScalarGridSpec(
            num_scalar_prefetch=1,
            grid=(q_tiles + 1,),
            in_specs=[
                whole((row_count, width)),
                pl.BlockSpec((row_count, in_rows), lambda tile, ref: (0, ref[row_count])),
                pl.BlockSpec((1, in_rows), lambda tile, ref: (0, ref[row_count])),
                pl.BlockSpec((in_rows, WORDS), lambda tile, ref: (0, last(tile))),
                pl.BlockSpec((scale_rows, COLS), lambda tile, ref: (0, last(tile))),
                whole((in_rows, WORDS)),
                whole((scale_rows, COLS)),
                whole(level.shape),
                whole(split.shape),
                whole(join.shape),
                whole(kv_join.shape),
                *adapter_specs,
            ],
            out_specs=[whole(chunk_shape)] * size_x,
            scratch_shapes=[
                pltpu.VMEM((PAD_ROWS + low_rank, in_rows), BF16),
                pltpu.VMEM((PAD_ROWS + low_rank, low_rank), F32),
                pltpu.VMEM((scale_rows, COLS), F32),
                pltpu.VMEM((size_x,) + chunk_shape, F32),
            ],
        ),
        out_shape=[jax.ShapeDtypeStruct(chunk_shape, F32)] * size_x,
        name="query",
    )(
        scalars,
        hidden,
        hidden,
        norm_gain.reshape(1, width),
        q_codes,
        q_absmax,
        kv_codes,
        kv_absmax,
        level,
        split,
        join,
        kv_join,
        *([q_down] * row_count),
        *([q_up] * row_count),
    )
    q_parts = exchange(q_parts, "gx", size_x)

    o_norm, w_output = pl.pallas_call(
        functools.partial(output_scale_kernel, row_count),
        grid_spec=pltpu.PrefetchScalarGridSpec(
            num_scalar_prefetch=1,
            grid=(q_tiles,),
            in_specs=[
                pl.BlockSpec((in_rows, WORDS), lambda tile, ref: (0, tile)),
                pl.BlockSpec((scale_rows, COLS), lambda tile, ref: (0, tile)),
                whole(level.shape),
                whole(split.shape),
                whole(join.shape),
                *adapter_specs,
            ],
            out_specs=[
                pl.BlockSpec((row_count, COLS), lambda tile, ref: (0, tile)),
                pl.BlockSpec((in_rows, COLS), lambda tile, ref: (0, tile)),
            ],
            scratch_shapes=[
                pltpu.VMEM((low_rank, in_rows), BF16),
                pltpu.VMEM((low_rank, low_rank), F32),
                pltpu.VMEM((scale_rows, COLS), F32),
            ],
        ),
        out_shape=[
            jax.ShapeDtypeStruct((row_count, q_cols), F32),
            jax.ShapeDtypeStruct((in_rows, q_cols), BF16),
        ],
        cost_estimate=pl.CostEstimate(
            flops=40_000_000 * 256, bytes_accessed=2 * 4 * in_rows * q_words, transcendentals=0
        ),
        name="output_scale",
    )(
        scalars,
        o_codes,
        o_absmax,
        level,
        split,
        join,
        *([o_down] * row_count),
        *([o_up] * row_count),
    )

    half = HEAD_DIM // 2
    step = half // size_x
    lane = jnp.arange(share + HEAD_DIM, dtype=jnp.int32)
    in_query = lane < share
    turn = jnp.where(in_query, lane % half, row_x * step + lane % step)
    second = jnp.where(in_query, lane % HEAD_DIM // half, lane % (2 * step) // step)
    frequency = ROPE_BASE ** (-2.0 * turn.astype(F32) / HEAD_DIM)
    angles = lengths.astype(F32)[:, None] * frequency[None, :]
    plain = jnp.logical_and(~in_query, col_y * kv_cols >= KV_HEADS * HEAD_DIM)[None, :]
    cosine = jnp.where(plain, 1.0, jnp.cos(angles))
    sine = jnp.sin(angles)
    sine = jnp.where(plain, 0.0, jnp.where(second[None, :] == 1, sine, -sine))

    query_all = pl.pallas_call(
        functools.partial(rotate_kernel, row_count, size_x, step),
        grid_spec=pltpu.PrefetchScalarGridSpec(
            num_scalar_prefetch=1,
            grid=(1,),
            in_specs=[
                pl.BlockSpec((TENANTS, share), lambda tile, ref: (0, ref[row_count])),
                whole(cosine.shape),
                whole(sine.shape),
            ]
            + [whole(chunk_shape)] * size_x,
            out_specs=whole((devices, row_count, share + HEAD_DIM)),
        ),
        out_shape=jax.ShapeDtypeStruct((devices, row_count, share + HEAD_DIM), BF16),
        name="rotate",
    )(scalars, q_magnitude, cosine, sine, *q_parts)
    gathered = lax.all_to_all(query_all, ("gx", "gy"), split_axis=0, concat_axis=0, tiled=True)

    slots = kv_cache.shape[0]
    owner_row, filled, used = slot_info(page_table, lengths, device, slots)
    info = jnp.concatenate([owner_row, filled, used[None], device[None]]).astype(jnp.int32)
    per_target = HEADS // devices
    send_shape = (devices, row_count * per_target + 2 * row_count, HEAD_DIM)
    sent = pl.pallas_call(
        functools.partial(attend_kernel, row_count, size_x, size_y),
        grid_spec=pltpu.PrefetchScalarGridSpec(
            num_scalar_prefetch=1,
            grid=(slots,),
            in_specs=[
                whole(gathered.shape),
                whole(kv_order[:kv_cols].shape),
                pl.BlockSpec(
                    (1,) + kv_cache.shape[1:],
                    lambda slot, ref: (
                        jnp.maximum(jnp.minimum(slot, ref[2 * slots] - 1), 0),
                        0,
                        0,
                        0,
                    ),
                ),
            ],
            out_specs=whole(send_shape),
            scratch_shapes=[
                pltpu.VMEM((row_count * HEADS, HEAD_DIM), F32),
                pltpu.VMEM((size_x, size_y * row_count, HEAD_DIM), F32),
                pltpu.VMEM((row_count * HEADS, HEAD_DIM), F32),
                pltpu.VMEM((row_count * HEADS, HEAD_DIM), F32),
                pltpu.VMEM((row_count * HEADS, HEAD_DIM), F32),
            ],
        ),
        out_shape=jax.ShapeDtypeStruct(send_shape, F32),
        name="attend",
    )(info, gathered, kv_order[:kv_cols], kv_cache)
    parts = lax.all_to_all(sent, ("gx", "gy"), split_axis=0, concat_axis=0, tiled=True)

    merged = pl.pallas_call(
        functools.partial(merge_kernel, row_count, per_target),
        in_specs=[
            pl.BlockSpec(memory_space=pltpu.SMEM),
            pl.BlockSpec(memory_space=pltpu.VMEM),
        ],
        out_specs=pl.BlockSpec(memory_space=pltpu.VMEM),
        out_shape=jax.ShapeDtypeStruct((row_count, per_target * HEAD_DIM), BF16),
        name="merge",
    )(device[None], parts)
    attended = lax.all_gather(merged, "gy", axis=0, tiled=False)

    own = row_count // size_x
    o_parts = pl.pallas_call(
        functools.partial(output_kernel, row_count, size_x),
        grid_spec=pltpu.PrefetchScalarGridSpec(
            num_scalar_prefetch=1,
            grid=(q_tiles,),
            in_specs=[
                whole(attended.shape),
                pl.BlockSpec((in_rows, COLS), lambda tile, ref: (0, tile)),
                pl.BlockSpec((row_count, COLS), lambda tile, ref: (0, tile)),
                whole(split.shape),
                whole(join.shape),
                *adapter_specs,
            ],
            out_specs=[whole((2 * own, q_cols))] * size_x,
            scratch_shapes=[
                pltpu.VMEM((PAD_ROWS, in_rows), BF16),
                pltpu.VMEM((PAD_ROWS, low_rank), F32),
                pltpu.VMEM((size_x, 2 * own, q_cols), F32),
            ],
        ),
        out_shape=[jax.ShapeDtypeStruct((2 * own, q_cols), F32)] * size_x,
        name="output",
    )(
        scalars,
        attended,
        w_output,
        o_norm,
        split,
        join,
        *([o_down] * row_count),
        *([o_up] * row_count),
    )
    o_parts = exchange(o_parts, "gx", size_x)
    return pl.pallas_call(
        functools.partial(finish_kernel, row_count, size_x),
        grid_spec=pltpu.PrefetchScalarGridSpec(
            num_scalar_prefetch=1,
            grid=(1,),
            in_specs=[
                pl.BlockSpec((row_count, q_cols), lambda tile, ref: (0, ref[row_count + 1])),
                whole(o_magnitude.shape),
            ]
            + [whole((2 * own, q_cols))] * size_x,
            out_specs=whole((own, q_cols)),
        ),
        out_shape=jax.ShapeDtypeStruct((own, q_cols), BF16),
        name="finish",
    )(scalars, hidden, o_magnitude, *o_parts)


def solution(mesh):
    in_specs = (
        P(),
        P(),
        P("gx", "gy"),
        P("gx", "gy"),
        P("gx", "gy"),
        P("gx", "gy"),
        P("gx", "gy"),
        P("gx", "gy"),
        P(None, "gx", None),
        P(None, None, "gy"),
        P(None, "gy"),
        P(None, "gx", None),
        P(None, None, "gy"),
        P(None, "gy"),
        P(),
        P(),
        P(),
        P(("gx", "gy"), None, None, None),
    )
    out_specs = P("gx", "gy")
    return jax.shard_map(local, mesh=mesh, in_specs=in_specs, out_specs=out_specs, check_vma=False)
```

```python
import functools
import math

import jax
import jax.numpy as jnp
import numpy as np
from jax import lax
from jax.experimental import pallas as pl
from jax.experimental.pallas import tpu as pltpu
from jax.sharding import PartitionSpec as P

HEADS = 128
KV_HEADS = 8
HEAD_DIM = 128
TENANTS = 8
RANK = 16
QBLOCK = 64
PAGE = 256

NF4_LEVELS = (
    -1.0,
    -0.6961928009986877,
    -0.5250730514526367,
    -0.39491748809814453,
    -0.28444138169288635,
    -0.18477343022833234,
    -0.09105003625154495,
    0.0,
    0.07958029955625534,
    0.16093020141124725,
    0.24611230194568634,
    0.33791524171829224,
    0.44070982933044434,
    0.5626170039176941,
    0.7229568362236023,
    1.0,
)
NORM_EPS = 1e-05
NEG_FILL = -1e30
ROPE_BASE = 500000.0
WORDS = 128
COLS = 2 * WORDS
CHUNK = 2048
PAD_ROWS = 16
DEPTH = 3
F32 = jnp.float32
BF16 = jnp.bfloat16
GATHER_ROWS = lax.GatherDimensionNumbers(
    offset_dims=(),
    collapsed_slice_dims=(0,),
    start_index_map=(0,),
    operand_batching_dims=(1,),
    start_indices_batching_dims=(1,),
)


def level_table():
    return np.broadcast_to(np.asarray(NF4_LEVELS, np.float32)[:, None], (16, WORDS)).copy()


def split_columns():
    matrix = np.zeros((COLS, COLS), np.float32)
    for column in range(COLS):
        matrix[column, column // 2 + WORDS * (column % 2)] = 1.0
    return matrix


def keyval_order(kv_columns, size_x):
    step = HEAD_DIM // 2 // size_x
    matrix = np.zeros((COLS, size_x * HEAD_DIM), np.float32)
    for column in range(kv_columns):
        head, inner = divmod(column, HEAD_DIM)
        half, turn = divmod(inner, HEAD_DIM // 2)
        piece, spot = divmod(turn, step)
        place = piece * HEAD_DIM + head * 2 * step + half * step + spot
        matrix[column, place] = 1.0
    return matrix


def dot(left, right):
    return jnp.dot(left, right, preferred_element_type=F32)


def dot_rows(left, right):
    return lax.dot_general(left, right, (((1,), (1,)), ((), ())), preferred_element_type=F32)


def three_parts(values):
    first = values.astype(BF16)
    rest = values - first.astype(F32)
    second = rest.astype(BF16)
    third = (rest - second.astype(F32)).astype(BF16)
    return first, second, third


def wide_dot(left, right):
    rows = left.shape[0]
    both = dot(jnp.concatenate(three_parts(left), 0), right)
    return (both[:rows] + both[rows : 2 * rows]) + both[2 * rows :]


def split_scales(absmax_ref, split_ref, scale_ref, first, tiles):
    rows = absmax_ref.shape[0]
    stacked = jnp.concatenate(
        [absmax_ref[:, COLS * tile : COLS * (tile + 1)] for tile in range(tiles)], 0
    )
    both = wide_dot(stacked, split_ref[...])
    for tile in range(tiles):
        scale_ref[first + tile] = both[rows * tile : rows * (tile + 1)]


def stack_tiles(array):
    return jnp.concatenate(
        [array[:, COLS * tile : COLS * (tile + 1)] for tile in range(array.shape[1] // COLS)], 0
    )


def pick_rows(table, index):
    return lax.gather(
        table,
        index[..., None],
        GATHER_ROWS,
        slice_sizes=(1, 1),
        mode=lax.GatherScatterMode.PROMISE_IN_BOUNDS,
    )


def weight_tile(codes_ref, scale_ref, level_ref, left_ref, store_ref):
    in_rows = codes_ref.shape[0]
    chunk = min(CHUNK, in_rows)
    blocks = chunk // QBLOCK

    def visit(step, carry):
        total, even_square, odd_square = carry
        even_list = []
        odd_list = []
        for block in range(blocks):
            scale_row = scale_ref[pl.ds(step * blocks + block, 1), :]
            tables = [
                (level_ref[8 * half : 8 * half + 8, :] * scale_row[:, WORDS * side : WORDS * side + WORDS])
                .astype(BF16)
                .astype(F32)
                for side in range(2)
                for half in range(2)
            ]
            for row in range(0, QBLOCK, 8):
                word = codes_ref[pl.ds(step * chunk + block * QBLOCK + row, 8), :]
                low = word & 7
                even = jnp.where(
                    (word & 8) != 0, pick_rows(tables[1], low), pick_rows(tables[0], low)
                )
                high = lax.shift_right_logical(word, 4) & 7
                odd = jnp.where(
                    word >= 128, pick_rows(tables[3], high), pick_rows(tables[2], high)
                )
                even_square = even_square + even * even
                odd_square = odd_square + odd * odd
                even_list.append(even)
                odd_list.append(odd)
        weight = jnp.concatenate(
            [jnp.concatenate(even_list, 0), jnp.concatenate(odd_list, 0)], 1
        ).astype(BF16)
        start = pl.multiple_of(step * chunk, chunk)
        if store_ref is not None:
            store_ref[pl.ds(start, chunk), :] = weight
        total = total + dot(left_ref[:, pl.ds(start, chunk)], weight)
        return (total, even_square, odd_square)

    zero = jnp.zeros((8, WORDS), F32)
    total, even_square, odd_square = lax.fori_loop(
        0,
        in_rows // chunk,
        visit,
        (jnp.zeros((left_ref.shape[0], COLS), F32), zero, zero),
    )
    return total, jnp.concatenate([even_square, odd_square], 1)


def block_mask(rows, columns, lead):
    row_id = lax.broadcasted_iota(jnp.int32, (rows, columns), 0)
    column_id = lax.broadcasted_iota(jnp.int32, (rows, columns), 1)
    owner = jnp.where(row_id < lead, row_id, lax.shift_right_logical(row_id - lead, 4))
    return owner == lax.shift_right_logical(column_id, 4)


def norm_terms(cross, gram, up_split, squares, row_count):
    inner = up_split * (2.0 * cross + gram)
    return jnp.sum(squares, 0, keepdims=True) + jnp.sum(
        inner.reshape(row_count, RANK, COLS), axis=1
    )


def code_copy(codes_ref, first, tile, buffer_ref, sems):
    columns = pl.ds(pl.multiple_of((first + tile) * WORDS, WORDS), WORDS)
    slot = tile % DEPTH if isinstance(tile, int) else lax.rem(tile, DEPTH)
    return pltpu.make_async_copy(codes_ref.at[:, columns], buffer_ref.at[slot], sems.at[slot])


def code_tile(codes_ref, first, tile, tiles, buffer_ref, sems):
    @pl.when(tile + DEPTH - 1 < tiles)
    def _():
        code_copy(codes_ref, first, tile + DEPTH - 1, buffer_ref, sems).start()

    code_copy(codes_ref, first, tile, buffer_ref, sems).wait()
    return buffer_ref.at[lax.rem(tile, DEPTH)]


def tenant_copies(scalar_ref, row_count, down_ref, up_ref, left_ref, lead, ups_ref, sems):
    downs = []
    ups = []
    for row in range(row_count):
        tenant = scalar_ref[row]
        downs.append(
            pltpu.make_async_copy(
                down_ref.at[tenant],
                left_ref.at[lead + RANK * row : lead + RANK * (row + 1), :],
                sems.at[row],
            )
        )
        ups.append(
            pltpu.make_async_copy(
                up_ref.at[tenant],
                ups_ref.at[RANK * row : RANK * (row + 1), :],
                sems.at[row_count + row],
            )
        )
    return downs, ups


def query_kernel(
    row_count,
    size_x,
    scalar_ref,
    hidden_ref,
    part_ref,
    gain_ref,
    absmax_ref,
    kv_absmax_ref,
    level_ref,
    split_ref,
    join_ref,
    kv_join_ref,
    codes_ref,
    kv_codes_ref,
    down_ref,
    up_ref,
    *refs,
):
    outs = refs[:size_x]
    (
        left_ref,
        scale_ref,
        total_ref,
        square_ref,
        chunk_ref,
        buffer_ref,
        kv_buffer_ref,
        ups_ref,
        code_sems,
        kv_sem,
        tenant_sems,
    ) = refs[size_x:]
    tiles = absmax_ref.shape[1] // COLS
    share = chunk_ref.shape[2] - HEAD_DIM
    low_rank = row_count * RANK
    here = scalar_ref[row_count]
    downs, ups = tenant_copies(
        scalar_ref, row_count, down_ref, up_ref, left_ref, PAD_ROWS, ups_ref, tenant_sems
    )
    kv_copy = pltpu.make_async_copy(kv_codes_ref, kv_buffer_ref, kv_sem.at[0])
    kv_copy.start()
    for copy in downs:
        copy.start()
    for tile in range(min(DEPTH - 1, tiles)):
        code_copy(codes_ref, 0, tile, buffer_ref, code_sems).start()
    for copy in ups:
        copy.start()

    states = hidden_ref[...].astype(F32)
    mean_square = jnp.mean(states * states, axis=1, keepdims=True)
    normed = part_ref[...].astype(F32) * lax.rsqrt(mean_square + NORM_EPS) * gain_ref[...]
    left_ref[0:PAD_ROWS, :] = jnp.concatenate(
        [normed, jnp.zeros((PAD_ROWS - row_count, normed.shape[1]), F32)], 0
    ).astype(BF16)
    split_scales(kv_absmax_ref, split_ref, scale_ref, 0, 1)
    split_scales(absmax_ref, split_ref, scale_ref, 1, tiles)
    kv_copy.wait()
    total, _ = weight_tile(
        kv_buffer_ref, scale_ref.at[0], level_ref, left_ref.at[0:PAD_ROWS, :], None
    )
    joined = wide_dot(total, kv_join_ref[...])
    for owner in range(size_x):
        chunk_ref[owner, :, share:] = joined[
            : 2 * row_count, owner * HEAD_DIM : (owner + 1) * HEAD_DIM
        ]
    for copy in downs:
        copy.wait()

    def visit(tile, carry):
        codes = code_tile(codes_ref, 0, tile, tiles, buffer_ref, code_sems)
        total, squares = weight_tile(
            codes, scale_ref.at[tile + 1], level_ref, left_ref, None
        )
        total_ref[tile] = total
        square_ref[tile] = squares
        return carry

    lax.fori_loop(0, tiles, visit, 0)
    for copy in ups:
        copy.wait()
    gram = dot_rows(left_ref[...], left_ref[PAD_ROWS:, :])
    gram = jnp.where(block_mask(*gram.shape, PAD_ROWS), gram, 0.0)
    up_split = dot(stack_tiles(ups_ref[...]), split_ref[...])
    lines = []
    for tile in range(tiles):
        up_tile = up_split[low_rank * tile : low_rank * (tile + 1)]
        extra = wide_dot(gram, up_tile.astype(BF16))
        total = total_ref[tile]
        lines.append(total[:row_count] + extra[:row_count])
        lines.append(
            norm_terms(total[PAD_ROWS:], extra[PAD_ROWS:], up_tile, square_ref[tile], row_count)
        )
    joined = wide_dot(jnp.concatenate(lines, 0), join_ref[...])
    piece = min(COLS, share)
    for tile in range(tiles):
        for part in range(COLS // piece):
            owner, place = divmod(tile * COLS + part * piece, share)
            chunk_ref[owner, :, place : place + piece] = joined[
                2 * row_count * tile : 2 * row_count * (tile + 1),
                part * piece : (part + 1) * piece,
            ]
    for shift in range(size_x):
        outs[shift][...] = chunk_ref[lax.rem(here + shift, size_x)]


def store_copy(store_ref, slot, weight_ref, tile, sems):
    return pltpu.make_async_copy(store_ref.at[slot], weight_ref.at[tile], sems.at[slot])


def output_scale_kernel(
    row_count,
    first,
    scalar_ref,
    absmax_ref,
    level_ref,
    split_ref,
    join_ref,
    codes_ref,
    down_ref,
    up_ref,
    norm_ref,
    up_split_ref,
    weight_ref,
    store_ref,
    left_ref,
    scale_ref,
    total_ref,
    square_ref,
    buffer_ref,
    ups_ref,
    code_sems,
    tenant_sems,
    store_sems,
):
    tiles = weight_ref.shape[0]
    low_rank = row_count * RANK
    downs, ups = tenant_copies(
        scalar_ref,
        row_count,
        down_ref,
        up_ref.at[:, :, first * COLS : (first + tiles) * COLS],
        left_ref,
        0,
        ups_ref,
        tenant_sems,
    )
    for copy in downs:
        copy.start()
    for tile in range(min(DEPTH - 1, tiles)):
        code_copy(codes_ref, first, tile, buffer_ref, code_sems).start()
    for copy in ups:
        copy.start()
    split_scales(absmax_ref, split_ref, scale_ref, 0, tiles)
    for copy in downs:
        copy.wait()

    def visit(tile, carry):
        codes = code_tile(codes_ref, first, tile, tiles, buffer_ref, code_sems)
        slot = lax.rem(tile, 2)

        @pl.when(tile >= 2)
        def _():
            store_copy(store_ref, slot, weight_ref, tile - 2, store_sems).wait()

        total, squares = weight_tile(
            codes, scale_ref.at[tile], level_ref, left_ref, store_ref.at[slot]
        )
        store_copy(store_ref, slot, weight_ref, tile, store_sems).start()
        total_ref[tile] = total
        square_ref[tile] = squares
        return carry

    lax.fori_loop(0, tiles, visit, 0)
    for copy in ups:
        copy.wait()
    gram = dot_rows(left_ref[...], left_ref[...])
    gram = jnp.where(block_mask(*gram.shape, 0), gram, 0.0)
    up_split = dot(stack_tiles(ups_ref[...]), split_ref[...])
    lines = []
    for tile in range(tiles):
        up_tile = up_split[low_rank * tile : low_rank * (tile + 1)]
        narrow = up_tile.astype(BF16)
        up_split_ref[:, COLS * tile : COLS * (tile + 1)] = narrow
        extra = wide_dot(gram, narrow)
        lines.append(norm_terms(total_ref[tile], extra, up_tile, square_ref[tile], row_count))
    joined = wide_dot(jnp.concatenate(lines, 0), join_ref[...])
    for tile in range(tiles):
        norm_ref[:, COLS * tile : COLS * (tile + 1)] = joined[
            row_count * tile : row_count * (tile + 1)
        ]
    for tile in range(max(tiles - 2, 0), tiles):
        store_copy(store_ref, tile % 2, weight_ref, tile, store_sems).wait()


def rotate_kernel(row_count, size_x, step, scalar_ref, magnitude_ref, cos_ref, sin_ref, *refs):
    parts = refs[:size_x]
    out_ref = refs[size_x]
    share = cos_ref.shape[1] - HEAD_DIM
    total = parts[0][...]
    for part in parts[1:]:
        total = total + part[...]
    magnitude = jnp.concatenate(
        [
            magnitude_ref[pl.ds(scalar_ref[row], 1), :]
            for row in range(row_count)
        ],
        0,
    )
    query = total[:row_count, :share] * (
        magnitude * lax.rsqrt(total[row_count:, :share])
    )
    keyval = total[:row_count, share:]
    half = HEAD_DIM // 2
    pieces = []
    for head in range(share // HEAD_DIM):
        block = query[:, head * HEAD_DIM : (head + 1) * HEAD_DIM]
        pieces.append(pltpu.roll(block, half, 1))
    lane = lax.broadcasted_iota(jnp.int32, keyval.shape, 1)
    other = jnp.where(
        (lane & step) != 0, pltpu.roll(keyval, step, 1), pltpu.roll(keyval, HEAD_DIM - step, 1)
    )
    values = jnp.concatenate([query, keyval], 1)
    partner = jnp.concatenate(pieces + [other], 1)
    turned = (values * cos_ref[...] + partner * sin_ref[...]).astype(BF16)
    for target in range(out_ref.shape[0]):
        out_ref[target] = turned


def attend_kernel(
    row_count,
    size_x,
    size_y,
    info_ref,
    gathered_ref,
    kv_order_ref,
    page_ref,
    send_ref,
    query_ref,
    mixed_ref,
    best_ref,
    total_ref,
    value_ref,
):
    slot = pl.program_id(0)
    slots = pl.num_programs(0)
    devices = size_x * size_y
    per_target = HEADS // devices
    group = HEADS // KV_HEADS
    inv_root = 1.0 / math.sqrt(HEAD_DIM)
    used = info_ref[2 * slots]
    device = info_ref[2 * slots + 1]
    share = gathered_ref.shape[2] - HEAD_DIM

    @pl.when(slot == 0)
    def _():
        heads_here = share // HEAD_DIM
        for place_x in range(size_x):
            for place_y in range(size_y):
                block = gathered_ref[place_x * size_y + place_y].astype(F32)
                for head in range(heads_here):
                    first = (place_y * size_x + place_x) * heads_here + head
                    query_ref[pl.ds(first, row_count, stride=HEADS), :] = block[
                        :, head * HEAD_DIM : (head + 1) * HEAD_DIM
                    ]
                mixed_ref[place_x, place_y * row_count : (place_y + 1) * row_count, :] = block[
                    :, share:
                ]
        best_ref[...] = jnp.full(best_ref.shape, NEG_FILL, F32)
        total_ref[...] = jnp.zeros(total_ref.shape, F32)
        value_ref[...] = jnp.zeros(value_ref.shape, F32)

        @pl.when(device < row_count)
        def _():
            columns = kv_order_ref.shape[0]
            plain = jnp.zeros((size_y * row_count, columns), F32)
            for place_x in range(size_x):
                plain = plain + dot_rows(
                    mixed_ref[place_x].astype(BF16),
                    kv_order_ref[:, place_x * HEAD_DIM : (place_x + 1) * HEAD_DIM],
                )
            heads_each = 2 * KV_HEADS // size_y
            for row in range(row_count):

                @pl.when(device == row)
                def _():
                    rows = []
                    for head in range(2 * KV_HEADS):
                        place_y, inner = divmod(head, heads_each)
                        line = place_y * row_count + row
                        one = plain[line : line + 1, inner * HEAD_DIM : (inner + 1) * HEAD_DIM]
                        rows.append(jnp.broadcast_to(one, (group, HEAD_DIM)))
                    new_keys = jnp.concatenate(rows[:KV_HEADS], 0)
                    new_values = jnp.concatenate(rows[KV_HEADS:], 0)
                    span = slice(row * HEADS, (row + 1) * HEADS)
                    score = jnp.sum(query_ref[span, :] * new_keys, 1, keepdims=True) * inv_root
                    best_ref[span, :] = jnp.broadcast_to(score, (HEADS, HEAD_DIM))
                    total_ref[span, :] = jnp.ones((HEADS, HEAD_DIM), F32)
                    value_ref[span, :] = new_values

    @pl.when(slot < used)
    def _():
        start = pl.multiple_of(info_ref[slot] * HEADS, HEADS)
        count = info_ref[slots + slot]
        span = pl.ds(start, HEADS)
        query = query_ref[span, :].astype(BF16)
        scores = jnp.concatenate(
            [
                dot_rows(
                    query[group * head : group * (head + 1), :],
                    page_ref[0, 0, :, head * HEAD_DIM : (head + 1) * HEAD_DIM],
                )
                for head in range(KV_HEADS)
            ],
            0,
        )
        inside = lax.broadcasted_iota(jnp.int32, (HEADS, PAGE), 1) < count
        scores = jnp.where(inside, scores * inv_root, NEG_FILL)
        old_best = best_ref[span, :]
        best = jnp.maximum(old_best, jnp.max(scores, axis=1, keepdims=True))
        weights = jnp.where(inside, jnp.exp(scores - best[:, :1]), 0.0)
        keep = jnp.exp(old_best - best)
        best_ref[span, :] = best
        total_ref[span, :] = total_ref[span, :] * keep + jnp.sum(weights, axis=1, keepdims=True)
        coarse = weights.astype(BF16)
        fine = (weights - coarse.astype(F32)).astype(BF16)
        gains = []
        for head in range(KV_HEADS):
            rows = slice(group * head, group * (head + 1))
            both = dot(
                jnp.concatenate([coarse[rows], fine[rows]], 0),
                page_ref[0, 1, :, head * HEAD_DIM : (head + 1) * HEAD_DIM],
            )
            gains.append(both[:group] + both[group:])
        value_ref[span, :] = value_ref[span, :] * keep + jnp.concatenate(gains, 0)

    @pl.when(slot == slots - 1)
    def _():
        eye = lax.broadcasted_iota(jnp.int32, (HEADS, HEAD_DIM), 0) == lax.broadcasted_iota(
            jnp.int32, (HEADS, HEAD_DIM), 1
        )
        lines = []
        for source in (best_ref, total_ref):
            for row in range(row_count):
                block = source[row * HEADS : (row + 1) * HEADS, :]
                lines.append(jnp.sum(jnp.where(eye, block, 0.0), axis=0, keepdims=True))
        scalars = jnp.concatenate(lines, 0)
        for target in range(devices):
            for row in range(row_count):
                begin = row * HEADS + target * per_target
                send_ref[target, row * per_target : (row + 1) * per_target, :] = value_ref[
                    begin : begin + per_target, :
                ]
            send_ref[target, row_count * per_target :, :] = scalars


def merge_kernel(row_count, per_target, info_ref, parts_ref, out_ref):
    offset = info_ref[0] * per_target
    values = parts_ref[:, : row_count * per_target, :]
    scalars = parts_ref[:, row_count * per_target :, :]
    lane = lax.broadcasted_iota(jnp.int32, scalars.shape, 2)
    for row in range(row_count):
        for head in range(per_target):
            chosen = jnp.sum(jnp.where(lane == offset + head, scalars, 0.0), axis=2, keepdims=True)
            best = chosen[:, row : row + 1, :]
            total = chosen[:, row_count + row : row_count + row + 1, :]
            factor = jnp.exp(best - jnp.max(best, axis=0, keepdims=True))
            line = row * per_target + head
            top = jnp.sum(values[:, line : line + 1, :] * factor, axis=0)
            bottom = jnp.sum(total * factor, axis=0)
            ratio = (top / bottom).astype(BF16)
            for target in range(out_ref.shape[0]):
                out_ref[target, row : row + 1, head * HEAD_DIM : (head + 1) * HEAD_DIM] = ratio


def output_kernel(row_count, size_x, tile_counts, scalar_ref, attended_ref, join_ref, down_ref, *refs):
    parts = len(tile_counts)
    norms = refs[:parts]
    ups = refs[parts : 2 * parts]
    weights = refs[2 * parts : 3 * parts]
    outs = refs[3 * parts : 3 * parts + size_x]
    left_ref, total_ref, chunk_ref, low_ref, held_ref, sems, held_sems = refs[3 * parts + size_x :]
    tiles = sum(tile_counts)
    own = row_count // size_x
    copies = [
        pltpu.make_async_copy(
            down_ref.at[scalar_ref[row]],
            low_ref.at[RANK * row : RANK * (row + 1), :],
            sems.at[row],
        )
        for row in range(row_count)
    ]
    first = 0
    for part in range(parts):
        for tile in range(tile_counts[part]):
            pltpu.make_async_copy(
                weights[part].at[tile], held_ref.at[first + tile], held_sems.at[first + tile]
            ).start()
        first += tile_counts[part]
    for copy in copies:
        copy.start()
    width = attended_ref.shape[2]
    for part in range(attended_ref.shape[0]):
        block = attended_ref[part].astype(F32)
        left_ref[:, part * width : (part + 1) * width] = jnp.concatenate(
            [block, jnp.zeros((PAD_ROWS - row_count, width), F32)], 0
        ).astype(BF16)
    first = 0
    for part in range(parts):

        def visit(tile, carry, part=part, first=first):
            pltpu.make_async_copy(
                weights[part].at[tile], held_ref.at[first + tile], held_sems.at[first + tile]
            ).wait()
            total_ref[first + tile] = dot(left_ref[...], held_ref[first + tile])
            return carry

        lax.fori_loop(0, tile_counts[part], visit, 0)
        first += tile_counts[part]
    for copy in copies:
        copy.wait()
    middle = dot_rows(left_ref[...], low_ref[...])
    middle = jnp.where(block_mask(*middle.shape, PAD_ROWS), middle, 0.0)
    lines = []
    spot = 0
    for part in range(parts):
        extra = wide_dot(middle, ups[part][...])
        for tile in range(tile_counts[part]):
            lines.append(
                total_ref[spot, 0:row_count] + extra[:row_count, COLS * tile : COLS * (tile + 1)]
            )
            spot += 1
    joined = wide_dot(jnp.concatenate(lines, 0), join_ref[...])
    for owner in range(size_x):
        for spot in range(tiles):
            begin = row_count * spot + owner * own
            chunk_ref[owner, 0:own, COLS * spot : COLS * (spot + 1)] = joined[begin : begin + own]
        begin = 0
        for part in range(parts):
            columns = COLS * tile_counts[part]
            chunk_ref[owner, own : 2 * own, begin : begin + columns] = norms[part][
                owner * own : (owner + 1) * own, :
            ]
            begin += columns
    here = scalar_ref[row_count]
    for shift in range(size_x):
        outs[shift][...] = chunk_ref[lax.rem(here + shift, size_x)]


def finish_kernel(row_count, size_x, scalar_ref, hidden_ref, magnitude_ref, *refs):
    parts = refs[:size_x]
    out_ref = refs[size_x]
    own = row_count // size_x
    total = parts[0][...]
    for part in parts[1:]:
        total = total + part[...]
    here = scalar_ref[row_count]
    states = hidden_ref[...].astype(F32)
    row_id = lax.broadcasted_iota(jnp.int32, states.shape, 0)
    for line in range(own):
        row = here * own + line
        state = jnp.sum(jnp.where(row_id == row, states, 0.0), axis=0, keepdims=True)
        magnitude = magnitude_ref[pl.ds(scalar_ref[row], 1), :]
        scale = magnitude * lax.rsqrt(total[own + line : own + line + 1])
        out_ref[line : line + 1, :] = (state + total[line : line + 1] * scale).astype(BF16)


def slot_info(page_table, lengths, device, slot_count):
    row_count, page_limit = page_table.shape
    page_need = (lengths + PAGE - 1) // PAGE
    page_numbers = jnp.arange(page_limit, dtype=jnp.int32)
    live_mask = page_numbers[None, :] < page_need[:, None]
    wanted = device * slot_count + jnp.arange(slot_count, dtype=jnp.int32)
    hits = ((page_table[None, :, :] == wanted[:, None, None]) & live_mask[None, :, :]).astype(
        jnp.int32
    )
    owner_row = jnp.sum(hits * jnp.arange(row_count, dtype=jnp.int32)[None, :, None], axis=(1, 2))
    remaining = jnp.clip(lengths[:, None] - page_numbers[None, :] * PAGE, 0, PAGE)
    filled = jnp.sum(hits * remaining[None, :, :], axis=(1, 2))
    return owner_row, filled, jnp.sum(hits)


def exchange(parts, axis, size):
    received = [parts[0]]
    for shift in range(1, size):
        received.append(
            lax.ppermute(parts[shift], axis, [(spot, (spot + shift) % size) for spot in range(size)])
        )
    return received


def whole(shape):
    return pl.BlockSpec(shape, lambda *_: (0,) * len(shape))


def local(
    hidden,
    norm_gain,
    q_codes,
    q_absmax,
    kv_codes,
    kv_absmax,
    o_codes,
    o_absmax,
    q_down,
    q_up,
    q_magnitude,
    o_down,
    o_up,
    o_magnitude,
    tenant,
    lengths,
    page_table,
    kv_cache,
):
    row_count, width = hidden.shape
    row_x = lax.axis_index("gx").astype(jnp.int32)
    col_y = lax.axis_index("gy").astype(jnp.int32)
    size_x = lax.axis_size("gx")
    size_y = lax.axis_size("gy")
    devices = size_x * size_y
    device = row_x * size_y + col_y
    in_rows, q_words = q_codes.shape
    q_cols = 2 * q_words
    share = q_cols // size_x
    kv_cols = 2 * kv_codes.shape[1]
    if kv_cols < COLS:
        kv_codes = jnp.pad(kv_codes, ((0, 0), (0, WORDS - kv_codes.shape[1])))
        kv_absmax = jnp.pad(kv_absmax, ((0, 0), (0, COLS - kv_cols)))
    low_rank = row_count * RANK
    level = jnp.asarray(level_table())
    split_matrix = split_columns()
    split = jnp.asarray(split_matrix, BF16)
    join = jnp.asarray(split_matrix.T, BF16)
    order = keyval_order(kv_cols, size_x)
    kv_join = jnp.asarray(split_matrix.T @ order, BF16)
    kv_order = jnp.asarray(order, BF16)
    scalars = jnp.concatenate([tenant, row_x[None], col_y[None]])
    q_down = jnp.swapaxes(q_down, 1, 2)
    o_down = jnp.swapaxes(o_down, 1, 2)
    q_tiles = q_words // WORDS
    scale_rows = in_rows // QBLOCK

    smem = pl.BlockSpec(memory_space=pltpu.SMEM)
    vmem = pl.BlockSpec(memory_space=pltpu.VMEM)
    anywhere = pl.BlockSpec(memory_space=pltpu.HBM)
    chunk_shape = (2 * row_count, share + HEAD_DIM)
    start = row_x * in_rows
    q_parts = pl.pallas_call(
        functools.partial(query_kernel, row_count, size_x),
        in_specs=[smem] + [vmem] * 9 + [anywhere] * 4,
        out_specs=[vmem] * size_x,
        scratch_shapes=[
            pltpu.VMEM((PAD_ROWS + low_rank, in_rows), BF16),
            pltpu.VMEM((q_tiles + 1, scale_rows, COLS), F32),
            pltpu.VMEM((q_tiles, PAD_ROWS + low_rank, COLS), F32),
            pltpu.VMEM((q_tiles, 8, COLS), F32),
            pltpu.VMEM((size_x,) + chunk_shape, F32),
            pltpu.VMEM((DEPTH, in_rows, WORDS), jnp.int32),
            pltpu.VMEM((in_rows, WORDS), jnp.int32),
            pltpu.VMEM((low_rank, q_cols), BF16),
            pltpu.SemaphoreType.DMA((DEPTH,)),
            pltpu.SemaphoreType.DMA((1,)),
            pltpu.SemaphoreType.DMA((2 * row_count,)),
        ],
        out_shape=[jax.ShapeDtypeStruct(chunk_shape, F32)] * size_x,
        name="query",
    )(
        scalars,
        hidden,
        lax.dynamic_slice_in_dim(hidden, start, in_rows, 1),
        lax.dynamic_slice_in_dim(norm_gain, start, in_rows, 0)[None, :],
        q_absmax,
        kv_absmax,
        level,
        split,
        join,
        kv_join,
        q_codes,
        kv_codes,
        q_down,
        q_up,
    )
    q_parts = exchange(q_parts, "gx", size_x)

    def output_scales(first, tiles):
        return pl.pallas_call(
            functools.partial(output_scale_kernel, row_count, first),
            in_specs=[smem] + [vmem] * 4 + [anywhere] * 3,
            out_specs=[vmem, vmem, anywhere],
            scratch_shapes=[
                pltpu.VMEM((2, in_rows, COLS), BF16),
                pltpu.VMEM((low_rank, in_rows), BF16),
                pltpu.VMEM((tiles, scale_rows, COLS), F32),
                pltpu.VMEM((tiles, low_rank, COLS), F32),
                pltpu.VMEM((tiles, 8, COLS), F32),
                pltpu.VMEM((DEPTH, in_rows, WORDS), jnp.int32),
                pltpu.VMEM((low_rank, tiles * COLS), BF16),
                pltpu.SemaphoreType.DMA((DEPTH,)),
                pltpu.SemaphoreType.DMA((2 * row_count,)),
                pltpu.SemaphoreType.DMA((2,)),
            ],
            out_shape=[
                jax.ShapeDtypeStruct((row_count, tiles * COLS), F32),
                jax.ShapeDtypeStruct((low_rank, tiles * COLS), BF16),
                jax.ShapeDtypeStruct((tiles, in_rows, COLS), BF16),
            ],
            cost_estimate=pl.CostEstimate(
                flops=tiles * 5_000_000 * 256,
                bytes_accessed=tiles * 8 * in_rows * WORDS,
                transcendentals=0,
            ),
            compiler_params=pltpu.CompilerParams(vmem_limit_bytes=24 * 2**20),
            name="output_scale",
        )(
            scalars,
            lax.slice_in_dim(o_absmax, first * COLS, (first + tiles) * COLS, axis=1),
            level,
            split,
            join,
            o_codes,
            o_down,
            o_up,
        )

    tile_counts = [q_tiles]
    scale_parts = [
        output_scales(sum(tile_counts[:part]), tile_counts[part])
        for part in range(len(tile_counts))
    ]

    half = HEAD_DIM // 2
    step = half // size_x
    lane = jnp.arange(share + HEAD_DIM, dtype=jnp.int32)
    in_query = lane < share
    turn = jnp.where(in_query, lane % half, row_x * step + lane % step)
    second = jnp.where(in_query, lane % HEAD_DIM // half, lane % (2 * step) // step)
    frequency = ROPE_BASE ** (-2.0 * turn.astype(F32) / HEAD_DIM)
    angles = lengths.astype(F32)[:, None] * frequency[None, :]
    plain = jnp.logical_and(~in_query, col_y * kv_cols >= KV_HEADS * HEAD_DIM)[None, :]
    cosine = jnp.where(plain, 1.0, jnp.cos(angles))
    sine = jnp.sin(angles)
    sine = jnp.where(plain, 0.0, jnp.where(second[None, :] == 1, sine, -sine))

    query_all = pl.pallas_call(
        functools.partial(rotate_kernel, row_count, size_x, step),
        grid_spec=pltpu.PrefetchScalarGridSpec(
            num_scalar_prefetch=1,
            grid=(1,),
            in_specs=[
                pl.BlockSpec((TENANTS, share), lambda tile, ref: (0, ref[row_count])),
                whole(cosine.shape),
                whole(sine.shape),
            ]
            + [whole(chunk_shape)] * size_x,
            out_specs=whole((devices, row_count, share + HEAD_DIM)),
        ),
        out_shape=jax.ShapeDtypeStruct((devices, row_count, share + HEAD_DIM), BF16),
        compiler_params=pltpu.CompilerParams(vmem_limit_bytes=8 * 2**20),
        name="rotate",
    )(scalars, q_magnitude, cosine, sine, *q_parts)
    gathered = lax.all_to_all(query_all, ("gx", "gy"), split_axis=0, concat_axis=0, tiled=True)

    slots = kv_cache.shape[0]
    owner_row, filled, used = slot_info(page_table, lengths, device, slots)
    info = jnp.concatenate([owner_row, filled, used[None], device[None]]).astype(jnp.int32)
    per_target = HEADS // devices
    send_shape = (devices, row_count * per_target + 2 * row_count, HEAD_DIM)
    sent = pl.pallas_call(
        functools.partial(attend_kernel, row_count, size_x, size_y),
        grid_spec=pltpu.PrefetchScalarGridSpec(
            num_scalar_prefetch=1,
            grid=(slots,),
            in_specs=[
                whole(gathered.shape),
                whole(kv_order[:kv_cols].shape),
                pl.BlockSpec(
                    (1,) + kv_cache.shape[1:],
                    lambda slot, ref: (
                        jnp.maximum(jnp.minimum(slot, ref[2 * slots] - 1), 0),
                        0,
                        0,
                        0,
                    ),
                ),
            ],
            out_specs=whole(send_shape),
            scratch_shapes=[
                pltpu.VMEM((row_count * HEADS, HEAD_DIM), F32),
                pltpu.VMEM((size_x, size_y * row_count, HEAD_DIM), F32),
                pltpu.VMEM((row_count * HEADS, HEAD_DIM), F32),
                pltpu.VMEM((row_count * HEADS, HEAD_DIM), F32),
                pltpu.VMEM((row_count * HEADS, HEAD_DIM), F32),
            ],
        ),
        out_shape=jax.ShapeDtypeStruct(send_shape, F32),
        compiler_params=pltpu.CompilerParams(vmem_limit_bytes=16 * 2**20),
        name="attend",
    )(info, gathered, kv_order[:kv_cols], kv_cache)
    parts = lax.all_to_all(sent, ("gx", "gy"), split_axis=0, concat_axis=0, tiled=True)

    merged = pl.pallas_call(
        functools.partial(merge_kernel, row_count, per_target),
        in_specs=[
            pl.BlockSpec(memory_space=pltpu.SMEM),
            pl.BlockSpec(memory_space=pltpu.VMEM),
        ],
        out_specs=pl.BlockSpec(memory_space=pltpu.VMEM),
        out_shape=jax.ShapeDtypeStruct((size_y, row_count, per_target * HEAD_DIM), BF16),
        compiler_params=pltpu.CompilerParams(vmem_limit_bytes=8 * 2**20),
        name="merge",
    )(device[None], parts)
    attended = lax.all_to_all(merged, "gy", split_axis=0, concat_axis=0, tiled=True)

    own = row_count // size_x
    o_parts = pl.pallas_call(
        functools.partial(output_kernel, row_count, size_x, tile_counts),
        in_specs=[smem, vmem, vmem, anywhere]
        + [vmem] * (2 * len(tile_counts))
        + [anywhere] * len(tile_counts),
        out_specs=[vmem] * size_x,
        scratch_shapes=[
            pltpu.VMEM((PAD_ROWS, in_rows), BF16),
            pltpu.VMEM((q_tiles, PAD_ROWS, COLS), F32),
            pltpu.VMEM((size_x, 2 * own, q_cols), F32),
            pltpu.VMEM((low_rank, in_rows), BF16),
            pltpu.VMEM((q_tiles, in_rows, COLS), BF16),
            pltpu.SemaphoreType.DMA((row_count,)),
            pltpu.SemaphoreType.DMA((q_tiles,)),
        ],
        out_shape=[jax.ShapeDtypeStruct((2 * own, q_cols), F32)] * size_x,
        compiler_params=pltpu.CompilerParams(vmem_limit_bytes=32 * 2**20),
        name="output",
    )(
        scalars,
        attended,
        join,
        o_down,
        *[part[0] for part in scale_parts],
        *[part[1] for part in scale_parts],
        *[part[2] for part in scale_parts],
    )
    o_parts = exchange(o_parts, "gx", size_x)
    return pl.pallas_call(
        functools.partial(finish_kernel, row_count, size_x),
        grid_spec=pltpu.PrefetchScalarGridSpec(
            num_scalar_prefetch=1,
            grid=(1,),
            in_specs=[
                pl.BlockSpec((row_count, q_cols), lambda tile, ref: (0, ref[row_count + 1])),
                whole(o_magnitude.shape),
            ]
            + [whole((2 * own, q_cols))] * size_x,
            out_specs=whole((own, q_cols)),
        ),
        out_shape=jax.ShapeDtypeStruct((own, q_cols), BF16),
        compiler_params=pltpu.CompilerParams(vmem_limit_bytes=4 * 2**20),
        name="finish",
    )(scalars, hidden, o_magnitude, *o_parts)


def solution(mesh):
    in_specs = (
        P(),
        P(),
        P("gx", "gy"),
        P("gx", "gy"),
        P("gx", "gy"),
        P("gx", "gy"),
        P("gx", "gy"),
        P("gx", "gy"),
        P(None, "gx", None),
        P(None, None, "gy"),
        P(None, "gy"),
        P(None, "gx", None),
        P(None, None, "gy"),
        P(None, "gy"),
        P(),
        P(),
        P(),
        P(("gx", "gy"), None, None, None),
    )
    out_specs = P("gx", "gy")
    return jax.shard_map(local, mesh=mesh, in_specs=in_specs, out_specs=out_specs, check_vma=False)
```

```python
import functools
import math

import jax
import jax.numpy as jnp
import numpy as np
from jax import lax
from jax.experimental import pallas as pl
from jax.experimental.pallas import tpu as pltpu
from jax.sharding import PartitionSpec as P

HEADS = 128
KV_HEADS = 8
HEAD_DIM = 128
TENANTS = 8
RANK = 16
QBLOCK = 64
PAGE = 256

NF4_LEVELS = (
    -1.0,
    -0.6961928009986877,
    -0.5250730514526367,
    -0.39491748809814453,
    -0.28444138169288635,
    -0.18477343022833234,
    -0.09105003625154495,
    0.0,
    0.07958029955625534,
    0.16093020141124725,
    0.24611230194568634,
    0.33791524171829224,
    0.44070982933044434,
    0.5626170039176941,
    0.7229568362236023,
    1.0,
)
NORM_EPS = 1e-05
NEG_FILL = -1e30
ROPE_BASE = 500000.0
WORDS = 128
COLS = 2 * WORDS
CHUNK = 2048
PAD_ROWS = 16
DEPTH = 3
F32 = jnp.float32
BF16 = jnp.bfloat16
GATHER_ROWS = lax.GatherDimensionNumbers(
    offset_dims=(),
    collapsed_slice_dims=(0,),
    start_index_map=(0,),
    operand_batching_dims=(1,),
    start_indices_batching_dims=(1,),
)


def level_table():
    return np.broadcast_to(np.asarray(NF4_LEVELS, np.float32)[:, None], (16, WORDS)).copy()


def split_columns():
    matrix = np.zeros((COLS, COLS), np.float32)
    for column in range(COLS):
        matrix[column, column // 2 + WORDS * (column % 2)] = 1.0
    return matrix


def keyval_order(kv_columns, size_x):
    step = HEAD_DIM // 2 // size_x
    matrix = np.zeros((COLS, size_x * HEAD_DIM), np.float32)
    for column in range(kv_columns):
        head, inner = divmod(column, HEAD_DIM)
        half, turn = divmod(inner, HEAD_DIM // 2)
        piece, spot = divmod(turn, step)
        place = piece * HEAD_DIM + head * 2 * step + half * step + spot
        matrix[column, place] = 1.0
    return matrix


def dot(left, right):
    return jnp.dot(left, right, preferred_element_type=F32)


def dot_rows(left, right):
    return lax.dot_general(left, right, (((1,), (1,)), ((), ())), preferred_element_type=F32)


def three_parts(values):
    first = values.astype(BF16)
    rest = values - first.astype(F32)
    second = rest.astype(BF16)
    third = (rest - second.astype(F32)).astype(BF16)
    return first, second, third


def wide_dot(left, right):
    rows = left.shape[0]
    both = dot(jnp.concatenate(three_parts(left), 0), right)
    return (both[:rows] + both[rows : 2 * rows]) + both[2 * rows :]


def split_scales(absmax_ref, split_ref, scale_ref, first, tiles):
    rows = absmax_ref.shape[0]
    stacked = jnp.concatenate(
        [absmax_ref[:, COLS * tile : COLS * (tile + 1)] for tile in range(tiles)], 0
    )
    both = wide_dot(stacked, split_ref[...])
    for tile in range(tiles):
        scale_ref[first + tile] = both[rows * tile : rows * (tile + 1)]


def stack_tiles(array):
    return jnp.concatenate(
        [array[:, COLS * tile : COLS * (tile + 1)] for tile in range(array.shape[1] // COLS)], 0
    )


def pick_rows(table, index):
    return lax.gather(
        table,
        index[..., None],
        GATHER_ROWS,
        slice_sizes=(1, 1),
        mode=lax.GatherScatterMode.PROMISE_IN_BOUNDS,
    )


def weight_tile(codes_ref, scale_ref, level_ref, left_ref, store_ref, squared=True):
    in_rows = codes_ref.shape[0]
    chunk = min(CHUNK, in_rows)
    blocks = chunk // QBLOCK

    def visit(step, carry):
        total, squares = carry
        even_list = []
        odd_list = []
        for block in range(blocks):
            scale_row = scale_ref[pl.ds(step * blocks + block, 1), :]
            tables = [
                level_ref[8 * half : 8 * half + 8, :]
                * scale_row[:, WORDS * side : WORDS * side + WORDS]
                for side in range(2)
                for half in range(2)
            ]
            for row in range(0, QBLOCK, 8):
                word = codes_ref[pl.ds(step * chunk + block * QBLOCK + row, 8), :]
                low = word & 7
                even = jnp.where(
                    (word & 8) != 0, pick_rows(tables[1], low), pick_rows(tables[0], low)
                )
                high = lax.shift_right_logical(word, 4) & 7
                odd = jnp.where(
                    word >= 128, pick_rows(tables[3], high), pick_rows(tables[2], high)
                )
                even_list.append(even)
                odd_list.append(odd)
        weight = jnp.concatenate(
            [jnp.concatenate(even_list, 0), jnp.concatenate(odd_list, 0)], 1
        ).astype(BF16)
        start = pl.multiple_of(step * chunk, chunk)
        if store_ref is not None:
            store_ref[pl.ds(start, chunk), :] = weight
        total = total + dot(left_ref[:, pl.ds(start, chunk)], weight)
        if squared:
            squares = squares + dot(jnp.ones((PAD_ROWS, chunk), BF16), weight * weight)
        return (total, squares)

    return lax.fori_loop(
        0,
        in_rows // chunk,
        visit,
        (jnp.zeros((left_ref.shape[0], COLS), F32), jnp.zeros((PAD_ROWS, COLS), F32)),
    )


def block_mask(rows, columns, lead):
    row_id = lax.broadcasted_iota(jnp.int32, (rows, columns), 0)
    column_id = lax.broadcasted_iota(jnp.int32, (rows, columns), 1)
    owner = jnp.where(row_id < lead, row_id, lax.shift_right_logical(row_id - lead, 4))
    return owner == lax.shift_right_logical(column_id, 4)


def norm_terms(cross, gram, up_split, squares, row_count):
    inner = up_split * (2.0 * cross + gram)
    return squares + jnp.sum(
        inner.reshape(row_count, RANK, COLS), axis=1
    )


def code_copy(codes_ref, first, tile, buffer_ref, sems):
    columns = pl.ds(pl.multiple_of((first + tile) * WORDS, WORDS), WORDS)
    slot = tile % DEPTH if isinstance(tile, int) else lax.rem(tile, DEPTH)
    return pltpu.make_async_copy(codes_ref.at[:, columns], buffer_ref.at[slot], sems.at[slot])


def code_tile(codes_ref, first, tile, tiles, buffer_ref, sems):
    @pl.when(tile + DEPTH - 1 < tiles)
    def _():
        code_copy(codes_ref, first, tile + DEPTH - 1, buffer_ref, sems).start()

    code_copy(codes_ref, first, tile, buffer_ref, sems).wait()
    return buffer_ref.at[lax.rem(tile, DEPTH)]


def tenant_copies(scalar_ref, row_count, down_ref, up_ref, left_ref, lead, ups_ref, sems):
    downs = []
    ups = []
    for row in range(row_count):
        tenant = scalar_ref[row]
        downs.append(
            pltpu.make_async_copy(
                down_ref.at[tenant],
                left_ref.at[lead + RANK * row : lead + RANK * (row + 1), :],
                sems.at[row],
            )
        )
        ups.append(
            pltpu.make_async_copy(
                up_ref.at[tenant],
                ups_ref.at[RANK * row : RANK * (row + 1), :],
                sems.at[row_count + row],
            )
        )
    return downs, ups


def query_kernel(
    row_count,
    size_x,
    scalar_ref,
    hidden_ref,
    gain_ref,
    absmax_ref,
    kv_absmax_ref,
    level_ref,
    split_ref,
    join_ref,
    kv_join_ref,
    codes_ref,
    kv_codes_ref,
    down_ref,
    up_ref,
    *refs,
):
    outs = refs[:size_x]
    (
        left_ref,
        scale_ref,
        total_ref,
        square_ref,
        chunk_ref,
        buffer_ref,
        kv_buffer_ref,
        ups_ref,
        code_sems,
        kv_sem,
        tenant_sems,
    ) = refs[size_x:]
    tiles = absmax_ref.shape[1] // COLS
    share = chunk_ref.shape[2] - HEAD_DIM
    low_rank = row_count * RANK
    here = lax.axis_index("gx")
    downs, ups = tenant_copies(
        scalar_ref, row_count, down_ref, up_ref, left_ref, PAD_ROWS, ups_ref, tenant_sems
    )
    kv_copy = pltpu.make_async_copy(kv_codes_ref, kv_buffer_ref, kv_sem.at[0])
    kv_copy.start()
    for copy in downs:
        copy.start()
    for tile in range(min(DEPTH - 1, tiles)):
        code_copy(codes_ref, 0, tile, buffer_ref, code_sems).start()
    for copy in ups:
        copy.start()

    states = hidden_ref[...].astype(F32)
    mean_square = jnp.mean(states * states, axis=1, keepdims=True)
    in_rows = left_ref.shape[1]
    own = pl.ds(pl.multiple_of(here * in_rows, in_rows), in_rows)
    normed = hidden_ref[:, own].astype(F32) * lax.rsqrt(mean_square + NORM_EPS) * gain_ref[:, own]
    left_ref[0:PAD_ROWS, :] = jnp.concatenate(
        [normed, jnp.zeros((PAD_ROWS - row_count, normed.shape[1]), F32)], 0
    ).astype(BF16)
    split_scales(kv_absmax_ref, split_ref, scale_ref, 0, 1)
    split_scales(absmax_ref, split_ref, scale_ref, 1, tiles)
    kv_copy.wait()
    total, _ = weight_tile(
        kv_buffer_ref, scale_ref.at[0], level_ref, left_ref.at[0:PAD_ROWS, :], None, False
    )
    joined = wide_dot(total, kv_join_ref[...])
    for owner in range(size_x):
        chunk_ref[owner, :, share:] = joined[
            : 2 * row_count, owner * HEAD_DIM : (owner + 1) * HEAD_DIM
        ]
    for copy in downs:
        copy.wait()

    def visit(tile, carry):
        codes = code_tile(codes_ref, 0, tile, tiles, buffer_ref, code_sems)
        total, squares = weight_tile(
            codes, scale_ref.at[tile + 1], level_ref, left_ref, None
        )
        total_ref[tile] = total
        square_ref[tile] = squares[0:8]
        return carry

    lax.fori_loop(0, tiles, visit, 0)
    for copy in ups:
        copy.wait()
    gram = dot_rows(left_ref[...], left_ref[PAD_ROWS:, :])
    gram = jnp.where(block_mask(*gram.shape, PAD_ROWS), gram, 0.0)
    up_split = dot(stack_tiles(ups_ref[...]), split_ref[...])
    lines = []
    for tile in range(tiles):
        up_tile = up_split[low_rank * tile : low_rank * (tile + 1)]
        extra = wide_dot(gram, up_tile.astype(BF16))
        total = total_ref[tile]
        lines.append(total[:row_count] + extra[:row_count])
        lines.append(
            norm_terms(total[PAD_ROWS:], extra[PAD_ROWS:], up_tile, square_ref[tile, 0:1], row_count)
        )
    joined = wide_dot(jnp.concatenate(lines, 0), join_ref[...])
    piece = min(COLS, share)
    for tile in range(tiles):
        for part in range(COLS // piece):
            owner, place = divmod(tile * COLS + part * piece, share)
            chunk_ref[owner, :, place : place + piece] = joined[
                2 * row_count * tile : 2 * row_count * (tile + 1),
                part * piece : (part + 1) * piece,
            ]
    for shift in range(size_x):
        outs[shift][...] = chunk_ref[lax.rem(here + shift, size_x)]


def store_copy(store_ref, slot, weight_ref, tile, sems):
    return pltpu.make_async_copy(store_ref.at[slot], weight_ref.at[tile], sems.at[slot])


def output_scale_kernel(
    row_count,
    first,
    scalar_ref,
    absmax_ref,
    level_ref,
    split_ref,
    join_ref,
    codes_ref,
    down_ref,
    up_ref,
    norm_ref,
    up_split_ref,
    weight_ref,
    store_ref,
    left_ref,
    scale_ref,
    total_ref,
    square_ref,
    buffer_ref,
    ups_ref,
    code_sems,
    tenant_sems,
    store_sems,
):
    tiles = weight_ref.shape[0]
    low_rank = row_count * RANK
    downs, ups = tenant_copies(
        scalar_ref,
        row_count,
        down_ref,
        up_ref.at[:, :, first * COLS : (first + tiles) * COLS],
        left_ref,
        0,
        ups_ref,
        tenant_sems,
    )
    for copy in downs:
        copy.start()
    for tile in range(min(DEPTH - 1, tiles)):
        code_copy(codes_ref, first, tile, buffer_ref, code_sems).start()
    for copy in ups:
        copy.start()
    split_scales(absmax_ref, split_ref, scale_ref, 0, tiles)
    for copy in downs:
        copy.wait()

    def visit(tile, carry):
        codes = code_tile(codes_ref, first, tile, tiles, buffer_ref, code_sems)
        slot = lax.rem(tile, 2)

        @pl.when(tile >= 2)
        def _():
            store_copy(store_ref, slot, weight_ref, tile - 2, store_sems).wait()

        total, squares = weight_tile(
            codes, scale_ref.at[tile], level_ref, left_ref, store_ref.at[slot]
        )
        store_copy(store_ref, slot, weight_ref, tile, store_sems).start()
        total_ref[tile] = total
        square_ref[tile] = squares[0:8]
        return carry

    lax.fori_loop(0, tiles, visit, 0)
    for copy in ups:
        copy.wait()
    gram = dot_rows(left_ref[...], left_ref[...])
    gram = jnp.where(block_mask(*gram.shape, 0), gram, 0.0)
    up_split = dot(stack_tiles(ups_ref[...]), split_ref[...])
    lines = []
    for tile in range(tiles):
        up_tile = up_split[low_rank * tile : low_rank * (tile + 1)]
        narrow = up_tile.astype(BF16)
        up_split_ref[:, COLS * tile : COLS * (tile + 1)] = narrow
        extra = wide_dot(gram, narrow)
        lines.append(norm_terms(total_ref[tile], extra, up_tile, square_ref[tile, 0:1], row_count))
    joined = wide_dot(jnp.concatenate(lines, 0), join_ref[...])
    for tile in range(tiles):
        norm_ref[:, COLS * tile : COLS * (tile + 1)] = joined[
            row_count * tile : row_count * (tile + 1)
        ]
    for tile in range(max(tiles - 2, 0), tiles):
        store_copy(store_ref, tile % 2, weight_ref, tile, store_sems).wait()


def rotate_kernel(row_count, size_x, step, scalar_ref, magnitude_ref, cos_ref, sin_ref, *refs):
    parts = refs[:size_x]
    out_ref = refs[size_x]
    share = cos_ref.shape[1] - HEAD_DIM
    total = parts[0][...]
    for part in parts[1:]:
        total = total + part[...]
    magnitude = jnp.concatenate(
        [
            magnitude_ref[pl.ds(scalar_ref[row], 1), :]
            for row in range(row_count)
        ],
        0,
    )
    query = total[:row_count, :share] * (
        magnitude * lax.rsqrt(total[row_count:, :share])
    )
    keyval = total[:row_count, share:]
    half = HEAD_DIM // 2
    pieces = []
    for head in range(share // HEAD_DIM):
        block = query[:, head * HEAD_DIM : (head + 1) * HEAD_DIM]
        pieces.append(pltpu.roll(block, half, 1))
    lane = lax.broadcasted_iota(jnp.int32, keyval.shape, 1)
    other = jnp.where(
        (lane & step) != 0, pltpu.roll(keyval, step, 1), pltpu.roll(keyval, HEAD_DIM - step, 1)
    )
    values = jnp.concatenate([query, keyval], 1)
    partner = jnp.concatenate(pieces + [other], 1)
    turned = (values * cos_ref[...] + partner * sin_ref[...]).astype(BF16)
    for target in range(out_ref.shape[0]):
        out_ref[target] = turned


def attend_kernel(
    row_count,
    size_x,
    size_y,
    info_ref,
    gathered_ref,
    kv_order_ref,
    pages_ref,
    send_ref,
    query_ref,
    mixed_ref,
    best_ref,
    total_ref,
    value_ref,
    held_ref,
    page_sems,
):
    slots = pages_ref.shape[0]
    devices = size_x * size_y
    per_target = HEADS // devices
    group = HEADS // KV_HEADS
    inv_root = 1.0 / math.sqrt(HEAD_DIM)
    used = info_ref[2 * slots]
    device = info_ref[2 * slots + 1]
    share = gathered_ref.shape[2] - HEAD_DIM

    def page_copy(slot):
        return pltpu.make_async_copy(pages_ref.at[slot], held_ref.at[slot], page_sems.at[slot])

    for slot in range(min(DEPTH, slots)):

        @pl.when(slot < used)
        def _(slot=slot):
            page_copy(slot).start()

    def setup():
        heads_here = share // HEAD_DIM
        for place_x in range(size_x):
            for place_y in range(size_y):
                block = gathered_ref[place_x * size_y + place_y].astype(F32)
                for head in range(heads_here):
                    first = (place_y * size_x + place_x) * heads_here + head
                    query_ref[pl.ds(first, row_count, stride=HEADS), :] = block[
                        :, head * HEAD_DIM : (head + 1) * HEAD_DIM
                    ]
                mixed_ref[place_x, place_y * row_count : (place_y + 1) * row_count, :] = block[
                    :, share:
                ]
        best_ref[...] = jnp.full(best_ref.shape, NEG_FILL, F32)
        total_ref[...] = jnp.zeros(total_ref.shape, F32)
        value_ref[...] = jnp.zeros(value_ref.shape, F32)

        @pl.when(device < row_count)
        def _():
            columns = kv_order_ref.shape[0]
            plain = jnp.zeros((size_y * row_count, columns), F32)
            for place_x in range(size_x):
                plain = plain + dot_rows(
                    mixed_ref[place_x].astype(BF16),
                    kv_order_ref[:, place_x * HEAD_DIM : (place_x + 1) * HEAD_DIM],
                )
            heads_each = 2 * KV_HEADS // size_y
            for row in range(row_count):

                @pl.when(device == row)
                def _():
                    rows = []
                    for head in range(2 * KV_HEADS):
                        place_y, inner = divmod(head, heads_each)
                        line = place_y * row_count + row
                        one = plain[line : line + 1, inner * HEAD_DIM : (inner + 1) * HEAD_DIM]
                        rows.append(jnp.broadcast_to(one, (group, HEAD_DIM)))
                    new_keys = jnp.concatenate(rows[:KV_HEADS], 0)
                    new_values = jnp.concatenate(rows[KV_HEADS:], 0)
                    span = slice(row * HEADS, (row + 1) * HEADS)
                    score = jnp.sum(query_ref[span, :] * new_keys, 1, keepdims=True) * inv_root
                    best_ref[span, :] = jnp.broadcast_to(score, (HEADS, HEAD_DIM))
                    total_ref[span, :] = jnp.ones((HEADS, HEAD_DIM), F32)
                    value_ref[span, :] = new_values

    setup()

    def visit(slot, carry):
        @pl.when(slot + DEPTH < used)
        def _():
            page_copy(slot + DEPTH).start()

        page_copy(slot).wait()
        start = pl.multiple_of(info_ref[slot] * HEADS, HEADS)
        count = info_ref[slots + slot]
        span = pl.ds(start, HEADS)
        query = query_ref[span, :].astype(BF16)
        scores = jnp.concatenate(
            [
                dot_rows(
                    query[group * head : group * (head + 1), :],
                    held_ref[slot, 0, :, head * HEAD_DIM : (head + 1) * HEAD_DIM],
                )
                for head in range(KV_HEADS)
            ],
            0,
        )
        inside = lax.broadcasted_iota(jnp.int32, (HEADS, PAGE), 1) < count
        scores = jnp.where(inside, scores * inv_root, NEG_FILL)
        old_best = best_ref[span, :]
        best = jnp.maximum(old_best, jnp.max(scores, axis=1, keepdims=True))
        weights = jnp.where(inside, jnp.exp(scores - best[:, :1]), 0.0)
        keep = jnp.exp(old_best - best)
        best_ref[span, :] = best
        total_ref[span, :] = total_ref[span, :] * keep + jnp.sum(weights, axis=1, keepdims=True)
        coarse = weights.astype(BF16)
        fine = (weights - coarse.astype(F32)).astype(BF16)
        gains = []
        for head in range(KV_HEADS):
            rows = slice(group * head, group * (head + 1))
            both = dot(
                jnp.concatenate([coarse[rows], fine[rows]], 0),
                held_ref[slot, 1, :, head * HEAD_DIM : (head + 1) * HEAD_DIM],
            )
            gains.append(both[:group] + both[group:])
        value_ref[span, :] = value_ref[span, :] * keep + jnp.concatenate(gains, 0)
        return carry

    lax.fori_loop(0, used, visit, 0)

    def close():
        eye = lax.broadcasted_iota(jnp.int32, (HEADS, HEAD_DIM), 0) == lax.broadcasted_iota(
            jnp.int32, (HEADS, HEAD_DIM), 1
        )
        lines = []
        for source in (best_ref, total_ref):
            for row in range(row_count):
                block = source[row * HEADS : (row + 1) * HEADS, :]
                lines.append(jnp.sum(jnp.where(eye, block, 0.0), axis=0, keepdims=True))
        scalars = jnp.concatenate(lines, 0)
        for target in range(devices):
            for row in range(row_count):
                begin = row * HEADS + target * per_target
                send_ref[target, row * per_target : (row + 1) * per_target, :] = value_ref[
                    begin : begin + per_target, :
                ]
            send_ref[target, row_count * per_target :, :] = scalars

    close()


def merge_kernel(row_count, per_target, info_ref, parts_ref, out_ref):
    offset = info_ref[0] * per_target
    values = parts_ref[:, : row_count * per_target, :]
    scalars = parts_ref[:, row_count * per_target :, :]
    lane = lax.broadcasted_iota(jnp.int32, scalars.shape, 2)
    for row in range(row_count):
        for head in range(per_target):
            chosen = jnp.sum(jnp.where(lane == offset + head, scalars, 0.0), axis=2, keepdims=True)
            best = chosen[:, row : row + 1, :]
            total = chosen[:, row_count + row : row_count + row + 1, :]
            factor = jnp.exp(best - jnp.max(best, axis=0, keepdims=True))
            line = row * per_target + head
            top = jnp.sum(values[:, line : line + 1, :] * factor, axis=0)
            bottom = jnp.sum(total * factor, axis=0)
            ratio = (top / bottom).astype(BF16)
            for target in range(out_ref.shape[0]):
                out_ref[target, row : row + 1, head * HEAD_DIM : (head + 1) * HEAD_DIM] = ratio


def output_kernel(row_count, size_x, tile_counts, scalar_ref, attended_ref, join_ref, down_ref, *refs):
    parts = len(tile_counts)
    norms = refs[:parts]
    ups = refs[parts : 2 * parts]
    weights = refs[2 * parts : 3 * parts]
    outs = refs[3 * parts : 3 * parts + size_x]
    left_ref, total_ref, chunk_ref, low_ref, held_ref, sems, held_sems = refs[3 * parts + size_x :]
    tiles = sum(tile_counts)
    own = row_count // size_x
    copies = [
        pltpu.make_async_copy(
            down_ref.at[scalar_ref[row]],
            low_ref.at[RANK * row : RANK * (row + 1), :],
            sems.at[row],
        )
        for row in range(row_count)
    ]
    first = 0
    for part in range(parts):
        for tile in range(tile_counts[part]):
            pltpu.make_async_copy(
                weights[part].at[tile], held_ref.at[first + tile], held_sems.at[first + tile]
            ).start()
        first += tile_counts[part]
    for copy in copies:
        copy.start()
    width = attended_ref.shape[2]
    for part in range(attended_ref.shape[0]):
        block = attended_ref[part].astype(F32)
        left_ref[:, part * width : (part + 1) * width] = jnp.concatenate(
            [block, jnp.zeros((PAD_ROWS - row_count, width), F32)], 0
        ).astype(BF16)
    first = 0
    for part in range(parts):

        def visit(tile, carry, part=part, first=first):
            pltpu.make_async_copy(
                weights[part].at[tile], held_ref.at[first + tile], held_sems.at[first + tile]
            ).wait()
            total_ref[first + tile] = dot(left_ref[...], held_ref[first + tile])
            return carry

        lax.fori_loop(0, tile_counts[part], visit, 0)
        first += tile_counts[part]
    for copy in copies:
        copy.wait()
    middle = dot_rows(left_ref[...], low_ref[...])
    middle = jnp.where(block_mask(*middle.shape, PAD_ROWS), middle, 0.0)
    lines = []
    spot = 0
    for part in range(parts):
        extra = wide_dot(middle, ups[part][...])
        for tile in range(tile_counts[part]):
            lines.append(
                total_ref[spot, 0:row_count] + extra[:row_count, COLS * tile : COLS * (tile + 1)]
            )
            spot += 1
    joined = wide_dot(jnp.concatenate(lines, 0), join_ref[...])
    for owner in range(size_x):
        for spot in range(tiles):
            begin = row_count * spot + owner * own
            chunk_ref[owner, 0:own, COLS * spot : COLS * (spot + 1)] = joined[begin : begin + own]
        begin = 0
        for part in range(parts):
            columns = COLS * tile_counts[part]
            chunk_ref[owner, own : 2 * own, begin : begin + columns] = norms[part][
                owner * own : (owner + 1) * own, :
            ]
            begin += columns
    here = lax.axis_index("gx")
    for shift in range(size_x):
        outs[shift][...] = chunk_ref[lax.rem(here + shift, size_x)]


def finish_kernel(row_count, size_x, scalar_ref, hidden_ref, magnitude_ref, *refs):
    parts = refs[:size_x]
    out_ref = refs[size_x]
    own = row_count // size_x
    total = parts[0][...]
    for part in parts[1:]:
        total = total + part[...]
    here = lax.axis_index("gx")
    states = hidden_ref[...].astype(F32)
    row_id = lax.broadcasted_iota(jnp.int32, states.shape, 0)
    for line in range(own):
        row = here * own + line
        state = jnp.sum(jnp.where(row_id == row, states, 0.0), axis=0, keepdims=True)
        magnitude = magnitude_ref[pl.ds(scalar_ref[row], 1), :]
        scale = magnitude * lax.rsqrt(total[own + line : own + line + 1])
        out_ref[line : line + 1, :] = (state + total[line : line + 1] * scale).astype(BF16)


def slot_info(page_table, lengths, device, slot_count):
    row_count, page_limit = page_table.shape
    page_need = (lengths + PAGE - 1) // PAGE
    page_numbers = jnp.arange(page_limit, dtype=jnp.int32)
    live_mask = page_numbers[None, :] < page_need[:, None]
    wanted = device * slot_count + jnp.arange(slot_count, dtype=jnp.int32)
    hits = ((page_table[None, :, :] == wanted[:, None, None]) & live_mask[None, :, :]).astype(
        jnp.int32
    )
    owner_row = jnp.sum(hits * jnp.arange(row_count, dtype=jnp.int32)[None, :, None], axis=(1, 2))
    remaining = jnp.clip(lengths[:, None] - page_numbers[None, :] * PAGE, 0, PAGE)
    filled = jnp.sum(hits * remaining[None, :, :], axis=(1, 2))
    return owner_row, filled, jnp.sum(hits)


def exchange(parts, axis, size):
    received = [parts[0]]
    for shift in range(1, size):
        received.append(
            lax.ppermute(parts[shift], axis, [(spot, (spot + shift) % size) for spot in range(size)])
        )
    return received


def whole(shape):
    return pl.BlockSpec(shape, lambda *_: (0,) * len(shape))


def local(
    hidden,
    norm_gain,
    q_codes,
    q_absmax,
    kv_codes,
    kv_absmax,
    o_codes,
    o_absmax,
    q_down,
    q_up,
    q_magnitude,
    o_down,
    o_up,
    o_magnitude,
    tenant,
    lengths,
    page_table,
    kv_cache,
):
    row_count, width = hidden.shape
    row_x = lax.axis_index("gx").astype(jnp.int32)
    col_y = lax.axis_index("gy").astype(jnp.int32)
    size_x = lax.axis_size("gx")
    size_y = lax.axis_size("gy")
    devices = size_x * size_y
    device = row_x * size_y + col_y
    in_rows, q_words = q_codes.shape
    q_cols = 2 * q_words
    share = q_cols // size_x
    kv_cols = 2 * kv_codes.shape[1]
    if kv_cols < COLS:
        kv_codes = jnp.pad(kv_codes, ((0, 0), (0, WORDS - kv_codes.shape[1])))
        kv_absmax = jnp.pad(kv_absmax, ((0, 0), (0, COLS - kv_cols)))
    low_rank = row_count * RANK
    level = jnp.asarray(level_table())
    split_matrix = split_columns()
    split = jnp.asarray(split_matrix, BF16)
    join = jnp.asarray(split_matrix.T, BF16)
    order = keyval_order(kv_cols, size_x)
    kv_join = jnp.asarray(split_matrix.T @ order, BF16)
    kv_order = jnp.asarray(order, BF16)
    scalars = tenant
    q_down = jnp.swapaxes(q_down, 1, 2)
    o_down = jnp.swapaxes(o_down, 1, 2)
    q_tiles = q_words // WORDS
    scale_rows = in_rows // QBLOCK

    smem = pl.BlockSpec(memory_space=pltpu.SMEM)
    vmem = pl.BlockSpec(memory_space=pltpu.VMEM)
    anywhere = pl.BlockSpec(memory_space=pltpu.HBM)
    chunk_shape = (2 * row_count, share + HEAD_DIM)
    q_parts = pl.pallas_call(
        functools.partial(query_kernel, row_count, size_x),
        in_specs=[smem] + [vmem] * 8 + [anywhere] * 4,
        out_specs=[vmem] * size_x,
        scratch_shapes=[
            pltpu.VMEM((PAD_ROWS + low_rank, in_rows), BF16),
            pltpu.VMEM((q_tiles + 1, scale_rows, COLS), F32),
            pltpu.VMEM((q_tiles, PAD_ROWS + low_rank, COLS), F32),
            pltpu.VMEM((q_tiles, 8, COLS), F32),
            pltpu.VMEM((size_x,) + chunk_shape, F32),
            pltpu.VMEM((DEPTH, in_rows, WORDS), jnp.int32),
            pltpu.VMEM((in_rows, WORDS), jnp.int32),
            pltpu.VMEM((low_rank, q_cols), BF16),
            pltpu.SemaphoreType.DMA((DEPTH,)),
            pltpu.SemaphoreType.DMA((1,)),
            pltpu.SemaphoreType.DMA((2 * row_count,)),
        ],
        out_shape=[jax.ShapeDtypeStruct(chunk_shape, F32)] * size_x,
        name="query",
    )(
        scalars,
        hidden,
        norm_gain[None, :],
        q_absmax,
        kv_absmax,
        level,
        split,
        join,
        kv_join,
        q_codes,
        kv_codes,
        q_down,
        q_up,
    )
    q_parts = exchange(q_parts, "gx", size_x)

    def output_scales(first, tiles, after):
        absmax, _ = lax.optimization_barrier((o_absmax, after))
        return pl.pallas_call(
            functools.partial(output_scale_kernel, row_count, first),
            in_specs=[smem] + [vmem] * 4 + [anywhere] * 3,
            out_specs=[vmem, vmem, anywhere],
            scratch_shapes=[
                pltpu.VMEM((2, in_rows, COLS), BF16),
                pltpu.VMEM((low_rank, in_rows), BF16),
                pltpu.VMEM((tiles, scale_rows, COLS), F32),
                pltpu.VMEM((tiles, low_rank, COLS), F32),
                pltpu.VMEM((tiles, 8, COLS), F32),
                pltpu.VMEM((DEPTH, in_rows, WORDS), jnp.int32),
                pltpu.VMEM((low_rank, tiles * COLS), BF16),
                pltpu.SemaphoreType.DMA((DEPTH,)),
                pltpu.SemaphoreType.DMA((2 * row_count,)),
                pltpu.SemaphoreType.DMA((2,)),
            ],
            out_shape=[
                jax.ShapeDtypeStruct((row_count, tiles * COLS), F32),
                jax.ShapeDtypeStruct((low_rank, tiles * COLS), BF16),
                pltpu.HBM((tiles, in_rows, COLS), BF16),
            ],
            cost_estimate=pl.CostEstimate(
                flops=tiles * 5_000_000 * 256,
                bytes_accessed=tiles * 8 * in_rows * WORDS,
                transcendentals=0,
            ),
            compiler_params=pltpu.CompilerParams(vmem_limit_bytes=56 * 2**20),
            name="output_scale",
        )(
            scalars,
            lax.slice_in_dim(absmax, first * COLS, (first + tiles) * COLS, axis=1),
            level,
            split,
            join,
            o_codes,
            o_down,
            o_up,
        )

    tile_counts = [q_tiles // 2, q_tiles - q_tiles // 2]

    half = HEAD_DIM // 2
    step = half // size_x
    lane = jnp.arange(share + HEAD_DIM, dtype=jnp.int32)
    in_query = lane < share
    turn = jnp.where(in_query, lane % half, row_x * step + lane % step)
    second = jnp.where(in_query, lane % HEAD_DIM // half, lane % (2 * step) // step)
    frequency = ROPE_BASE ** (-2.0 * turn.astype(F32) / HEAD_DIM)
    angles = lengths.astype(F32)[:, None] * frequency[None, :]
    plain = jnp.logical_and(~in_query, col_y * kv_cols >= KV_HEADS * HEAD_DIM)[None, :]
    cosine = jnp.where(plain, 1.0, jnp.cos(angles))
    sine = jnp.sin(angles)
    sine = jnp.where(plain, 0.0, jnp.where(second[None, :] == 1, sine, -sine))

    query_all = pl.pallas_call(
        functools.partial(rotate_kernel, row_count, size_x, step),
        grid_spec=pltpu.PrefetchScalarGridSpec(
            num_scalar_prefetch=1,
            grid=(1,),
            in_specs=[
                pl.BlockSpec((TENANTS, share), lambda tile, ref: (0, lax.axis_index("gx"))),
                whole(cosine.shape),
                whole(sine.shape),
            ]
            + [whole(chunk_shape)] * size_x,
            out_specs=whole((devices, row_count, share + HEAD_DIM)),
        ),
        out_shape=jax.ShapeDtypeStruct((devices, row_count, share + HEAD_DIM), BF16),
        compiler_params=pltpu.CompilerParams(vmem_limit_bytes=8 * 2**20),
        name="rotate",
    )(scalars, q_magnitude, cosine, sine, *q_parts)
    gathered = lax.all_to_all(query_all, ("gx", "gy"), split_axis=0, concat_axis=0, tiled=True)
    scale_parts = [output_scales(0, tile_counts[0], query_all)]
    gathered, scale_parts[0] = lax.optimization_barrier((gathered, scale_parts[0]))

    slots = kv_cache.shape[0]
    owner_row, filled, used = slot_info(page_table, lengths, device, slots)
    info = jnp.concatenate([owner_row, filled, used[None], device[None]]).astype(jnp.int32)
    per_target = HEADS // devices
    send_shape = (devices, row_count * per_target + 2 * row_count, HEAD_DIM)
    sent = pl.pallas_call(
        functools.partial(attend_kernel, row_count, size_x, size_y),
        in_specs=[smem, vmem, vmem, anywhere],
        out_specs=vmem,
        scratch_shapes=[
            pltpu.VMEM((row_count * HEADS, HEAD_DIM), F32),
            pltpu.VMEM((size_x, size_y * row_count, HEAD_DIM), F32),
            pltpu.VMEM((row_count * HEADS, HEAD_DIM), F32),
            pltpu.VMEM((row_count * HEADS, HEAD_DIM), F32),
            pltpu.VMEM((row_count * HEADS, HEAD_DIM), F32),
            pltpu.VMEM(kv_cache.shape, BF16),
            pltpu.SemaphoreType.DMA((slots,)),
        ],
        out_shape=jax.ShapeDtypeStruct(send_shape, F32),
        compiler_params=pltpu.CompilerParams(vmem_limit_bytes=58 * 2**20),
        name="attend",
    )(info, gathered, kv_order[:kv_cols], kv_cache)
    parts = lax.all_to_all(sent, ("gx", "gy"), split_axis=0, concat_axis=0, tiled=True)
    scale_parts.append(output_scales(tile_counts[0], tile_counts[1], sent))
    parts, scale_parts[1] = lax.optimization_barrier((parts, scale_parts[1]))

    merged = pl.pallas_call(
        functools.partial(merge_kernel, row_count, per_target),
        in_specs=[
            pl.BlockSpec(memory_space=pltpu.SMEM),
            pl.BlockSpec(memory_space=pltpu.VMEM),
        ],
        out_specs=pl.BlockSpec(memory_space=pltpu.VMEM),
        out_shape=jax.ShapeDtypeStruct((size_y, row_count, per_target * HEAD_DIM), BF16),
        compiler_params=pltpu.CompilerParams(vmem_limit_bytes=8 * 2**20),
        name="merge",
    )(device[None], parts)
    attended = lax.all_to_all(merged, "gy", split_axis=0, concat_axis=0, tiled=True)

    own = row_count // size_x
    o_parts = pl.pallas_call(
        functools.partial(output_kernel, row_count, size_x, tile_counts),
        in_specs=[smem, vmem, vmem, anywhere]
        + [vmem] * (2 * len(tile_counts))
        + [anywhere] * len(tile_counts),
        out_specs=[vmem] * size_x,
        scratch_shapes=[
            pltpu.VMEM((PAD_ROWS, in_rows), BF16),
            pltpu.VMEM((q_tiles, PAD_ROWS, COLS), F32),
            pltpu.VMEM((size_x, 2 * own, q_cols), F32),
            pltpu.VMEM((low_rank, in_rows), BF16),
            pltpu.VMEM((q_tiles, in_rows, COLS), BF16),
            pltpu.SemaphoreType.DMA((row_count,)),
            pltpu.SemaphoreType.DMA((q_tiles,)),
        ],
        out_shape=[jax.ShapeDtypeStruct((2 * own, q_cols), F32)] * size_x,
        compiler_params=pltpu.CompilerParams(vmem_limit_bytes=56 * 2**20),
        name="output",
    )(
        scalars,
        attended,
        join,
        o_down,
        *[part[0] for part in scale_parts],
        *[part[1] for part in scale_parts],
        *[part[2] for part in scale_parts],
    )
    o_parts = exchange(o_parts, "gx", size_x)
    return pl.pallas_call(
        functools.partial(finish_kernel, row_count, size_x),
        grid_spec=pltpu.PrefetchScalarGridSpec(
            num_scalar_prefetch=1,
            grid=(1,),
            in_specs=[
                pl.BlockSpec((row_count, q_cols), lambda tile, ref: (0, lax.axis_index("gy"))),
                whole(o_magnitude.shape),
            ]
            + [whole((2 * own, q_cols))] * size_x,
            out_specs=whole((own, q_cols)),
        ),
        out_shape=jax.ShapeDtypeStruct((own, q_cols), BF16),
        compiler_params=pltpu.CompilerParams(vmem_limit_bytes=4 * 2**20),
        name="finish",
    )(scalars, hidden, o_magnitude, *o_parts)


def solution(mesh):
    in_specs = (
        P(),
        P(),
        P("gx", "gy"),
        P("gx", "gy"),
        P("gx", "gy"),
        P("gx", "gy"),
        P("gx", "gy"),
        P("gx", "gy"),
        P(None, "gx", None),
        P(None, None, "gy"),
        P(None, "gy"),
        P(None, "gx", None),
        P(None, None, "gy"),
        P(None, "gy"),
        P(),
        P(),
        P(),
        P(("gx", "gy"), None, None, None),
    )
    out_specs = P("gx", "gy")
    return jax.shard_map(local, mesh=mesh, in_specs=in_specs, out_specs=out_specs, check_vma=False)
```

```python
import functools
import math

import jax
import jax.numpy as jnp
import numpy as np
from jax import lax
from jax.experimental import pallas as pl
from jax.experimental.pallas import tpu as pltpu
from jax.sharding import PartitionSpec as P

HEADS = 128
KV_HEADS = 8
HEAD_DIM = 128
TENANTS = 8
RANK = 16
QBLOCK = 64
PAGE = 256

NF4_LEVELS = (
    -1.0,
    -0.6961928009986877,
    -0.5250730514526367,
    -0.39491748809814453,
    -0.28444138169288635,
    -0.18477343022833234,
    -0.09105003625154495,
    0.0,
    0.07958029955625534,
    0.16093020141124725,
    0.24611230194568634,
    0.33791524171829224,
    0.44070982933044434,
    0.5626170039176941,
    0.7229568362236023,
    1.0,
)
NORM_EPS = 1e-05
NEG_FILL = -1e30
ROPE_BASE = 500000.0
WORDS = 128
COLS = 2 * WORDS
CHUNK = 2048
PAD_ROWS = 16
DEPTH = 3
F32 = jnp.float32
BF16 = jnp.bfloat16
GATHER_ROWS = lax.GatherDimensionNumbers(
    offset_dims=(),
    collapsed_slice_dims=(0,),
    start_index_map=(0,),
    operand_batching_dims=(1,),
    start_indices_batching_dims=(1,),
)


def level_table():
    return np.broadcast_to(np.asarray(NF4_LEVELS, np.float32)[:, None], (16, WORDS)).copy()


def split_columns():
    matrix = np.zeros((COLS, COLS), np.float32)
    for column in range(COLS):
        matrix[column, column // 2 + WORDS * (column % 2)] = 1.0
    return matrix


def keyval_order(kv_columns, size_x):
    step = HEAD_DIM // 2 // size_x
    matrix = np.zeros((COLS, size_x * HEAD_DIM), np.float32)
    for column in range(kv_columns):
        head, inner = divmod(column, HEAD_DIM)
        half, turn = divmod(inner, HEAD_DIM // 2)
        piece, spot = divmod(turn, step)
        place = piece * HEAD_DIM + head * 2 * step + half * step + spot
        matrix[column, place] = 1.0
    return matrix


def dot(left, right):
    return jnp.dot(left, right, preferred_element_type=F32)


def dot_rows(left, right):
    return lax.dot_general(left, right, (((1,), (1,)), ((), ())), preferred_element_type=F32)


def three_parts(values):
    first = values.astype(BF16)
    rest = values - first.astype(F32)
    second = rest.astype(BF16)
    third = (rest - second.astype(F32)).astype(BF16)
    return first, second, third


def wide_dot(left, right):
    rows = left.shape[0]
    both = dot(jnp.concatenate(three_parts(left), 0), right)
    return (both[:rows] + both[rows : 2 * rows]) + both[2 * rows :]


def split_scales(absmax_ref, split_ref, scale_ref, first, tiles):
    rows = absmax_ref.shape[0]
    stacked = jnp.concatenate(
        [absmax_ref[:, COLS * tile : COLS * (tile + 1)] for tile in range(tiles)], 0
    )
    both = wide_dot(stacked, split_ref[...])
    for tile in range(tiles):
        scale_ref[first + tile] = both[rows * tile : rows * (tile + 1)]


def stack_tiles(array):
    return jnp.concatenate(
        [array[:, COLS * tile : COLS * (tile + 1)] for tile in range(array.shape[1] // COLS)], 0
    )


def pick_rows(table, index):
    return lax.gather(
        table,
        index[..., None],
        GATHER_ROWS,
        slice_sizes=(1, 1),
        mode=lax.GatherScatterMode.PROMISE_IN_BOUNDS,
    )


def weight_tile(codes_ref, scale_ref, level_ref, left_ref, store_ref, squared=True):
    in_rows = codes_ref.shape[0]
    chunk = min(CHUNK, in_rows)
    blocks = chunk // QBLOCK

    def visit(step, carry):
        total, squares = carry
        even_list = []
        odd_list = []
        for block in range(blocks):
            scale_row = scale_ref[pl.ds(step * blocks + block, 1), :]
            tables = [
                level_ref[8 * half : 8 * half + 8, :]
                * scale_row[:, WORDS * side : WORDS * side + WORDS]
                for side in range(2)
                for half in range(2)
            ]
            for row in range(0, QBLOCK, 8):
                word = codes_ref[pl.ds(step * chunk + block * QBLOCK + row, 8), :]
                low = word & 7
                even = jnp.where(
                    (word & 8) != 0, pick_rows(tables[1], low), pick_rows(tables[0], low)
                )
                high = lax.shift_right_logical(word, 4) & 7
                odd = jnp.where(
                    word >= 128, pick_rows(tables[3], high), pick_rows(tables[2], high)
                )
                even_list.append(even)
                odd_list.append(odd)
        weight = jnp.concatenate(
            [jnp.concatenate(even_list, 0), jnp.concatenate(odd_list, 0)], 1
        ).astype(BF16)
        start = pl.multiple_of(step * chunk, chunk)
        if store_ref is not None:
            store_ref[pl.ds(start, chunk), :] = weight
        total = total + dot(left_ref[:, pl.ds(start, chunk)], weight)
        if squared:
            squares = squares + dot(jnp.ones((PAD_ROWS, chunk), BF16), weight * weight)
        return (total, squares)

    return lax.fori_loop(
        0,
        in_rows // chunk,
        visit,
        (jnp.zeros((left_ref.shape[0], COLS), F32), jnp.zeros((PAD_ROWS, COLS), F32)),
    )


def block_mask(rows, columns, lead):
    row_id = lax.broadcasted_iota(jnp.int32, (rows, columns), 0)
    column_id = lax.broadcasted_iota(jnp.int32, (rows, columns), 1)
    owner = jnp.where(row_id < lead, row_id, lax.shift_right_logical(row_id - lead, 4))
    return owner == lax.shift_right_logical(column_id, 4)


def norm_terms(cross, gram, up_split, squares, row_count):
    inner = up_split * (2.0 * cross + gram)
    return squares + jnp.sum(
        inner.reshape(row_count, RANK, COLS), axis=1
    )


def code_copy(codes_ref, first, tile, buffer_ref, sems):
    columns = pl.ds(pl.multiple_of((first + tile) * WORDS, WORDS), WORDS)
    slot = tile % DEPTH if isinstance(tile, int) else lax.rem(tile, DEPTH)
    return pltpu.make_async_copy(codes_ref.at[:, columns], buffer_ref.at[slot], sems.at[slot])


def code_tile(codes_ref, first, tile, tiles, buffer_ref, sems):
    @pl.when(tile + DEPTH - 1 < tiles)
    def _():
        code_copy(codes_ref, first, tile + DEPTH - 1, buffer_ref, sems).start()

    code_copy(codes_ref, first, tile, buffer_ref, sems).wait()
    return buffer_ref.at[lax.rem(tile, DEPTH)]


def fetch(sources, buffers, sems):
    copies = [
        pltpu.make_async_copy(source, buffer, sems.at[spot])
        for spot, (source, buffer) in enumerate(zip(sources, buffers))
    ]
    for copy in copies:
        copy.start()
    return copies


def finish_all(copies):
    for copy in copies:
        copy.wait()


def read_scalars(source, buffer, sem):
    copy = pltpu.make_async_copy(source, buffer, sem)
    copy.start()
    return copy


def tenant_fetch(scalar_ref, row_count, source_ref, buffer_ref, lead, sems):
    return fetch(
        [source_ref.at[scalar_ref[row]] for row in range(row_count)],
        [
            buffer_ref.at[lead + RANK * row : lead + RANK * (row + 1), :]
            for row in range(row_count)
        ],
        sems,
    )


def query_kernel(
    row_count,
    size_x,
    tenant_hbm,
    hidden_hbm,
    gain_hbm,
    absmax_hbm,
    kv_absmax_hbm,
    level_hbm,
    split_hbm,
    join_hbm,
    kv_join_hbm,
    codes_ref,
    kv_codes_ref,
    down_ref,
    up_ref,
    *refs,
):
    outs = refs[:size_x]
    (
        hidden_ref,
        gain_ref,
        absmax_ref,
        kv_absmax_ref,
        level_ref,
        split_ref,
        join_ref,
        kv_join_ref,
        left_ref,
        scale_ref,
        total_ref,
        square_ref,
        chunk_ref,
        buffer_ref,
        kv_buffer_ref,
        ups_ref,
        code_sems,
        kv_sem,
        down_sems,
        up_sems,
        small_sems,
        scalar_ref,
        scalar_sem,
    ) = refs[size_x:]
    tiles = absmax_ref.shape[1] // COLS
    share = chunk_ref.shape[2] - HEAD_DIM
    low_rank = row_count * RANK
    here = lax.axis_index("gx")
    kv_copy = pltpu.make_async_copy(kv_codes_ref, kv_buffer_ref, kv_sem.at[0])
    scalars = read_scalars(tenant_hbm, scalar_ref, scalar_sem.at[0])
    kv_copy.start()
    smalls = fetch(
        [
            split_hbm,
            kv_absmax_hbm,
            level_hbm,
            hidden_hbm,
            gain_hbm,
            absmax_hbm,
            kv_join_hbm,
            join_hbm,
        ],
        [
            split_ref,
            kv_absmax_ref,
            level_ref,
            hidden_ref,
            gain_ref,
            absmax_ref,
            kv_join_ref,
            join_ref,
        ],
        small_sems,
    )
    code_copy(codes_ref, 0, 0, buffer_ref, code_sems).start()
    scalars.wait()
    downs = tenant_fetch(scalar_ref, row_count, down_ref, left_ref, PAD_ROWS, down_sems)
    finish_all(smalls[:5])
    states = hidden_ref[...].astype(F32)
    mean_square = jnp.mean(states * states, axis=1, keepdims=True)
    in_rows = left_ref.shape[1]
    own = pl.ds(pl.multiple_of(here * in_rows, in_rows), in_rows)
    normed = hidden_ref[:, own].astype(F32) * lax.rsqrt(mean_square + NORM_EPS) * gain_ref[:, own]
    left_ref[0:PAD_ROWS, :] = jnp.concatenate(
        [normed, jnp.zeros((PAD_ROWS - row_count, normed.shape[1]), F32)], 0
    ).astype(BF16)
    split_scales(kv_absmax_ref, split_ref, scale_ref, 0, 1)
    kv_copy.wait()
    for tile in range(1, min(DEPTH - 1, tiles)):
        code_copy(codes_ref, 0, tile, buffer_ref, code_sems).start()
    total, _ = weight_tile(
        kv_buffer_ref, scale_ref.at[0], level_ref, left_ref.at[0:PAD_ROWS, :], None, False
    )
    finish_all(smalls[5:])
    split_scales(absmax_ref, split_ref, scale_ref, 1, tiles)
    joined = wide_dot(total, kv_join_ref[...])
    for owner in range(size_x):
        chunk_ref[owner, :, share:] = joined[
            : 2 * row_count, owner * HEAD_DIM : (owner + 1) * HEAD_DIM
        ]
    ups = tenant_fetch(scalar_ref, row_count, up_ref, ups_ref, 0, up_sems)
    finish_all(downs)

    def visit(tile, carry):
        codes = code_tile(codes_ref, 0, tile, tiles, buffer_ref, code_sems)
        total, squares = weight_tile(codes, scale_ref.at[tile + 1], level_ref, left_ref, None)
        total_ref[tile] = total
        square_ref[tile] = squares[0:8]
        return carry

    lax.fori_loop(0, tiles, visit, 0)
    finish_all(ups)
    gram = dot_rows(left_ref[...], left_ref[PAD_ROWS:, :])
    gram = jnp.where(block_mask(*gram.shape, PAD_ROWS), gram, 0.0)
    up_split = dot(stack_tiles(ups_ref[...]), split_ref[...])
    lines = []
    for tile in range(tiles):
        up_tile = up_split[low_rank * tile : low_rank * (tile + 1)]
        extra = wide_dot(gram, up_tile.astype(BF16))
        total = total_ref[tile]
        lines.append(total[:row_count] + extra[:row_count])
        lines.append(
            norm_terms(
                total[PAD_ROWS:], extra[PAD_ROWS:], up_tile, square_ref[tile, 0:1], row_count
            )
        )
    joined = wide_dot(jnp.concatenate(lines, 0), join_ref[...])
    piece = min(COLS, share)
    for tile in range(tiles):
        for part in range(COLS // piece):
            owner, place = divmod(tile * COLS + part * piece, share)
            chunk_ref[owner, :, place : place + piece] = joined[
                2 * row_count * tile : 2 * row_count * (tile + 1),
                part * piece : (part + 1) * piece,
            ]
    for shift in range(size_x):
        outs[shift][...] = chunk_ref[lax.rem(here + shift, size_x)]


def store_copy(store_ref, slot, weight_ref, tile, sems):
    return pltpu.make_async_copy(store_ref.at[slot], weight_ref.at[tile], sems.at[slot])


def output_scale_kernel(
    row_count,
    first,
    tenant_hbm,
    absmax_hbm,
    level_hbm,
    split_hbm,
    join_hbm,
    codes_ref,
    down_ref,
    up_ref,
    norm_ref,
    up_split_ref,
    weight_ref,
    absmax_ref,
    level_ref,
    split_ref,
    join_ref,
    store_ref,
    left_ref,
    scale_ref,
    total_ref,
    square_ref,
    buffer_ref,
    ups_ref,
    code_sems,
    down_sems,
    up_sems,
    store_sems,
    small_sems,
    scalar_ref,
    scalar_sem,
):
    scalars = read_scalars(tenant_hbm, scalar_ref, scalar_sem.at[0])
    tiles = weight_ref.shape[0]
    low_rank = row_count * RANK
    columns = slice(first * COLS, (first + tiles) * COLS)
    code_copy(codes_ref, first, 0, buffer_ref, code_sems).start()
    smalls = fetch(
        [split_hbm, absmax_hbm.at[:, columns], level_hbm, join_hbm],
        [split_ref, absmax_ref, level_ref, join_ref],
        small_sems,
    )
    scalars.wait()
    downs = tenant_fetch(scalar_ref, row_count, down_ref, left_ref, 0, down_sems)
    for tile in range(1, min(DEPTH - 1, tiles)):
        code_copy(codes_ref, first, tile, buffer_ref, code_sems).start()
    ups = tenant_fetch(
        scalar_ref, row_count, up_ref.at[:, :, columns], ups_ref, 0, up_sems
    )
    finish_all(smalls)
    split_scales(absmax_ref, split_ref, scale_ref, 0, tiles)
    finish_all(downs)

    def visit(tile, carry):
        codes = code_tile(codes_ref, first, tile, tiles, buffer_ref, code_sems)
        slot = lax.rem(tile, 2)

        @pl.when(tile >= 2)
        def _():
            store_copy(store_ref, slot, weight_ref, tile - 2, store_sems).wait()

        total, squares = weight_tile(
            codes, scale_ref.at[tile], level_ref, left_ref, store_ref.at[slot]
        )
        store_copy(store_ref, slot, weight_ref, tile, store_sems).start()
        total_ref[tile] = total
        square_ref[tile] = squares[0:8]
        return carry

    lax.fori_loop(0, tiles, visit, 0)
    finish_all(ups)
    gram = dot_rows(left_ref[...], left_ref[...])
    gram = jnp.where(block_mask(*gram.shape, 0), gram, 0.0)
    up_split = dot(stack_tiles(ups_ref[...]), split_ref[...])
    lines = []
    for tile in range(tiles):
        up_tile = up_split[low_rank * tile : low_rank * (tile + 1)]
        narrow = up_tile.astype(BF16)
        up_split_ref[:, COLS * tile : COLS * (tile + 1)] = narrow
        extra = wide_dot(gram, narrow)
        lines.append(norm_terms(total_ref[tile], extra, up_tile, square_ref[tile, 0:1], row_count))
    joined = wide_dot(jnp.concatenate(lines, 0), join_ref[...])
    for tile in range(tiles):
        norm_ref[:, COLS * tile : COLS * (tile + 1)] = joined[
            row_count * tile : row_count * (tile + 1)
        ]
    for tile in range(max(tiles - 2, 0), tiles):
        store_copy(store_ref, tile % 2, weight_ref, tile, store_sems).wait()


def rotate_kernel(row_count, size_x, step, scalar_ref, magnitude_ref, cos_ref, sin_ref, *refs):
    parts = refs[:size_x]
    out_ref = refs[size_x]
    share = cos_ref.shape[1] - HEAD_DIM
    total = parts[0][...]
    for part in parts[1:]:
        total = total + part[...]
    magnitude = jnp.concatenate(
        [
            magnitude_ref[pl.ds(scalar_ref[row], 1), :]
            for row in range(row_count)
        ],
        0,
    )
    query = total[:row_count, :share] * (
        magnitude * lax.rsqrt(total[row_count:, :share])
    )
    keyval = total[:row_count, share:]
    half = HEAD_DIM // 2
    pieces = []
    for head in range(share // HEAD_DIM):
        block = query[:, head * HEAD_DIM : (head + 1) * HEAD_DIM]
        pieces.append(pltpu.roll(block, half, 1))
    lane = lax.broadcasted_iota(jnp.int32, keyval.shape, 1)
    other = jnp.where(
        (lane & step) != 0, pltpu.roll(keyval, step, 1), pltpu.roll(keyval, HEAD_DIM - step, 1)
    )
    values = jnp.concatenate([query, keyval], 1)
    partner = jnp.concatenate(pieces + [other], 1)
    turned = (values * cos_ref[...] + partner * sin_ref[...]).astype(BF16)
    for target in range(out_ref.shape[0]):
        out_ref[target] = turned


def attend_kernel(
    row_count,
    size_x,
    size_y,
    info_hbm,
    gathered_hbm,
    kv_order_hbm,
    pages_ref,
    send_ref,
    query_ref,
    mixed_ref,
    best_ref,
    total_ref,
    value_ref,
    held_ref,
    gathered_ref,
    kv_order_ref,
    info_ref,
    page_sems,
    small_sems,
):
    slots = pages_ref.shape[0]

    def page_copy(slot):
        return pltpu.make_async_copy(pages_ref.at[slot], held_ref.at[slot], page_sems.at[slot])

    smalls = fetch(
        [info_hbm, gathered_hbm, kv_order_hbm], [info_ref, gathered_ref, kv_order_ref], small_sems
    )
    ahead = min(DEPTH, slots)
    for slot in range(ahead):
        page_copy(slot).start()
    finish_all(smalls)
    devices = size_x * size_y
    per_target = HEADS // devices
    group = HEADS // KV_HEADS
    inv_root = 1.0 / math.sqrt(HEAD_DIM)
    used = info_ref[2 * slots]
    device = info_ref[2 * slots + 1]
    share = gathered_ref.shape[2] - HEAD_DIM

    def setup():
        heads_here = share // HEAD_DIM
        for place_x in range(size_x):
            for place_y in range(size_y):
                block = gathered_ref[place_x * size_y + place_y].astype(F32)
                for head in range(heads_here):
                    first = (place_y * size_x + place_x) * heads_here + head
                    query_ref[pl.ds(first, row_count, stride=HEADS), :] = block[
                        :, head * HEAD_DIM : (head + 1) * HEAD_DIM
                    ]
                mixed_ref[place_x, place_y * row_count : (place_y + 1) * row_count, :] = block[
                    :, share:
                ]
        best_ref[...] = jnp.full(best_ref.shape, NEG_FILL, F32)
        total_ref[...] = jnp.zeros(total_ref.shape, F32)
        value_ref[...] = jnp.zeros(value_ref.shape, F32)

        @pl.when(device < row_count)
        def _():
            columns = kv_order_ref.shape[0]
            plain = jnp.zeros((size_y * row_count, columns), F32)
            for place_x in range(size_x):
                plain = plain + dot_rows(
                    mixed_ref[place_x].astype(BF16),
                    kv_order_ref[:, place_x * HEAD_DIM : (place_x + 1) * HEAD_DIM],
                )
            heads_each = 2 * KV_HEADS // size_y
            for row in range(row_count):

                @pl.when(device == row)
                def _():
                    rows = []
                    for head in range(2 * KV_HEADS):
                        place_y, inner = divmod(head, heads_each)
                        line = place_y * row_count + row
                        one = plain[line : line + 1, inner * HEAD_DIM : (inner + 1) * HEAD_DIM]
                        rows.append(jnp.broadcast_to(one, (group, HEAD_DIM)))
                    new_keys = jnp.concatenate(rows[:KV_HEADS], 0)
                    new_values = jnp.concatenate(rows[KV_HEADS:], 0)
                    span = slice(row * HEADS, (row + 1) * HEADS)
                    score = jnp.sum(query_ref[span, :] * new_keys, 1, keepdims=True) * inv_root
                    best_ref[span, :] = jnp.broadcast_to(score, (HEADS, HEAD_DIM))
                    total_ref[span, :] = jnp.ones((HEADS, HEAD_DIM), F32)
                    value_ref[span, :] = new_values

    setup()

    def visit(slot, carry):
        @pl.when(slot + ahead < used)
        def _():
            page_copy(slot + ahead).start()

        page_copy(slot).wait()
        start = pl.multiple_of(info_ref[slot] * HEADS, HEADS)
        count = info_ref[slots + slot]
        span = pl.ds(start, HEADS)
        query = query_ref[span, :].astype(BF16)
        scores = jnp.concatenate(
            [
                dot_rows(
                    query[group * head : group * (head + 1), :],
                    held_ref[slot, 0, :, head * HEAD_DIM : (head + 1) * HEAD_DIM],
                )
                for head in range(KV_HEADS)
            ],
            0,
        )
        inside = lax.broadcasted_iota(jnp.int32, (HEADS, PAGE), 1) < count
        scores = jnp.where(inside, scores * inv_root, NEG_FILL)
        old_best = best_ref[span, :]
        best = jnp.maximum(old_best, jnp.max(scores, axis=1, keepdims=True))
        weights = jnp.where(inside, jnp.exp(scores - best[:, :1]), 0.0)
        keep = jnp.exp(old_best - best)
        best_ref[span, :] = best
        total_ref[span, :] = total_ref[span, :] * keep + jnp.sum(weights, axis=1, keepdims=True)
        coarse = weights.astype(BF16)
        fine = (weights - coarse.astype(F32)).astype(BF16)
        gains = []
        for head in range(KV_HEADS):
            rows = slice(group * head, group * (head + 1))
            both = dot(
                jnp.concatenate([coarse[rows], fine[rows]], 0),
                held_ref[slot, 1, :, head * HEAD_DIM : (head + 1) * HEAD_DIM],
            )
            gains.append(both[:group] + both[group:])
        value_ref[span, :] = value_ref[span, :] * keep + jnp.concatenate(gains, 0)
        return carry

    lax.fori_loop(0, used, visit, 0)
    for slot in range(ahead):

        @pl.when(slot >= used)
        def _(slot=slot):
            page_copy(slot).wait()


    def close():
        eye = lax.broadcasted_iota(jnp.int32, (HEADS, HEAD_DIM), 0) == lax.broadcasted_iota(
            jnp.int32, (HEADS, HEAD_DIM), 1
        )
        lines = []
        for source in (best_ref, total_ref):
            for row in range(row_count):
                block = source[row * HEADS : (row + 1) * HEADS, :]
                lines.append(jnp.sum(jnp.where(eye, block, 0.0), axis=0, keepdims=True))
        scalars = jnp.concatenate(lines, 0)
        for target in range(devices):
            for row in range(row_count):
                begin = row * HEADS + target * per_target
                send_ref[target, row * per_target : (row + 1) * per_target, :] = value_ref[
                    begin : begin + per_target, :
                ]
            send_ref[target, row_count * per_target :, :] = scalars

    close()


def merge_kernel(row_count, per_target, info_ref, parts_ref, out_ref):
    offset = info_ref[0] * per_target
    values = parts_ref[:, : row_count * per_target, :]
    scalars = parts_ref[:, row_count * per_target :, :]
    lane = lax.broadcasted_iota(jnp.int32, scalars.shape, 2)
    for row in range(row_count):
        for head in range(per_target):
            chosen = jnp.sum(jnp.where(lane == offset + head, scalars, 0.0), axis=2, keepdims=True)
            best = chosen[:, row : row + 1, :]
            total = chosen[:, row_count + row : row_count + row + 1, :]
            factor = jnp.exp(best - jnp.max(best, axis=0, keepdims=True))
            line = row * per_target + head
            top = jnp.sum(values[:, line : line + 1, :] * factor, axis=0)
            bottom = jnp.sum(total * factor, axis=0)
            ratio = (top / bottom).astype(BF16)
            for target in range(out_ref.shape[0]):
                out_ref[target, row : row + 1, head * HEAD_DIM : (head + 1) * HEAD_DIM] = ratio


def output_kernel(
    row_count,
    size_x,
    tile_counts,
    tenant_hbm,
    attended_hbm,
    join_hbm,
    down_ref,
    *refs,
):
    parts = len(tile_counts)
    norms_hbm = refs[:parts]
    ups_hbm = refs[parts : 2 * parts]
    weights = refs[2 * parts : 3 * parts]
    outs = refs[3 * parts : 3 * parts + size_x]
    refs = refs[3 * parts + size_x :]
    norms = refs[:parts]
    splits = refs[parts : 2 * parts]
    (
        attended_ref,
        join_ref,
        left_ref,
        low_ref,
        total_ref,
        chunk_ref,
        held_ref,
        down_sems,
        held_sems,
        small_sems,
        scalar_ref,
        scalar_sem,
    ) = refs[2 * parts :]
    tiles = sum(tile_counts)
    own = row_count // size_x
    scalars = read_scalars(tenant_hbm, scalar_ref, scalar_sem.at[0])
    smalls = fetch(
        [attended_hbm, join_hbm] + list(norms_hbm) + list(ups_hbm),
        [attended_ref, join_ref] + list(norms) + list(splits),
        small_sems,
    )
    loads = [
        pltpu.make_async_copy(
            weights[part].at[tile],
            held_ref.at[sum(tile_counts[:part]) + tile],
            held_sems.at[sum(tile_counts[:part]) + tile],
        )
        for part in range(parts)
        for tile in range(tile_counts[part])
    ]
    scalars.wait()
    downs = tenant_fetch(scalar_ref, row_count, down_ref, low_ref, 0, down_sems)
    for load in loads[:1]:
        load.start()
    smalls[0].wait()
    width = attended_ref.shape[2]
    for part in range(attended_ref.shape[0]):
        block = attended_ref[part].astype(F32)
        left_ref[:, part * width : (part + 1) * width] = jnp.concatenate(
            [block, jnp.zeros((PAD_ROWS - row_count, width), F32)], 0
        ).astype(BF16)
    finish_all(downs)
    finish_all(smalls[1:])
    for load in loads[1:3]:
        load.start()
    middle = dot_rows(left_ref[...], low_ref[...])
    middle = jnp.where(block_mask(*middle.shape, PAD_ROWS), middle, 0.0)
    extras = [wide_dot(middle, up[...]) for up in splits]
    numbers = []
    for part in range(parts):
        for tile in range(tile_counts[part]):
            spot = len(numbers)
            loads[spot].wait()
            if spot + 3 < tiles:
                loads[spot + 3].start()
            total_ref[spot] = dot(left_ref[...], held_ref[spot]) + extras[part][
                :, COLS * tile : COLS * (tile + 1)
            ]
            numbers.append(total_ref[spot, 0:row_count])
    joined = wide_dot(jnp.concatenate(numbers, 0), join_ref[...])
    for owner in range(size_x):
        for spot in range(tiles):
            begin = row_count * spot + owner * own
            chunk_ref[owner, 0:own, COLS * spot : COLS * (spot + 1)] = joined[begin : begin + own]
        for part in range(parts):
            begin = COLS * sum(tile_counts[:part])
            chunk_ref[owner, own : 2 * own, begin : begin + COLS * tile_counts[part]] = norms[
                part
            ][owner * own : (owner + 1) * own, :]
    here = lax.axis_index("gx")
    for shift in range(size_x):
        outs[shift][...] = chunk_ref[lax.rem(here + shift, size_x)]


def finish_kernel(row_count, size_x, scalar_ref, hidden_ref, magnitude_ref, *refs):
    parts = refs[:size_x]
    out_ref = refs[size_x]
    own = row_count // size_x
    total = parts[0][...]
    for part in parts[1:]:
        total = total + part[...]
    here = lax.axis_index("gx")
    states = hidden_ref[...].astype(F32)
    row_id = lax.broadcasted_iota(jnp.int32, states.shape, 0)
    for line in range(own):
        row = here * own + line
        state = jnp.sum(jnp.where(row_id == row, states, 0.0), axis=0, keepdims=True)
        magnitude = magnitude_ref[pl.ds(scalar_ref[row], 1), :]
        scale = magnitude * lax.rsqrt(total[own + line : own + line + 1])
        out_ref[line : line + 1, :] = (state + total[line : line + 1] * scale).astype(BF16)


def slot_info(page_table, lengths, device, slot_count):
    row_count, page_limit = page_table.shape
    page_need = (lengths + PAGE - 1) // PAGE
    page_numbers = jnp.arange(page_limit, dtype=jnp.int32)
    live_mask = page_numbers[None, :] < page_need[:, None]
    wanted = device * slot_count + jnp.arange(slot_count, dtype=jnp.int32)
    hits = ((page_table[None, :, :] == wanted[:, None, None]) & live_mask[None, :, :]).astype(
        jnp.int32
    )
    owner_row = jnp.sum(hits * jnp.arange(row_count, dtype=jnp.int32)[None, :, None], axis=(1, 2))
    remaining = jnp.clip(lengths[:, None] - page_numbers[None, :] * PAGE, 0, PAGE)
    filled = jnp.sum(hits * remaining[None, :, :], axis=(1, 2))
    return owner_row, filled, jnp.sum(hits)


def exchange(parts, axis, size):
    received = [parts[0]]
    for shift in range(1, size):
        received.append(
            lax.ppermute(parts[shift], axis, [(spot, (spot + shift) % size) for spot in range(size)])
        )
    return received


def whole(shape):
    return pl.BlockSpec(shape, lambda *_: (0,) * len(shape))


def local(
    hidden,
    norm_gain,
    q_codes,
    q_absmax,
    kv_codes,
    kv_absmax,
    o_codes,
    o_absmax,
    q_down,
    q_up,
    q_magnitude,
    o_down,
    o_up,
    o_magnitude,
    tenant,
    lengths,
    page_table,
    kv_cache,
):
    row_count, width = hidden.shape
    row_x = lax.axis_index("gx").astype(jnp.int32)
    col_y = lax.axis_index("gy").astype(jnp.int32)
    size_x = lax.axis_size("gx")
    size_y = lax.axis_size("gy")
    devices = size_x * size_y
    device = row_x * size_y + col_y
    in_rows, q_words = q_codes.shape
    q_cols = 2 * q_words
    share = q_cols // size_x
    kv_cols = 2 * kv_codes.shape[1]
    if kv_cols < COLS:
        kv_codes = jnp.pad(kv_codes, ((0, 0), (0, WORDS - kv_codes.shape[1])))
        kv_absmax = jnp.pad(kv_absmax, ((0, 0), (0, COLS - kv_cols)))
    low_rank = row_count * RANK
    level = jnp.asarray(level_table())
    split_matrix = split_columns()
    split = jnp.asarray(split_matrix, BF16)
    join = jnp.asarray(split_matrix.T, BF16)
    order = keyval_order(kv_cols, size_x)
    kv_join = jnp.asarray(split_matrix.T @ order, BF16)
    kv_order = jnp.asarray(order, BF16)
    scalars = tenant
    q_down = jnp.swapaxes(q_down, 1, 2)
    o_down = jnp.swapaxes(o_down, 1, 2)
    q_tiles = q_words // WORDS
    scale_rows = in_rows // QBLOCK

    smem = pl.BlockSpec(memory_space=pltpu.SMEM)
    vmem = pl.BlockSpec(memory_space=pltpu.VMEM)
    anywhere = pl.BlockSpec(memory_space=pltpu.HBM)
    chunk_shape = (2 * row_count, share + HEAD_DIM)
    scalar_scratch = [pltpu.SMEM((row_count,), jnp.int32), pltpu.SemaphoreType.DMA((1,))]
    small = [
        pltpu.VMEM((scale_rows, q_cols), F32),
        pltpu.VMEM((scale_rows, COLS), F32),
        pltpu.VMEM(level.shape, F32),
        pltpu.VMEM(split.shape, BF16),
        pltpu.VMEM(join.shape, BF16),
    ]
    q_parts = pl.pallas_call(
        functools.partial(query_kernel, row_count, size_x),
        in_specs=[anywhere] * 13,
        out_specs=[vmem] * size_x,
        scratch_shapes=[
            pltpu.VMEM((row_count, width), BF16),
            pltpu.VMEM((1, width), F32),
            *small,
            pltpu.VMEM(kv_join.shape, BF16),
            pltpu.VMEM((PAD_ROWS + low_rank, in_rows), BF16),
            pltpu.VMEM((q_tiles + 1, scale_rows, COLS), F32),
            pltpu.VMEM((q_tiles, PAD_ROWS + low_rank, COLS), F32),
            pltpu.VMEM((q_tiles, 8, COLS), F32),
            pltpu.VMEM((size_x,) + chunk_shape, F32),
            pltpu.VMEM((DEPTH, in_rows, WORDS), jnp.int32),
            pltpu.VMEM((in_rows, WORDS), jnp.int32),
            pltpu.VMEM((low_rank, q_cols), BF16),
            pltpu.SemaphoreType.DMA((DEPTH,)),
            pltpu.SemaphoreType.DMA((1,)),
            pltpu.SemaphoreType.DMA((row_count,)),
            pltpu.SemaphoreType.DMA((row_count,)),
            pltpu.SemaphoreType.DMA((8,)),
            *scalar_scratch,
        ],
        out_shape=[jax.ShapeDtypeStruct(chunk_shape, F32)] * size_x,
        name="query",
    )(
        tenant,
        hidden,
        norm_gain[None, :],
        q_absmax,
        kv_absmax,
        level,
        split,
        join,
        kv_join,
        q_codes,
        kv_codes,
        q_down,
        q_up,
    )
    q_parts = exchange(q_parts, "gx", size_x)

    def output_scales(first, tiles, after):
        owners, _ = lax.optimization_barrier((tenant, after))
        return pl.pallas_call(
            functools.partial(output_scale_kernel, row_count, first),
            in_specs=[anywhere] * 8,
            out_specs=[vmem, vmem, anywhere],
            scratch_shapes=[
                pltpu.VMEM((scale_rows, tiles * COLS), F32),
                *small[2:],
                pltpu.VMEM((2, in_rows, COLS), BF16),
                pltpu.VMEM((low_rank, in_rows), BF16),
                pltpu.VMEM((tiles, scale_rows, COLS), F32),
                pltpu.VMEM((tiles, low_rank, COLS), F32),
                pltpu.VMEM((tiles, 8, COLS), F32),
                pltpu.VMEM((DEPTH, in_rows, WORDS), jnp.int32),
                pltpu.VMEM((low_rank, tiles * COLS), BF16),
                pltpu.SemaphoreType.DMA((DEPTH,)),
                pltpu.SemaphoreType.DMA((row_count,)),
                pltpu.SemaphoreType.DMA((row_count,)),
                pltpu.SemaphoreType.DMA((2,)),
                pltpu.SemaphoreType.DMA((4,)),
                *scalar_scratch,
            ],
            out_shape=[
                jax.ShapeDtypeStruct((row_count, tiles * COLS), F32),
                jax.ShapeDtypeStruct((low_rank, tiles * COLS), BF16),
                pltpu.HBM((tiles, in_rows, COLS), BF16),
            ],
            compiler_params=pltpu.CompilerParams(vmem_limit_bytes=56 * 2**20),
            cost_estimate=pl.CostEstimate(
                flops=tiles * 5_000_000 * 256,
                bytes_accessed=tiles * 8 * in_rows * WORDS,
                transcendentals=0,
            ),
            name="output_scale",
        )(owners, o_absmax, level, split, join, o_codes, o_down, o_up)

    tile_counts = [q_tiles // 2, q_tiles - q_tiles // 2]

    half = HEAD_DIM // 2
    step = half // size_x
    lane = jnp.arange(share + HEAD_DIM, dtype=jnp.int32)
    in_query = lane < share
    turn = jnp.where(in_query, lane % half, row_x * step + lane % step)
    second = jnp.where(in_query, lane % HEAD_DIM // half, lane % (2 * step) // step)
    frequency = ROPE_BASE ** (-2.0 * turn.astype(F32) / HEAD_DIM)
    angles = lengths.astype(F32)[:, None] * frequency[None, :]
    plain = jnp.logical_and(~in_query, col_y * kv_cols >= KV_HEADS * HEAD_DIM)[None, :]
    cosine = jnp.where(plain, 1.0, jnp.cos(angles))
    sine = jnp.sin(angles)
    sine = jnp.where(plain, 0.0, jnp.where(second[None, :] == 1, sine, -sine))

    query_all = pl.pallas_call(
        functools.partial(rotate_kernel, row_count, size_x, step),
        grid_spec=pltpu.PrefetchScalarGridSpec(
            num_scalar_prefetch=1,
            grid=(1,),
            in_specs=[
                pl.BlockSpec((TENANTS, share), lambda tile, ref: (0, lax.axis_index("gx"))),
                whole(cosine.shape),
                whole(sine.shape),
            ]
            + [whole(chunk_shape)] * size_x,
            out_specs=whole((devices, row_count, share + HEAD_DIM)),
        ),
        out_shape=jax.ShapeDtypeStruct((devices, row_count, share + HEAD_DIM), BF16),
        compiler_params=pltpu.CompilerParams(vmem_limit_bytes=8 * 2**20),
        name="rotate",
    )(scalars, q_magnitude, cosine, sine, *q_parts)
    gathered = lax.all_to_all(query_all, ("gx", "gy"), split_axis=0, concat_axis=0, tiled=True)
    scale_parts = [output_scales(0, tile_counts[0], query_all)]
    gathered, scale_parts[0] = lax.optimization_barrier((gathered, scale_parts[0]))

    slots = kv_cache.shape[0]
    owner_row, filled, used = slot_info(page_table, lengths, device, slots)
    info = jnp.concatenate([owner_row, filled, used[None], device[None]]).astype(jnp.int32)
    per_target = HEADS // devices
    send_shape = (devices, row_count * per_target + 2 * row_count, HEAD_DIM)
    sent = pl.pallas_call(
        functools.partial(attend_kernel, row_count, size_x, size_y),
        in_specs=[anywhere] * 4,
        out_specs=vmem,
        scratch_shapes=[
            pltpu.VMEM((row_count * HEADS, HEAD_DIM), F32),
            pltpu.VMEM((size_x, size_y * row_count, HEAD_DIM), F32),
            pltpu.VMEM((row_count * HEADS, HEAD_DIM), F32),
            pltpu.VMEM((row_count * HEADS, HEAD_DIM), F32),
            pltpu.VMEM((row_count * HEADS, HEAD_DIM), F32),
            pltpu.VMEM(kv_cache.shape, BF16),
            pltpu.VMEM(gathered.shape, BF16),
            pltpu.VMEM((kv_cols, kv_order.shape[1]), BF16),
            pltpu.SMEM(info.shape, jnp.int32),
            pltpu.SemaphoreType.DMA((slots,)),
            pltpu.SemaphoreType.DMA((3,)),
        ],
        out_shape=jax.ShapeDtypeStruct(send_shape, F32),
        compiler_params=pltpu.CompilerParams(vmem_limit_bytes=58 * 2**20),
        name="attend",
    )(info, gathered, kv_order[:kv_cols], kv_cache)
    parts = lax.all_to_all(sent, ("gx", "gy"), split_axis=0, concat_axis=0, tiled=True)
    scale_parts.append(output_scales(tile_counts[0], tile_counts[1], sent))
    parts, scale_parts[1] = lax.optimization_barrier((parts, scale_parts[1]))

    merged = pl.pallas_call(
        functools.partial(merge_kernel, row_count, per_target),
        in_specs=[
            pl.BlockSpec(memory_space=pltpu.SMEM),
            pl.BlockSpec(memory_space=pltpu.VMEM),
        ],
        out_specs=pl.BlockSpec(memory_space=pltpu.VMEM),
        out_shape=jax.ShapeDtypeStruct((size_y, row_count, per_target * HEAD_DIM), BF16),
        compiler_params=pltpu.CompilerParams(vmem_limit_bytes=8 * 2**20),
        name="merge",
    )(device[None], parts)
    attended = lax.all_to_all(merged, "gy", split_axis=0, concat_axis=0, tiled=True)

    own = row_count // size_x
    o_parts = pl.pallas_call(
        functools.partial(output_kernel, row_count, size_x, tile_counts),
        in_specs=[anywhere] * (4 + 3 * len(scale_parts)),
        out_specs=[vmem] * size_x,
        scratch_shapes=[
            *[pltpu.VMEM((row_count, count * COLS), F32) for count in tile_counts],
            *[pltpu.VMEM((low_rank, count * COLS), BF16) for count in tile_counts],
            pltpu.VMEM(attended.shape, BF16),
            pltpu.VMEM(join.shape, BF16),
            pltpu.VMEM((PAD_ROWS, in_rows), BF16),
            pltpu.VMEM((low_rank, in_rows), BF16),
            pltpu.VMEM((q_tiles, PAD_ROWS, COLS), F32),
            pltpu.VMEM((size_x, 2 * own, q_cols), F32),
            pltpu.VMEM((q_tiles, in_rows, COLS), BF16),
            pltpu.SemaphoreType.DMA((row_count,)),
            pltpu.SemaphoreType.DMA((q_tiles,)),
            pltpu.SemaphoreType.DMA((2 + 2 * len(scale_parts),)),
            *scalar_scratch,
        ],
        out_shape=[jax.ShapeDtypeStruct((2 * own, q_cols), F32)] * size_x,
        compiler_params=pltpu.CompilerParams(vmem_limit_bytes=56 * 2**20),
        name="output",
    )(
        tenant,
        attended,
        join,
        o_down,
        *[part[0] for part in scale_parts],
        *[part[1] for part in scale_parts],
        *[part[2] for part in scale_parts],
    )
    o_parts = exchange(o_parts, "gx", size_x)
    return pl.pallas_call(
        functools.partial(finish_kernel, row_count, size_x),
        grid_spec=pltpu.PrefetchScalarGridSpec(
            num_scalar_prefetch=1,
            grid=(1,),
            in_specs=[
                pl.BlockSpec((row_count, q_cols), lambda tile, ref: (0, lax.axis_index("gy"))),
                whole(o_magnitude.shape),
            ]
            + [whole((2 * own, q_cols))] * size_x,
            out_specs=whole((own, q_cols)),
        ),
        out_shape=jax.ShapeDtypeStruct((own, q_cols), BF16),
        compiler_params=pltpu.CompilerParams(vmem_limit_bytes=4 * 2**20),
        name="finish",
    )(scalars, hidden, o_magnitude, *o_parts)


def solution(mesh):
    in_specs = (
        P(),
        P(),
        P("gx", "gy"),
        P("gx", "gy"),
        P("gx", "gy"),
        P("gx", "gy"),
        P("gx", "gy"),
        P("gx", "gy"),
        P(None, "gx", None),
        P(None, None, "gy"),
        P(None, "gy"),
        P(None, "gx", None),
        P(None, None, "gy"),
        P(None, "gy"),
        P(),
        P(),
        P(),
        P(("gx", "gy"), None, None, None),
    )
    out_specs = P("gx", "gy")
    return jax.shard_map(local, mesh=mesh, in_specs=in_specs, out_specs=out_specs, check_vma=False)
```

```python
import functools
import math

import jax
import jax.numpy as jnp
import numpy as np
from jax import lax
from jax.experimental import pallas as pl
from jax.experimental.pallas import tpu as pltpu
from jax.sharding import PartitionSpec as P

HEADS = 128
KV_HEADS = 8
HEAD_DIM = 128
TENANTS = 8
RANK = 16
QBLOCK = 64
PAGE = 256

NF4_LEVELS = (
    -1.0,
    -0.6961928009986877,
    -0.5250730514526367,
    -0.39491748809814453,
    -0.28444138169288635,
    -0.18477343022833234,
    -0.09105003625154495,
    0.0,
    0.07958029955625534,
    0.16093020141124725,
    0.24611230194568634,
    0.33791524171829224,
    0.44070982933044434,
    0.5626170039176941,
    0.7229568362236023,
    1.0,
)
NORM_EPS = 1e-05
NEG_FILL = -1e30
ROPE_BASE = 500000.0
WORDS = 128
COLS = 2 * WORDS
CHUNK = 2048
PAD_ROWS = 16
DEPTH = 3
LANE_VECTORS = 2
F32 = jnp.float32
BF16 = jnp.bfloat16
GATHER_ROWS = lax.GatherDimensionNumbers(
    offset_dims=(),
    collapsed_slice_dims=(0,),
    start_index_map=(0,),
    operand_batching_dims=(1,),
    start_indices_batching_dims=(1,),
)


def level_table():
    levels = np.asarray(NF4_LEVELS, np.float32)
    down = np.broadcast_to(levels[:, None], (16, WORDS))
    across = np.broadcast_to(np.tile(levels, WORDS // 16)[None, :], (8, WORDS))
    return np.concatenate([down, across], 0)


def split_columns():
    matrix = np.zeros((COLS, COLS), np.float32)
    for column in range(COLS):
        matrix[column, column // 2 + WORDS * (column % 2)] = 1.0
    return matrix


def keyval_order(kv_columns, size_x):
    step = HEAD_DIM // 2 // size_x
    matrix = np.zeros((COLS, size_x * HEAD_DIM), np.float32)
    for column in range(kv_columns):
        head, inner = divmod(column, HEAD_DIM)
        half, turn = divmod(inner, HEAD_DIM // 2)
        piece, spot = divmod(turn, step)
        place = piece * HEAD_DIM + head * 2 * step + half * step + spot
        matrix[column, place] = 1.0
    return matrix


def dot(left, right):
    return jnp.dot(left, right, preferred_element_type=F32)


def dot_rows(left, right):
    return lax.dot_general(left, right, (((1,), (1,)), ((), ())), preferred_element_type=F32)


def three_parts(values):
    first = values.astype(BF16)
    rest = values - first.astype(F32)
    second = rest.astype(BF16)
    third = (rest - second.astype(F32)).astype(BF16)
    return first, second, third


def wide_dot(left, right):
    rows = left.shape[0]
    both = dot(jnp.concatenate(three_parts(left), 0), right)
    return (both[:rows] + both[rows : 2 * rows]) + both[2 * rows :]


def split_scales(absmax_ref, split_ref, scale_ref, first, tiles):
    rows = absmax_ref.shape[0]
    stacked = jnp.concatenate(
        [absmax_ref[:, COLS * tile : COLS * (tile + 1)] for tile in range(tiles)], 0
    )
    both = wide_dot(stacked, split_ref[...])
    for tile in range(tiles):
        scale_ref[first + tile] = both[rows * tile : rows * (tile + 1)]


def stack_tiles(array):
    return jnp.concatenate(
        [array[:, COLS * tile : COLS * (tile + 1)] for tile in range(array.shape[1] // COLS)], 0
    )


GATHER_LANES = lax.GatherDimensionNumbers(
    offset_dims=(),
    collapsed_slice_dims=(1,),
    start_index_map=(1,),
    operand_batching_dims=(0,),
    start_indices_batching_dims=(0,),
)


def pick_lanes(table, index):
    return lax.gather(
        table,
        index[..., None],
        GATHER_LANES,
        slice_sizes=(1, 1),
        mode=lax.GatherScatterMode.PROMISE_IN_BOUNDS,
    )


def pick_rows(table, index):
    return lax.gather(
        table,
        index[..., None],
        GATHER_ROWS,
        slice_sizes=(1, 1),
        mode=lax.GatherScatterMode.PROMISE_IN_BOUNDS,
    )


def weight_tile(codes_ref, scale_ref, level_ref, left_ref, store_ref, squared=True):
    in_rows = codes_ref.shape[0]
    chunk = min(CHUNK, in_rows)
    blocks = chunk // QBLOCK

    def visit(step, carry):
        total, squares = carry
        even_list = []
        odd_list = []
        for block in range(blocks):
            scale_row = scale_ref[pl.ds(step * blocks + block, 1), :]
            tables = [
                level_ref[8 * half : 8 * half + 8, :]
                * scale_row[:, WORDS * side : WORDS * side + WORDS]
                for side in range(2)
                for half in range(2)
            ]
            for row in range(0, QBLOCK, 8):
                word = codes_ref[pl.ds(step * chunk + block * QBLOCK + row, 8), :]
                if row < 8 * LANE_VECTORS:
                    across = level_ref[16:24, :]
                    even = pick_lanes(across, word & 15) * scale_row[:, :WORDS]
                    odd = pick_lanes(across, lax.shift_right_logical(word, 4)) * scale_row[:, WORDS:]
                else:
                    low = word & 7
                    even = jnp.where(
                        (word & 8) != 0, pick_rows(tables[1], low), pick_rows(tables[0], low)
                    )
                    high = lax.shift_right_logical(word, 4) & 7
                    odd = jnp.where(
                        word >= 128, pick_rows(tables[3], high), pick_rows(tables[2], high)
                    )
                even_list.append(even)
                odd_list.append(odd)
        weight = jnp.concatenate(
            [jnp.concatenate(even_list, 0), jnp.concatenate(odd_list, 0)], 1
        ).astype(BF16)
        start = pl.multiple_of(step * chunk, chunk)
        if store_ref is not None:
            store_ref[pl.ds(start, chunk), :] = weight
        total = total + dot(left_ref[:, pl.ds(start, chunk)], weight)
        if squared:
            squares = squares + dot(jnp.ones((PAD_ROWS, chunk), BF16), weight * weight)
        return (total, squares)

    return lax.fori_loop(
        0,
        in_rows // chunk,
        visit,
        (jnp.zeros((left_ref.shape[0], COLS), F32), jnp.zeros((PAD_ROWS, COLS), F32)),
    )


def block_mask(rows, columns, lead):
    row_id = lax.broadcasted_iota(jnp.int32, (rows, columns), 0)
    column_id = lax.broadcasted_iota(jnp.int32, (rows, columns), 1)
    owner = jnp.where(row_id < lead, row_id, lax.shift_right_logical(row_id - lead, 4))
    return owner == lax.shift_right_logical(column_id, 4)


def norm_terms(cross, gram, up_split, squares, row_count):
    inner = up_split * (2.0 * cross + gram)
    return squares + jnp.sum(
        inner.reshape(row_count, RANK, COLS), axis=1
    )


def code_copy(codes_ref, first, tile, buffer_ref, sems):
    columns = pl.ds(pl.multiple_of((first + tile) * WORDS, WORDS), WORDS)
    slot = tile % DEPTH if isinstance(tile, int) else lax.rem(tile, DEPTH)
    return pltpu.make_async_copy(codes_ref.at[:, columns], buffer_ref.at[slot], sems.at[slot])


def code_tile(codes_ref, first, tile, tiles, buffer_ref, sems):
    @pl.when(tile + DEPTH - 1 < tiles)
    def _():
        code_copy(codes_ref, first, tile + DEPTH - 1, buffer_ref, sems).start(priority=1)

    code_copy(codes_ref, first, tile, buffer_ref, sems).wait()
    return buffer_ref.at[lax.rem(tile, DEPTH)]


def fetch(sources, buffers, sems):
    copies = [
        pltpu.make_async_copy(source, buffer, sems.at[spot])
        for spot, (source, buffer) in enumerate(zip(sources, buffers))
    ]
    for copy in copies:
        copy.start(priority=0)
    return copies


def finish_all(copies):
    for copy in copies:
        copy.wait()


def read_scalars(source, buffer, sem):
    copy = pltpu.make_async_copy(source, buffer, sem)
    copy.start()
    return copy


def tenant_fetch(scalar_ref, row_count, source_ref, buffer_ref, lead, sems):
    return fetch(
        [source_ref.at[scalar_ref[row]] for row in range(row_count)],
        [
            buffer_ref.at[lead + RANK * row : lead + RANK * (row + 1), :]
            for row in range(row_count)
        ],
        sems,
    )


def query_kernel(
    row_count,
    size_x,
    tenant_hbm,
    hidden_hbm,
    gain_hbm,
    absmax_hbm,
    kv_absmax_hbm,
    level_hbm,
    split_hbm,
    join_hbm,
    kv_join_hbm,
    codes_ref,
    kv_codes_ref,
    down_ref,
    up_ref,
    *refs,
):
    outs = refs[:size_x]
    (
        hidden_ref,
        gain_ref,
        absmax_ref,
        kv_absmax_ref,
        level_ref,
        split_ref,
        join_ref,
        kv_join_ref,
        left_ref,
        scale_ref,
        total_ref,
        square_ref,
        chunk_ref,
        buffer_ref,
        kv_buffer_ref,
        ups_ref,
        code_sems,
        kv_sem,
        down_sems,
        up_sems,
        small_sems,
        scalar_ref,
        scalar_sem,
    ) = refs[size_x:]
    tiles = absmax_ref.shape[1] // COLS
    share = chunk_ref.shape[2] - HEAD_DIM
    low_rank = row_count * RANK
    here = lax.axis_index("gx")
    kv_copy = pltpu.make_async_copy(kv_codes_ref, kv_buffer_ref, kv_sem.at[0])
    scalars = read_scalars(tenant_hbm, scalar_ref, scalar_sem.at[0])
    kv_copy.start(priority=1)
    smalls = fetch(
        [
            split_hbm,
            kv_absmax_hbm,
            level_hbm,
            hidden_hbm,
            gain_hbm,
            absmax_hbm,
            kv_join_hbm,
            join_hbm,
        ],
        [
            split_ref,
            kv_absmax_ref,
            level_ref,
            hidden_ref,
            gain_ref,
            absmax_ref,
            kv_join_ref,
            join_ref,
        ],
        small_sems,
    )
    code_copy(codes_ref, 0, 0, buffer_ref, code_sems).start(priority=1)
    scalars.wait()
    downs = tenant_fetch(scalar_ref, row_count, down_ref, left_ref, PAD_ROWS, down_sems)
    finish_all(smalls[:5])
    states = hidden_ref[...].astype(F32)
    mean_square = jnp.mean(states * states, axis=1, keepdims=True)
    in_rows = left_ref.shape[1]
    own = pl.ds(pl.multiple_of(here * in_rows, in_rows), in_rows)
    normed = hidden_ref[:, own].astype(F32) * lax.rsqrt(mean_square + NORM_EPS) * gain_ref[:, own]
    left_ref[0:PAD_ROWS, :] = jnp.concatenate(
        [normed, jnp.zeros((PAD_ROWS - row_count, normed.shape[1]), F32)], 0
    ).astype(BF16)
    split_scales(kv_absmax_ref, split_ref, scale_ref, 0, 1)
    kv_copy.wait()
    for tile in range(1, min(DEPTH - 1, tiles)):
        code_copy(codes_ref, 0, tile, buffer_ref, code_sems).start(priority=1)
    total, _ = weight_tile(
        kv_buffer_ref, scale_ref.at[0], level_ref, left_ref.at[0:PAD_ROWS, :], None, False
    )
    finish_all(smalls[5:])
    split_scales(absmax_ref, split_ref, scale_ref, 1, tiles)
    joined = wide_dot(total, kv_join_ref[...])
    for owner in range(size_x):
        chunk_ref[owner, :, share:] = joined[
            : 2 * row_count, owner * HEAD_DIM : (owner + 1) * HEAD_DIM
        ]
    ups = tenant_fetch(scalar_ref, row_count, up_ref, ups_ref, 0, up_sems)
    finish_all(downs)

    def visit(tile, carry):
        codes = code_tile(codes_ref, 0, tile, tiles, buffer_ref, code_sems)
        total, squares = weight_tile(codes, scale_ref.at[tile + 1], level_ref, left_ref, None)
        total_ref[tile] = total
        square_ref[tile] = squares[0:8]
        return carry

    lax.fori_loop(0, tiles, visit, 0)
    finish_all(ups)
    gram = dot_rows(left_ref[...], left_ref[PAD_ROWS:, :])
    gram = jnp.where(block_mask(*gram.shape, PAD_ROWS), gram, 0.0)
    up_split = dot(stack_tiles(ups_ref[...]), split_ref[...])
    lines = []
    for tile in range(tiles):
        up_tile = up_split[low_rank * tile : low_rank * (tile + 1)]
        extra = wide_dot(gram, up_tile.astype(BF16))
        total = total_ref[tile]
        lines.append(total[:row_count] + extra[:row_count])
        lines.append(
            norm_terms(
                total[PAD_ROWS:], extra[PAD_ROWS:], up_tile, square_ref[tile, 0:1], row_count
            )
        )
    joined = wide_dot(jnp.concatenate(lines, 0), join_ref[...])
    piece = min(COLS, share)
    for tile in range(tiles):
        for part in range(COLS // piece):
            owner, place = divmod(tile * COLS + part * piece, share)
            chunk_ref[owner, :, place : place + piece] = joined[
                2 * row_count * tile : 2 * row_count * (tile + 1),
                part * piece : (part + 1) * piece,
            ]
    for shift in range(size_x):
        outs[shift][...] = chunk_ref[lax.rem(here + shift, size_x)]


def store_copy(store_ref, slot, weight_ref, tile, sems):
    return pltpu.make_async_copy(store_ref.at[slot], weight_ref.at[tile], sems.at[slot])


def output_scale_kernel(
    row_count,
    first,
    tenant_hbm,
    absmax_hbm,
    level_hbm,
    split_hbm,
    join_hbm,
    codes_ref,
    down_ref,
    up_ref,
    norm_ref,
    up_split_ref,
    weight_ref,
    absmax_ref,
    level_ref,
    split_ref,
    join_ref,
    store_ref,
    left_ref,
    scale_ref,
    total_ref,
    square_ref,
    buffer_ref,
    ups_ref,
    code_sems,
    down_sems,
    up_sems,
    store_sems,
    small_sems,
    scalar_ref,
    scalar_sem,
):
    scalars = read_scalars(tenant_hbm, scalar_ref, scalar_sem.at[0])
    tiles = weight_ref.shape[0]
    low_rank = row_count * RANK
    columns = slice(first * COLS, (first + tiles) * COLS)
    code_copy(codes_ref, first, 0, buffer_ref, code_sems).start(priority=1)
    smalls = fetch(
        [split_hbm, absmax_hbm.at[:, columns], level_hbm, join_hbm],
        [split_ref, absmax_ref, level_ref, join_ref],
        small_sems,
    )
    scalars.wait()
    downs = tenant_fetch(scalar_ref, row_count, down_ref, left_ref, 0, down_sems)
    for tile in range(1, min(DEPTH - 1, tiles)):
        code_copy(codes_ref, first, tile, buffer_ref, code_sems).start(priority=1)
    ups = tenant_fetch(
        scalar_ref, row_count, up_ref.at[:, :, columns], ups_ref, 0, up_sems
    )
    finish_all(smalls)
    split_scales(absmax_ref, split_ref, scale_ref, 0, tiles)
    finish_all(downs)

    def visit(tile, carry):
        codes = code_tile(codes_ref, first, tile, tiles, buffer_ref, code_sems)
        slot = lax.rem(tile, 2)

        @pl.when(tile >= 2)
        def _():
            store_copy(store_ref, slot, weight_ref, tile - 2, store_sems).wait()

        total, squares = weight_tile(
            codes, scale_ref.at[tile], level_ref, left_ref, store_ref.at[slot]
        )
        store_copy(store_ref, slot, weight_ref, tile, store_sems).start()
        total_ref[tile] = total
        square_ref[tile] = squares[0:8]
        return carry

    lax.fori_loop(0, tiles, visit, 0)
    finish_all(ups)
    gram = dot_rows(left_ref[...], left_ref[...])
    gram = jnp.where(block_mask(*gram.shape, 0), gram, 0.0)
    up_split = dot(stack_tiles(ups_ref[...]), split_ref[...])
    lines = []
    for tile in range(tiles):
        up_tile = up_split[low_rank * tile : low_rank * (tile + 1)]
        narrow = up_tile.astype(BF16)
        up_split_ref[:, COLS * tile : COLS * (tile + 1)] = narrow
        extra = wide_dot(gram, narrow)
        lines.append(norm_terms(total_ref[tile], extra, up_tile, square_ref[tile, 0:1], row_count))
    joined = wide_dot(jnp.concatenate(lines, 0), join_ref[...])
    for tile in range(tiles):
        norm_ref[:, COLS * tile : COLS * (tile + 1)] = joined[
            row_count * tile : row_count * (tile + 1)
        ]
    for tile in range(max(tiles - 2, 0), tiles):
        store_copy(store_ref, tile % 2, weight_ref, tile, store_sems).wait()


def rotate_kernel(row_count, size_x, step, scalar_ref, magnitude_ref, cos_ref, sin_ref, *refs):
    parts = refs[:size_x]
    out_ref = refs[size_x]
    share = cos_ref.shape[1] - HEAD_DIM
    total = parts[0][...]
    for part in parts[1:]:
        total = total + part[...]
    magnitude = jnp.concatenate(
        [
            magnitude_ref[pl.ds(scalar_ref[row], 1), :]
            for row in range(row_count)
        ],
        0,
    )
    query = total[:row_count, :share] * (
        magnitude * lax.rsqrt(total[row_count:, :share])
    )
    keyval = total[:row_count, share:]
    half = HEAD_DIM // 2
    pieces = []
    for head in range(share // HEAD_DIM):
        block = query[:, head * HEAD_DIM : (head + 1) * HEAD_DIM]
        pieces.append(pltpu.roll(block, half, 1))
    lane = lax.broadcasted_iota(jnp.int32, keyval.shape, 1)
    other = jnp.where(
        (lane & step) != 0, pltpu.roll(keyval, step, 1), pltpu.roll(keyval, HEAD_DIM - step, 1)
    )
    values = jnp.concatenate([query, keyval], 1)
    partner = jnp.concatenate(pieces + [other], 1)
    turned = (values * cos_ref[...] + partner * sin_ref[...]).astype(BF16)
    for target in range(out_ref.shape[0]):
        out_ref[target] = turned


def attend_kernel(
    row_count,
    size_x,
    size_y,
    info_hbm,
    gathered_hbm,
    kv_order_hbm,
    pages_ref,
    send_ref,
    query_ref,
    mixed_ref,
    best_ref,
    total_ref,
    value_ref,
    held_ref,
    gathered_ref,
    kv_order_ref,
    info_ref,
    page_sems,
    small_sems,
):
    slots = pages_ref.shape[0]

    def page_copy(slot):
        return pltpu.make_async_copy(pages_ref.at[slot], held_ref.at[slot], page_sems.at[slot])

    smalls = fetch(
        [info_hbm, gathered_hbm, kv_order_hbm], [info_ref, gathered_ref, kv_order_ref], small_sems
    )
    ahead = min(DEPTH, slots)
    for slot in range(ahead):
        page_copy(slot).start(priority=1)
    finish_all(smalls)
    devices = size_x * size_y
    per_target = HEADS // devices
    group = HEADS // KV_HEADS
    inv_root = 1.0 / math.sqrt(HEAD_DIM)
    used = info_ref[2 * slots]
    device = info_ref[2 * slots + 1]
    share = gathered_ref.shape[2] - HEAD_DIM

    def setup():
        heads_here = share // HEAD_DIM
        for place_x in range(size_x):
            for place_y in range(size_y):
                block = gathered_ref[place_x * size_y + place_y].astype(F32)
                for head in range(heads_here):
                    first = (place_y * size_x + place_x) * heads_here + head
                    query_ref[pl.ds(first, row_count, stride=HEADS), :] = block[
                        :, head * HEAD_DIM : (head + 1) * HEAD_DIM
                    ]
                mixed_ref[place_x, place_y * row_count : (place_y + 1) * row_count, :] = block[
                    :, share:
                ]
        best_ref[...] = jnp.full(best_ref.shape, NEG_FILL, F32)
        total_ref[...] = jnp.zeros(total_ref.shape, F32)
        value_ref[...] = jnp.zeros(value_ref.shape, F32)

        @pl.when(device < row_count)
        def _():
            columns = kv_order_ref.shape[0]
            plain = jnp.zeros((size_y * row_count, columns), F32)
            for place_x in range(size_x):
                plain = plain + dot_rows(
                    mixed_ref[place_x].astype(BF16),
                    kv_order_ref[:, place_x * HEAD_DIM : (place_x + 1) * HEAD_DIM],
                )
            heads_each = 2 * KV_HEADS // size_y
            for row in range(row_count):

                @pl.when(device == row)
                def _():
                    rows = []
                    for head in range(2 * KV_HEADS):
                        place_y, inner = divmod(head, heads_each)
                        line = place_y * row_count + row
                        one = plain[line : line + 1, inner * HEAD_DIM : (inner + 1) * HEAD_DIM]
                        rows.append(jnp.broadcast_to(one, (group, HEAD_DIM)))
                    new_keys = jnp.concatenate(rows[:KV_HEADS], 0)
                    new_values = jnp.concatenate(rows[KV_HEADS:], 0)
                    span = slice(row * HEADS, (row + 1) * HEADS)
                    score = jnp.sum(query_ref[span, :] * new_keys, 1, keepdims=True) * inv_root
                    best_ref[span, :] = jnp.broadcast_to(score, (HEADS, HEAD_DIM))
                    total_ref[span, :] = jnp.ones((HEADS, HEAD_DIM), F32)
                    value_ref[span, :] = new_values

    setup()

    def visit(slot, carry):
        @pl.when(slot + ahead < used)
        def _():
            page_copy(slot + ahead).start(priority=1)

        page_copy(slot).wait()
        start = pl.multiple_of(info_ref[slot] * HEADS, HEADS)
        count = info_ref[slots + slot]
        span = pl.ds(start, HEADS)
        query = query_ref[span, :].astype(BF16)
        scores = jnp.concatenate(
            [
                dot_rows(
                    query[group * head : group * (head + 1), :],
                    held_ref[slot, 0, :, head * HEAD_DIM : (head + 1) * HEAD_DIM],
                )
                for head in range(KV_HEADS)
            ],
            0,
        )
        inside = lax.broadcasted_iota(jnp.int32, (HEADS, PAGE), 1) < count
        scores = jnp.where(inside, scores * inv_root, NEG_FILL)
        old_best = best_ref[span, :]
        best = jnp.maximum(old_best, jnp.max(scores, axis=1, keepdims=True))
        weights = jnp.where(inside, jnp.exp(scores - best[:, :1]), 0.0)
        keep = jnp.exp(old_best - best)
        best_ref[span, :] = best
        total_ref[span, :] = total_ref[span, :] * keep + jnp.sum(weights, axis=1, keepdims=True)
        coarse = weights.astype(BF16)
        fine = (weights - coarse.astype(F32)).astype(BF16)
        gains = []
        for head in range(KV_HEADS):
            rows = slice(group * head, group * (head + 1))
            both = dot(
                jnp.concatenate([coarse[rows], fine[rows]], 0),
                held_ref[slot, 1, :, head * HEAD_DIM : (head + 1) * HEAD_DIM],
            )
            gains.append(both[:group] + both[group:])
        value_ref[span, :] = value_ref[span, :] * keep + jnp.concatenate(gains, 0)
        return carry

    lax.fori_loop(0, used, visit, 0)
    for slot in range(ahead):

        @pl.when(slot >= used)
        def _(slot=slot):
            page_copy(slot).wait()


    def close():
        eye = lax.broadcasted_iota(jnp.int32, (HEADS, HEAD_DIM), 0) == lax.broadcasted_iota(
            jnp.int32, (HEADS, HEAD_DIM), 1
        )
        lines = []
        for source in (best_ref, total_ref):
            for row in range(row_count):
                block = source[row * HEADS : (row + 1) * HEADS, :]
                lines.append(jnp.sum(jnp.where(eye, block, 0.0), axis=0, keepdims=True))
        scalars = jnp.concatenate(lines, 0)
        for target in range(devices):
            for row in range(row_count):
                begin = row * HEADS + target * per_target
                send_ref[target, row * per_target : (row + 1) * per_target, :] = value_ref[
                    begin : begin + per_target, :
                ]
            send_ref[target, row_count * per_target :, :] = scalars

    close()


def merge_kernel(row_count, per_target, info_ref, parts_ref, out_ref):
    offset = info_ref[0] * per_target
    values = parts_ref[:, : row_count * per_target, :]
    scalars = parts_ref[:, row_count * per_target :, :]
    lane = lax.broadcasted_iota(jnp.int32, scalars.shape, 2)
    for row in range(row_count):
        for head in range(per_target):
            chosen = jnp.sum(jnp.where(lane == offset + head, scalars, 0.0), axis=2, keepdims=True)
            best = chosen[:, row : row + 1, :]
            total = chosen[:, row_count + row : row_count + row + 1, :]
            factor = jnp.exp(best - jnp.max(best, axis=0, keepdims=True))
            line = row * per_target + head
            top = jnp.sum(values[:, line : line + 1, :] * factor, axis=0)
            bottom = jnp.sum(total * factor, axis=0)
            ratio = (top / bottom).astype(BF16)
            for target in range(out_ref.shape[0]):
                out_ref[target, row : row + 1, head * HEAD_DIM : (head + 1) * HEAD_DIM] = ratio


def output_kernel(
    row_count,
    size_x,
    tile_counts,
    tenant_hbm,
    attended_hbm,
    join_hbm,
    down_ref,
    *refs,
):
    parts = len(tile_counts)
    norms_hbm = refs[:parts]
    ups_hbm = refs[parts : 2 * parts]
    weights = refs[2 * parts : 3 * parts]
    outs = refs[3 * parts : 3 * parts + size_x]
    refs = refs[3 * parts + size_x :]
    norms = refs[:parts]
    splits = refs[parts : 2 * parts]
    (
        attended_ref,
        join_ref,
        left_ref,
        low_ref,
        total_ref,
        chunk_ref,
        held_ref,
        down_sems,
        held_sems,
        small_sems,
        scalar_ref,
        scalar_sem,
    ) = refs[2 * parts :]
    tiles = sum(tile_counts)
    own = row_count // size_x
    scalars = read_scalars(tenant_hbm, scalar_ref, scalar_sem.at[0])
    smalls = fetch(
        [attended_hbm, join_hbm] + list(norms_hbm) + list(ups_hbm),
        [attended_ref, join_ref] + list(norms) + list(splits),
        small_sems,
    )
    loads = [
        pltpu.make_async_copy(
            weights[part].at[tile],
            held_ref.at[sum(tile_counts[:part]) + tile],
            held_sems.at[sum(tile_counts[:part]) + tile],
        )
        for part in range(parts)
        for tile in range(tile_counts[part])
    ]
    scalars.wait()
    downs = tenant_fetch(scalar_ref, row_count, down_ref, low_ref, 0, down_sems)
    for load in loads:
        load.start(priority=1)
    smalls[0].wait()
    width = attended_ref.shape[2]
    for part in range(attended_ref.shape[0]):
        block = attended_ref[part].astype(F32)
        left_ref[:, part * width : (part + 1) * width] = jnp.concatenate(
            [block, jnp.zeros((PAD_ROWS - row_count, width), F32)], 0
        ).astype(BF16)
    finish_all(downs)
    finish_all(smalls[1:])
    middle = dot_rows(left_ref[...], low_ref[...])
    middle = jnp.where(block_mask(*middle.shape, PAD_ROWS), middle, 0.0)
    extras = [wide_dot(middle, up[...]) for up in splits]
    numbers = []
    for part in range(parts):
        for tile in range(tile_counts[part]):
            spot = len(numbers)
            loads[spot].wait()
            total_ref[spot] = dot(left_ref[...], held_ref[spot]) + extras[part][
                :, COLS * tile : COLS * (tile + 1)
            ]
            numbers.append(total_ref[spot, 0:row_count])
    joined = wide_dot(jnp.concatenate(numbers, 0), join_ref[...])
    for owner in range(size_x):
        for spot in range(tiles):
            begin = row_count * spot + owner * own
            chunk_ref[owner, 0:own, COLS * spot : COLS * (spot + 1)] = joined[begin : begin + own]
        for part in range(parts):
            begin = COLS * sum(tile_counts[:part])
            chunk_ref[owner, own : 2 * own, begin : begin + COLS * tile_counts[part]] = norms[
                part
            ][owner * own : (owner + 1) * own, :]
    here = lax.axis_index("gx")
    for shift in range(size_x):
        outs[shift][...] = chunk_ref[lax.rem(here + shift, size_x)]


def finish_kernel(row_count, size_x, scalar_ref, hidden_ref, magnitude_ref, *refs):
    parts = refs[:size_x]
    out_ref = refs[size_x]
    own = row_count // size_x
    total = parts[0][...]
    for part in parts[1:]:
        total = total + part[...]
    here = lax.axis_index("gx")
    states = hidden_ref[...].astype(F32)
    row_id = lax.broadcasted_iota(jnp.int32, states.shape, 0)
    for line in range(own):
        row = here * own + line
        state = jnp.sum(jnp.where(row_id == row, states, 0.0), axis=0, keepdims=True)
        magnitude = magnitude_ref[pl.ds(scalar_ref[row], 1), :]
        scale = magnitude * lax.rsqrt(total[own + line : own + line + 1])
        out_ref[line : line + 1, :] = (state + total[line : line + 1] * scale).astype(BF16)


def slot_info(page_table, lengths, device, slot_count):
    row_count, page_limit = page_table.shape
    page_need = (lengths + PAGE - 1) // PAGE
    page_numbers = jnp.arange(page_limit, dtype=jnp.int32)
    live_mask = page_numbers[None, :] < page_need[:, None]
    wanted = device * slot_count + jnp.arange(slot_count, dtype=jnp.int32)
    hits = ((page_table[None, :, :] == wanted[:, None, None]) & live_mask[None, :, :]).astype(
        jnp.int32
    )
    owner_row = jnp.sum(hits * jnp.arange(row_count, dtype=jnp.int32)[None, :, None], axis=(1, 2))
    remaining = jnp.clip(lengths[:, None] - page_numbers[None, :] * PAGE, 0, PAGE)
    filled = jnp.sum(hits * remaining[None, :, :], axis=(1, 2))
    return owner_row, filled, jnp.sum(hits)


def exchange(parts, axis, size):
    received = [parts[0]]
    for shift in range(1, size):
        received.append(
            lax.ppermute(parts[shift], axis, [(spot, (spot + shift) % size) for spot in range(size)])
        )
    return received


def whole(shape):
    return pl.BlockSpec(shape, lambda *_: (0,) * len(shape))


def local(
    hidden,
    norm_gain,
    q_codes,
    q_absmax,
    kv_codes,
    kv_absmax,
    o_codes,
    o_absmax,
    q_down,
    q_up,
    q_magnitude,
    o_down,
    o_up,
    o_magnitude,
    tenant,
    lengths,
    page_table,
    kv_cache,
):
    row_count, width = hidden.shape
    row_x = lax.axis_index("gx").astype(jnp.int32)
    col_y = lax.axis_index("gy").astype(jnp.int32)
    size_x = lax.axis_size("gx")
    size_y = lax.axis_size("gy")
    devices = size_x * size_y
    device = row_x * size_y + col_y
    in_rows, q_words = q_codes.shape
    q_cols = 2 * q_words
    share = q_cols // size_x
    kv_cols = 2 * kv_codes.shape[1]
    if kv_cols < COLS:
        kv_codes = jnp.pad(kv_codes, ((0, 0), (0, WORDS - kv_codes.shape[1])))
        kv_absmax = jnp.pad(kv_absmax, ((0, 0), (0, COLS - kv_cols)))
    low_rank = row_count * RANK
    level = jnp.asarray(level_table())
    split_matrix = split_columns()
    split = jnp.asarray(split_matrix, BF16)
    join = jnp.asarray(split_matrix.T, BF16)
    order = keyval_order(kv_cols, size_x)
    kv_join = jnp.asarray(split_matrix.T @ order, BF16)
    kv_order = jnp.asarray(order, BF16)
    scalars = tenant
    q_down = jnp.swapaxes(q_down, 1, 2)
    o_down = jnp.swapaxes(o_down, 1, 2)
    q_tiles = q_words // WORDS
    scale_rows = in_rows // QBLOCK

    smem = pl.BlockSpec(memory_space=pltpu.SMEM)
    vmem = pl.BlockSpec(memory_space=pltpu.VMEM)
    anywhere = pl.BlockSpec(memory_space=pltpu.HBM)
    chunk_shape = (2 * row_count, share + HEAD_DIM)
    scalar_scratch = [pltpu.SMEM((row_count,), jnp.int32), pltpu.SemaphoreType.DMA((1,))]
    small = [
        pltpu.VMEM((scale_rows, q_cols), F32),
        pltpu.VMEM((scale_rows, COLS), F32),
        pltpu.VMEM(level.shape, F32),
        pltpu.VMEM(split.shape, BF16),
        pltpu.VMEM(join.shape, BF16),
    ]
    q_parts = pl.pallas_call(
        functools.partial(query_kernel, row_count, size_x),
        in_specs=[anywhere] * 13,
        out_specs=[vmem] * size_x,
        scratch_shapes=[
            pltpu.VMEM((row_count, width), BF16),
            pltpu.VMEM((1, width), F32),
            *small,
            pltpu.VMEM(kv_join.shape, BF16),
            pltpu.VMEM((PAD_ROWS + low_rank, in_rows), BF16),
            pltpu.VMEM((q_tiles + 1, scale_rows, COLS), F32),
            pltpu.VMEM((q_tiles, PAD_ROWS + low_rank, COLS), F32),
            pltpu.VMEM((q_tiles, 8, COLS), F32),
            pltpu.VMEM((size_x,) + chunk_shape, F32),
            pltpu.VMEM((DEPTH, in_rows, WORDS), jnp.int32),
            pltpu.VMEM((in_rows, WORDS), jnp.int32),
            pltpu.VMEM((low_rank, q_cols), BF16),
            pltpu.SemaphoreType.DMA((DEPTH,)),
            pltpu.SemaphoreType.DMA((1,)),
            pltpu.SemaphoreType.DMA((row_count,)),
            pltpu.SemaphoreType.DMA((row_count,)),
            pltpu.SemaphoreType.DMA((8,)),
            *scalar_scratch,
        ],
        out_shape=[jax.ShapeDtypeStruct(chunk_shape, F32)] * size_x,
        name="query",
    )(
        tenant,
        hidden,
        norm_gain[None, :],
        q_absmax,
        kv_absmax,
        level,
        split,
        join,
        kv_join,
        q_codes,
        kv_codes,
        q_down,
        q_up,
    )
    q_parts = exchange(q_parts, "gx", size_x)

    def output_scales(first, tiles, after):
        owners, _ = lax.optimization_barrier((tenant, after))
        return pl.pallas_call(
            functools.partial(output_scale_kernel, row_count, first),
            in_specs=[anywhere] * 8,
            out_specs=[vmem, vmem, anywhere],
            scratch_shapes=[
                pltpu.VMEM((scale_rows, tiles * COLS), F32),
                *small[2:],
                pltpu.VMEM((2, in_rows, COLS), BF16),
                pltpu.VMEM((low_rank, in_rows), BF16),
                pltpu.VMEM((tiles, scale_rows, COLS), F32),
                pltpu.VMEM((tiles, low_rank, COLS), F32),
                pltpu.VMEM((tiles, 8, COLS), F32),
                pltpu.VMEM((DEPTH, in_rows, WORDS), jnp.int32),
                pltpu.VMEM((low_rank, tiles * COLS), BF16),
                pltpu.SemaphoreType.DMA((DEPTH,)),
                pltpu.SemaphoreType.DMA((row_count,)),
                pltpu.SemaphoreType.DMA((row_count,)),
                pltpu.SemaphoreType.DMA((2,)),
                pltpu.SemaphoreType.DMA((4,)),
                *scalar_scratch,
            ],
            out_shape=[
                jax.ShapeDtypeStruct((row_count, tiles * COLS), F32),
                jax.ShapeDtypeStruct((low_rank, tiles * COLS), BF16),
                pltpu.HBM((tiles, in_rows, COLS), BF16),
            ],
            compiler_params=pltpu.CompilerParams(vmem_limit_bytes=56 * 2**20),
            cost_estimate=pl.CostEstimate(
                flops=tiles * 5_000_000 * 256,
                bytes_accessed=tiles * 8 * in_rows * WORDS,
                transcendentals=0,
            ),
            name="output_scale",
        )(owners, o_absmax, level, split, join, o_codes, o_down, o_up)

    tile_counts = [3 * q_tiles // 8, q_tiles - 3 * q_tiles // 8]

    half = HEAD_DIM // 2
    step = half // size_x
    lane = jnp.arange(share + HEAD_DIM, dtype=jnp.int32)
    in_query = lane < share
    turn = jnp.where(in_query, lane % half, row_x * step + lane % step)
    second = jnp.where(in_query, lane % HEAD_DIM // half, lane % (2 * step) // step)
    frequency = ROPE_BASE ** (-2.0 * turn.astype(F32) / HEAD_DIM)
    angles = lengths.astype(F32)[:, None] * frequency[None, :]
    plain = jnp.logical_and(~in_query, col_y * kv_cols >= KV_HEADS * HEAD_DIM)[None, :]
    cosine = jnp.where(plain, 1.0, jnp.cos(angles))
    sine = jnp.sin(angles)
    sine = jnp.where(plain, 0.0, jnp.where(second[None, :] == 1, sine, -sine))

    query_all = pl.pallas_call(
        functools.partial(rotate_kernel, row_count, size_x, step),
        grid_spec=pltpu.PrefetchScalarGridSpec(
            num_scalar_prefetch=1,
            grid=(1,),
            in_specs=[
                pl.BlockSpec((TENANTS, share), lambda tile, ref: (0, lax.axis_index("gx"))),
                whole(cosine.shape),
                whole(sine.shape),
            ]
            + [whole(chunk_shape)] * size_x,
            out_specs=whole((devices, row_count, share + HEAD_DIM)),
        ),
        out_shape=jax.ShapeDtypeStruct((devices, row_count, share + HEAD_DIM), BF16),
        compiler_params=pltpu.CompilerParams(vmem_limit_bytes=8 * 2**20),
        name="rotate",
    )(scalars, q_magnitude, cosine, sine, *q_parts)
    gathered = lax.all_to_all(query_all, ("gx", "gy"), split_axis=0, concat_axis=0, tiled=True)
    scale_parts = [output_scales(0, tile_counts[0], query_all)]
    gathered, scale_parts[0] = lax.optimization_barrier((gathered, scale_parts[0]))

    slots = kv_cache.shape[0]
    owner_row, filled, used = slot_info(page_table, lengths, device, slots)
    info = jnp.concatenate([owner_row, filled, used[None], device[None]]).astype(jnp.int32)
    per_target = HEADS // devices
    send_shape = (devices, row_count * per_target + 2 * row_count, HEAD_DIM)
    sent = pl.pallas_call(
        functools.partial(attend_kernel, row_count, size_x, size_y),
        in_specs=[anywhere] * 4,
        out_specs=vmem,
        scratch_shapes=[
            pltpu.VMEM((row_count * HEADS, HEAD_DIM), F32),
            pltpu.VMEM((size_x, size_y * row_count, HEAD_DIM), F32),
            pltpu.VMEM((row_count * HEADS, HEAD_DIM), F32),
            pltpu.VMEM((row_count * HEADS, HEAD_DIM), F32),
            pltpu.VMEM((row_count * HEADS, HEAD_DIM), F32),
            pltpu.VMEM(kv_cache.shape, BF16),
            pltpu.VMEM(gathered.shape, BF16),
            pltpu.VMEM((kv_cols, kv_order.shape[1]), BF16),
            pltpu.SMEM(info.shape, jnp.int32),
            pltpu.SemaphoreType.DMA((slots,)),
            pltpu.SemaphoreType.DMA((3,)),
        ],
        out_shape=jax.ShapeDtypeStruct(send_shape, F32),
        compiler_params=pltpu.CompilerParams(vmem_limit_bytes=58 * 2**20),
        name="attend",
    )(info, gathered, kv_order[:kv_cols], kv_cache)
    parts = lax.all_to_all(sent, ("gx", "gy"), split_axis=0, concat_axis=0, tiled=True)
    scale_parts.append(output_scales(tile_counts[0], tile_counts[1], sent))
    parts, scale_parts[1] = lax.optimization_barrier((parts, scale_parts[1]))

    merged = pl.pallas_call(
        functools.partial(merge_kernel, row_count, per_target),
        in_specs=[
            pl.BlockSpec(memory_space=pltpu.SMEM),
            pl.BlockSpec(memory_space=pltpu.VMEM),
        ],
        out_specs=pl.BlockSpec(memory_space=pltpu.VMEM),
        out_shape=jax.ShapeDtypeStruct((size_y, row_count, per_target * HEAD_DIM), BF16),
        compiler_params=pltpu.CompilerParams(vmem_limit_bytes=8 * 2**20),
        name="merge",
    )(device[None], parts)
    attended = lax.all_to_all(merged, "gy", split_axis=0, concat_axis=0, tiled=True)

    own = row_count // size_x
    o_parts = pl.pallas_call(
        functools.partial(output_kernel, row_count, size_x, tile_counts),
        in_specs=[anywhere] * (4 + 3 * len(scale_parts)),
        out_specs=[vmem] * size_x,
        scratch_shapes=[
            *[pltpu.VMEM((row_count, count * COLS), F32) for count in tile_counts],
            *[pltpu.VMEM((low_rank, count * COLS), BF16) for count in tile_counts],
            pltpu.VMEM(attended.shape, BF16),
            pltpu.VMEM(join.shape, BF16),
            pltpu.VMEM((PAD_ROWS, in_rows), BF16),
            pltpu.VMEM((low_rank, in_rows), BF16),
            pltpu.VMEM((q_tiles, PAD_ROWS, COLS), F32),
            pltpu.VMEM((size_x, 2 * own, q_cols), F32),
            pltpu.VMEM((q_tiles, in_rows, COLS), BF16),
            pltpu.SemaphoreType.DMA((row_count,)),
            pltpu.SemaphoreType.DMA((q_tiles,)),
            pltpu.SemaphoreType.DMA((2 + 2 * len(scale_parts),)),
            *scalar_scratch,
        ],
        out_shape=[jax.ShapeDtypeStruct((2 * own, q_cols), F32)] * size_x,
        compiler_params=pltpu.CompilerParams(vmem_limit_bytes=56 * 2**20),
        name="output",
    )(
        tenant,
        attended,
        join,
        o_down,
        *[part[0] for part in scale_parts],
        *[part[1] for part in scale_parts],
        *[part[2] for part in scale_parts],
    )
    o_parts = exchange(o_parts, "gx", size_x)
    return pl.pallas_call(
        functools.partial(finish_kernel, row_count, size_x),
        grid_spec=pltpu.PrefetchScalarGridSpec(
            num_scalar_prefetch=1,
            grid=(1,),
            in_specs=[
                pl.BlockSpec((row_count, q_cols), lambda tile, ref: (0, lax.axis_index("gy"))),
                whole(o_magnitude.shape),
            ]
            + [whole((2 * own, q_cols))] * size_x,
            out_specs=whole((own, q_cols)),
        ),
        out_shape=jax.ShapeDtypeStruct((own, q_cols), BF16),
        compiler_params=pltpu.CompilerParams(vmem_limit_bytes=4 * 2**20),
        name="finish",
    )(scalars, hidden, o_magnitude, *o_parts)


def solution(mesh):
    in_specs = (
        P(),
        P(),
        P("gx", "gy"),
        P("gx", "gy"),
        P("gx", "gy"),
        P("gx", "gy"),
        P("gx", "gy"),
        P("gx", "gy"),
        P(None, "gx", None),
        P(None, None, "gy"),
        P(None, "gy"),
        P(None, "gx", None),
        P(None, None, "gy"),
        P(None, "gy"),
        P(),
        P(),
        P(),
        P(("gx", "gy"), None, None, None),
    )
    out_specs = P("gx", "gy")
    return jax.shard_map(local, mesh=mesh, in_specs=in_specs, out_specs=out_specs, check_vma=False)
```

```python
import functools
import math

import jax
import jax.numpy as jnp
import numpy as np
from jax import lax
from jax.experimental import pallas as pl
from jax.experimental.pallas import tpu as pltpu
from jax.sharding import PartitionSpec as P

HEADS = 128
KV_HEADS = 8
HEAD_DIM = 128
TENANTS = 8
RANK = 16
QBLOCK = 64
PAGE = 256

NF4_LEVELS = (
    -1.0,
    -0.6961928009986877,
    -0.5250730514526367,
    -0.39491748809814453,
    -0.28444138169288635,
    -0.18477343022833234,
    -0.09105003625154495,
    0.0,
    0.07958029955625534,
    0.16093020141124725,
    0.24611230194568634,
    0.33791524171829224,
    0.44070982933044434,
    0.5626170039176941,
    0.7229568362236023,
    1.0,
)
NORM_EPS = 1e-05
NEG_FILL = -1e30
ROPE_BASE = 500000.0
WORDS = 128
COLS = 2 * WORDS
CHUNK = 2048
PAD_ROWS = 16
DEPTH = 3
LANE_VECTORS = 2
F32 = jnp.float32
BF16 = jnp.bfloat16
GATHER_ROWS = lax.GatherDimensionNumbers(
    offset_dims=(),
    collapsed_slice_dims=(0,),
    start_index_map=(0,),
    operand_batching_dims=(1,),
    start_indices_batching_dims=(1,),
)


def level_table():
    levels = np.asarray(NF4_LEVELS, np.float32)
    down = np.broadcast_to(levels[:, None], (16, WORDS))
    across = np.broadcast_to(np.tile(levels, WORDS // 16)[None, :], (8, WORDS))
    return np.concatenate([down, across], 0)


def split_columns():
    matrix = np.zeros((COLS, COLS), np.float32)
    for column in range(COLS):
        matrix[column, column // 2 + WORDS * (column % 2)] = 1.0
    return matrix


def keyval_order(kv_columns, size_x):
    step = HEAD_DIM // 2 // size_x
    matrix = np.zeros((COLS, size_x * HEAD_DIM), np.float32)
    for column in range(kv_columns):
        head, inner = divmod(column, HEAD_DIM)
        half, turn = divmod(inner, HEAD_DIM // 2)
        piece, spot = divmod(turn, step)
        place = piece * HEAD_DIM + head * 2 * step + half * step + spot
        matrix[column, place] = 1.0
    return matrix


def dot(left, right):
    return jnp.dot(left, right, preferred_element_type=F32)


def dot_rows(left, right):
    return lax.dot_general(left, right, (((1,), (1,)), ((), ())), preferred_element_type=F32)


def three_parts(values):
    first = values.astype(BF16)
    rest = values - first.astype(F32)
    second = rest.astype(BF16)
    third = (rest - second.astype(F32)).astype(BF16)
    return first, second, third


def wide_dot(left, right):
    rows = left.shape[0]
    both = dot(jnp.concatenate(three_parts(left), 0), right)
    return (both[:rows] + both[rows : 2 * rows]) + both[2 * rows :]


def split_scales(absmax_ref, split_ref, scale_ref, first, tiles):
    rows = absmax_ref.shape[0]
    stacked = jnp.concatenate(
        [absmax_ref[:, COLS * tile : COLS * (tile + 1)] for tile in range(tiles)], 0
    )
    both = wide_dot(stacked, split_ref[...])
    for tile in range(tiles):
        scale_ref[first + tile] = both[rows * tile : rows * (tile + 1)]


def stack_tiles(array):
    return jnp.concatenate(
        [array[:, COLS * tile : COLS * (tile + 1)] for tile in range(array.shape[1] // COLS)], 0
    )


GATHER_LANES = lax.GatherDimensionNumbers(
    offset_dims=(),
    collapsed_slice_dims=(1,),
    start_index_map=(1,),
    operand_batching_dims=(0,),
    start_indices_batching_dims=(0,),
)


def pick_lanes(table, index):
    return lax.gather(
        table,
        index[..., None],
        GATHER_LANES,
        slice_sizes=(1, 1),
        mode=lax.GatherScatterMode.PROMISE_IN_BOUNDS,
    )


def pick_rows(table, index):
    return lax.gather(
        table,
        index[..., None],
        GATHER_ROWS,
        slice_sizes=(1, 1),
        mode=lax.GatherScatterMode.PROMISE_IN_BOUNDS,
    )


def weight_tile(codes_ref, scale_ref, level_ref, left_ref, store_ref, squared=True):
    in_rows = codes_ref.shape[0]
    chunk = min(CHUNK, in_rows)
    blocks = chunk // QBLOCK

    def visit(step, carry):
        total, squares = carry
        even_list = []
        odd_list = []
        for block in range(blocks):
            scale_row = scale_ref[pl.ds(step * blocks + block, 1), :]
            tables = [
                level_ref[8 * half : 8 * half + 8, :]
                * scale_row[:, WORDS * side : WORDS * side + WORDS]
                for side in range(2)
                for half in range(2)
            ]
            for row in range(0, QBLOCK, 8):
                word = codes_ref[pl.ds(step * chunk + block * QBLOCK + row, 8), :]
                if row < 8 * LANE_VECTORS:
                    across = level_ref[16:24, :]
                    even = pick_lanes(across, word & 15) * scale_row[:, :WORDS]
                    odd = pick_lanes(across, lax.shift_right_logical(word, 4)) * scale_row[:, WORDS:]
                else:
                    low = word & 7
                    even = jnp.where(
                        (word & 8) != 0, pick_rows(tables[1], low), pick_rows(tables[0], low)
                    )
                    high = lax.shift_right_logical(word, 4) & 7
                    odd = jnp.where(
                        word >= 128, pick_rows(tables[3], high), pick_rows(tables[2], high)
                    )
                even_list.append(even)
                odd_list.append(odd)
        weight = jnp.concatenate(
            [jnp.concatenate(even_list, 0), jnp.concatenate(odd_list, 0)], 1
        ).astype(BF16)
        start = pl.multiple_of(step * chunk, chunk)
        if store_ref is not None:
            store_ref[pl.ds(start, chunk), :] = weight
        total = total + dot(left_ref[:, pl.ds(start, chunk)], weight)
        if squared:
            squares = squares + dot(jnp.ones((PAD_ROWS, chunk), BF16), weight * weight)
        return (total, squares)

    return lax.fori_loop(
        0,
        in_rows // chunk,
        visit,
        (jnp.zeros((left_ref.shape[0], COLS), F32), jnp.zeros((PAD_ROWS, COLS), F32)),
    )


def block_mask(rows, columns, lead):
    row_id = lax.broadcasted_iota(jnp.int32, (rows, columns), 0)
    column_id = lax.broadcasted_iota(jnp.int32, (rows, columns), 1)
    owner = jnp.where(row_id < lead, row_id, lax.shift_right_logical(row_id - lead, 4))
    return owner == lax.shift_right_logical(column_id, 4)


def norm_terms(cross, gram, up_split, squares, row_count):
    inner = up_split * (2.0 * cross + gram)
    return squares + jnp.sum(
        inner.reshape(row_count, RANK, COLS), axis=1
    )


def code_copy(codes_ref, first, tile, buffer_ref, sems):
    columns = pl.ds(pl.multiple_of((first + tile) * WORDS, WORDS), WORDS)
    slot = tile % DEPTH if isinstance(tile, int) else lax.rem(tile, DEPTH)
    return pltpu.make_async_copy(codes_ref.at[:, columns], buffer_ref.at[slot], sems.at[slot])


def code_tile(codes_ref, first, tile, tiles, buffer_ref, sems):
    @pl.when(tile + DEPTH - 1 < tiles)
    def _():
        code_copy(codes_ref, first, tile + DEPTH - 1, buffer_ref, sems).start(priority=1)

    code_copy(codes_ref, first, tile, buffer_ref, sems).wait()
    return buffer_ref.at[lax.rem(tile, DEPTH)]


def fetch(sources, buffers, sems):
    copies = [
        pltpu.make_async_copy(source, buffer, sems.at[spot])
        for spot, (source, buffer) in enumerate(zip(sources, buffers))
    ]
    for copy in copies:
        copy.start(priority=0)
    return copies


def finish_all(copies):
    for copy in copies:
        copy.wait()


def read_scalars(source, buffer, sem):
    copy = pltpu.make_async_copy(source, buffer, sem)
    copy.start()
    return copy


def tenant_fetch(scalar_ref, row_count, source_ref, buffer_ref, lead, sems):
    return fetch(
        [source_ref.at[scalar_ref[row]] for row in range(row_count)],
        [
            buffer_ref.at[lead + RANK * row : lead + RANK * (row + 1), :]
            for row in range(row_count)
        ],
        sems,
    )


def query_kernel(
    row_count,
    size_x,
    tenant_hbm,
    hidden_hbm,
    gain_hbm,
    absmax_hbm,
    kv_absmax_hbm,
    level_hbm,
    split_hbm,
    join_hbm,
    kv_join_hbm,
    codes_ref,
    kv_codes_ref,
    down_ref,
    up_ref,
    *refs,
):
    outs = refs[:size_x]
    (
        hidden_ref,
        gain_ref,
        absmax_ref,
        kv_absmax_ref,
        level_ref,
        split_ref,
        join_ref,
        kv_join_ref,
        left_ref,
        scale_ref,
        total_ref,
        square_ref,
        chunk_ref,
        buffer_ref,
        kv_buffer_ref,
        ups_ref,
        code_sems,
        kv_sem,
        down_sems,
        up_sems,
        small_sems,
        scalar_ref,
        scalar_sem,
    ) = refs[size_x:]
    tiles = absmax_ref.shape[1] // COLS
    share = chunk_ref.shape[2] - HEAD_DIM
    low_rank = row_count * RANK
    here = lax.axis_index("gx")
    kv_copy = pltpu.make_async_copy(kv_codes_ref, kv_buffer_ref, kv_sem.at[0])
    scalars = read_scalars(tenant_hbm, scalar_ref, scalar_sem.at[0])
    kv_copy.start(priority=1)
    smalls = fetch(
        [
            split_hbm,
            kv_absmax_hbm,
            level_hbm,
            hidden_hbm,
            gain_hbm,
            absmax_hbm,
            kv_join_hbm,
            join_hbm,
        ],
        [
            split_ref,
            kv_absmax_ref,
            level_ref,
            hidden_ref,
            gain_ref,
            absmax_ref,
            kv_join_ref,
            join_ref,
        ],
        small_sems,
    )
    code_copy(codes_ref, 0, 0, buffer_ref, code_sems).start(priority=1)
    scalars.wait()
    downs = tenant_fetch(scalar_ref, row_count, down_ref, left_ref, PAD_ROWS, down_sems)
    finish_all(smalls[:5])
    states = hidden_ref[...].astype(F32)
    mean_square = jnp.mean(states * states, axis=1, keepdims=True)
    in_rows = left_ref.shape[1]
    own = pl.ds(pl.multiple_of(here * in_rows, in_rows), in_rows)
    normed = hidden_ref[:, own].astype(F32) * lax.rsqrt(mean_square + NORM_EPS) * gain_ref[:, own]
    left_ref[0:PAD_ROWS, :] = jnp.concatenate(
        [normed, jnp.zeros((PAD_ROWS - row_count, normed.shape[1]), F32)], 0
    ).astype(BF16)
    split_scales(kv_absmax_ref, split_ref, scale_ref, 0, 1)
    kv_copy.wait()
    for tile in range(1, min(DEPTH - 1, tiles)):
        code_copy(codes_ref, 0, tile, buffer_ref, code_sems).start(priority=1)
    total, _ = weight_tile(
        kv_buffer_ref, scale_ref.at[0], level_ref, left_ref.at[0:PAD_ROWS, :], None, False
    )
    finish_all(smalls[5:])
    split_scales(absmax_ref, split_ref, scale_ref, 1, tiles)
    joined = wide_dot(total, kv_join_ref[...])
    for owner in range(size_x):
        chunk_ref[owner, :, share:] = joined[
            : 2 * row_count, owner * HEAD_DIM : (owner + 1) * HEAD_DIM
        ]
    ups = tenant_fetch(scalar_ref, row_count, up_ref, ups_ref, 0, up_sems)
    finish_all(downs)

    def visit(tile, carry):
        codes = code_tile(codes_ref, 0, tile, tiles, buffer_ref, code_sems)
        total, squares = weight_tile(codes, scale_ref.at[tile + 1], level_ref, left_ref, None)
        total_ref[tile] = total
        square_ref[tile] = squares[0:8]
        return carry

    lax.fori_loop(0, tiles, visit, 0)
    finish_all(ups)
    gram = dot_rows(left_ref[...], left_ref[PAD_ROWS:, :])
    gram = jnp.where(block_mask(*gram.shape, PAD_ROWS), gram, 0.0)
    up_split = dot(stack_tiles(ups_ref[...]), split_ref[...])
    lines = []
    for tile in range(tiles):
        up_tile = up_split[low_rank * tile : low_rank * (tile + 1)]
        extra = wide_dot(gram, up_tile.astype(BF16))
        total = total_ref[tile]
        lines.append(total[:row_count] + extra[:row_count])
        lines.append(
            norm_terms(
                total[PAD_ROWS:], extra[PAD_ROWS:], up_tile, square_ref[tile, 0:1], row_count
            )
        )
    joined = wide_dot(jnp.concatenate(lines, 0), join_ref[...])
    piece = min(COLS, share)
    for tile in range(tiles):
        for part in range(COLS // piece):
            owner, place = divmod(tile * COLS + part * piece, share)
            chunk_ref[owner, :, place : place + piece] = joined[
                2 * row_count * tile : 2 * row_count * (tile + 1),
                part * piece : (part + 1) * piece,
            ]
    for shift in range(size_x):
        outs[shift][...] = chunk_ref[lax.rem(here + shift, size_x)]


def store_copy(store_ref, slot, weight_ref, tile, sems):
    return pltpu.make_async_copy(store_ref.at[slot], weight_ref.at[tile], sems.at[slot])


def output_scale_kernel(
    row_count,
    first,
    tenant_hbm,
    absmax_hbm,
    level_hbm,
    split_hbm,
    join_hbm,
    codes_ref,
    down_ref,
    up_ref,
    norm_ref,
    up_split_ref,
    weight_ref,
    absmax_ref,
    level_ref,
    split_ref,
    join_ref,
    store_ref,
    left_ref,
    scale_ref,
    total_ref,
    square_ref,
    buffer_ref,
    ups_ref,
    code_sems,
    down_sems,
    up_sems,
    store_sems,
    small_sems,
    scalar_ref,
    scalar_sem,
):
    scalars = read_scalars(tenant_hbm, scalar_ref, scalar_sem.at[0])
    tiles = weight_ref.shape[0]
    low_rank = row_count * RANK
    columns = slice(first * COLS, (first + tiles) * COLS)
    code_copy(codes_ref, first, 0, buffer_ref, code_sems).start(priority=1)
    smalls = fetch(
        [split_hbm, absmax_hbm.at[:, columns], level_hbm, join_hbm],
        [split_ref, absmax_ref, level_ref, join_ref],
        small_sems,
    )
    scalars.wait()
    downs = tenant_fetch(scalar_ref, row_count, down_ref, left_ref, 0, down_sems)
    for tile in range(1, min(DEPTH - 1, tiles)):
        code_copy(codes_ref, first, tile, buffer_ref, code_sems).start(priority=1)
    ups = tenant_fetch(
        scalar_ref, row_count, up_ref.at[:, :, columns], ups_ref, 0, up_sems
    )
    finish_all(smalls)
    split_scales(absmax_ref, split_ref, scale_ref, 0, tiles)
    finish_all(downs)

    def visit(tile, carry):
        codes = code_tile(codes_ref, first, tile, tiles, buffer_ref, code_sems)
        slot = lax.rem(tile, 2)

        @pl.when(tile >= 2)
        def _():
            store_copy(store_ref, slot, weight_ref, tile - 2, store_sems).wait()

        total, squares = weight_tile(
            codes, scale_ref.at[tile], level_ref, left_ref, store_ref.at[slot]
        )
        store_copy(store_ref, slot, weight_ref, tile, store_sems).start()
        total_ref[tile] = total
        square_ref[tile] = squares[0:8]
        return carry

    lax.fori_loop(0, tiles, visit, 0)
    finish_all(ups)
    gram = dot_rows(left_ref[...], left_ref[...])
    gram = jnp.where(block_mask(*gram.shape, 0), gram, 0.0)
    up_split = dot(stack_tiles(ups_ref[...]), split_ref[...])
    lines = []
    for tile in range(tiles):
        up_tile = up_split[low_rank * tile : low_rank * (tile + 1)]
        narrow = up_tile.astype(BF16)
        up_split_ref[:, COLS * tile : COLS * (tile + 1)] = narrow
        extra = wide_dot(gram, narrow)
        lines.append(norm_terms(total_ref[tile], extra, up_tile, square_ref[tile, 0:1], row_count))
    joined = wide_dot(jnp.concatenate(lines, 0), join_ref[...])
    for tile in range(tiles):
        norm_ref[:, COLS * tile : COLS * (tile + 1)] = joined[
            row_count * tile : row_count * (tile + 1)
        ]
    for tile in range(max(tiles - 2, 0), tiles):
        store_copy(store_ref, tile % 2, weight_ref, tile, store_sems).wait()


def rotate_kernel(row_count, size_x, step, scalar_ref, magnitude_ref, cos_ref, sin_ref, *refs):
    parts = refs[:size_x]
    out_ref = refs[size_x]
    share = cos_ref.shape[1] - HEAD_DIM
    total = parts[0][...]
    for part in parts[1:]:
        total = total + part[...]
    magnitude = jnp.concatenate(
        [
            magnitude_ref[pl.ds(scalar_ref[row], 1), :]
            for row in range(row_count)
        ],
        0,
    )
    query = total[:row_count, :share] * (
        magnitude * lax.rsqrt(total[row_count:, :share])
    )
    keyval = total[:row_count, share:]
    half = HEAD_DIM // 2
    pieces = []
    for head in range(share // HEAD_DIM):
        block = query[:, head * HEAD_DIM : (head + 1) * HEAD_DIM]
        pieces.append(pltpu.roll(block, half, 1))
    lane = lax.broadcasted_iota(jnp.int32, keyval.shape, 1)
    other = jnp.where(
        (lane & step) != 0, pltpu.roll(keyval, step, 1), pltpu.roll(keyval, HEAD_DIM - step, 1)
    )
    values = jnp.concatenate([query, keyval], 1)
    partner = jnp.concatenate(pieces + [other], 1)
    turned = (values * cos_ref[...] + partner * sin_ref[...]).astype(BF16)
    for target in range(out_ref.shape[0]):
        out_ref[target] = turned


def attend_kernel(
    row_count,
    size_x,
    size_y,
    owner_hbm,
    filled_hbm,
    gathered_hbm,
    kv_order_hbm,
    pages_ref,
    send_ref,
    query_ref,
    mixed_ref,
    best_ref,
    total_ref,
    value_ref,
    held_ref,
    gathered_ref,
    kv_order_ref,
    owner_ref,
    filled_ref,
    page_sems,
    small_sems,
):
    slots = pages_ref.shape[0]

    def page_copy(slot):
        return pltpu.make_async_copy(pages_ref.at[slot], held_ref.at[slot], page_sems.at[slot])

    smalls = fetch(
        [owner_hbm, filled_hbm, gathered_hbm, kv_order_hbm],
        [owner_ref, filled_ref, gathered_ref, kv_order_ref],
        small_sems,
    )
    ahead = min(4, slots)
    for slot in range(ahead):
        page_copy(slot).start(priority=1)
    finish_all(smalls)
    devices = size_x * size_y
    per_target = HEADS // devices
    group = HEADS // KV_HEADS
    inv_root = 1.0 / math.sqrt(HEAD_DIM)
    used = sum((filled_ref[slot] > 0).astype(jnp.int32) for slot in range(slots))
    device = lax.axis_index("gx") * size_y + lax.axis_index("gy")
    share = gathered_ref.shape[2] - HEAD_DIM

    def setup():
        heads_here = share // HEAD_DIM
        for place_x in range(size_x):
            for place_y in range(size_y):
                block = gathered_ref[place_x * size_y + place_y].astype(F32)
                for head in range(heads_here):
                    first = (place_y * size_x + place_x) * heads_here + head
                    query_ref[pl.ds(first, row_count, stride=HEADS), :] = block[
                        :, head * HEAD_DIM : (head + 1) * HEAD_DIM
                    ]
                mixed_ref[place_x, place_y * row_count : (place_y + 1) * row_count, :] = block[
                    :, share:
                ]
        best_ref[...] = jnp.full(best_ref.shape, NEG_FILL, F32)
        total_ref[...] = jnp.zeros(total_ref.shape, F32)
        value_ref[...] = jnp.zeros(value_ref.shape, F32)

        @pl.when(device < row_count)
        def _():
            columns = kv_order_ref.shape[0]
            plain = jnp.zeros((size_y * row_count, columns), F32)
            for place_x in range(size_x):
                plain = plain + dot_rows(
                    mixed_ref[place_x].astype(BF16),
                    kv_order_ref[:, place_x * HEAD_DIM : (place_x + 1) * HEAD_DIM],
                )
            heads_each = 2 * KV_HEADS // size_y
            for row in range(row_count):

                @pl.when(device == row)
                def _():
                    rows = []
                    for head in range(2 * KV_HEADS):
                        place_y, inner = divmod(head, heads_each)
                        line = place_y * row_count + row
                        one = plain[line : line + 1, inner * HEAD_DIM : (inner + 1) * HEAD_DIM]
                        rows.append(jnp.broadcast_to(one, (group, HEAD_DIM)))
                    new_keys = jnp.concatenate(rows[:KV_HEADS], 0)
                    new_values = jnp.concatenate(rows[KV_HEADS:], 0)
                    span = slice(row * HEADS, (row + 1) * HEADS)
                    score = jnp.sum(query_ref[span, :] * new_keys, 1, keepdims=True) * inv_root
                    best_ref[span, :] = jnp.broadcast_to(score, (HEADS, HEAD_DIM))
                    total_ref[span, :] = jnp.ones((HEADS, HEAD_DIM), F32)
                    value_ref[span, :] = new_values

    setup()

    def page_terms(slot, count):
        start = pl.multiple_of(owner_ref[slot] * HEADS, HEADS)
        query = query_ref[pl.ds(start, HEADS), :].astype(BF16)
        scores = jnp.concatenate(
            [
                dot_rows(
                    query[group * head : group * (head + 1), :],
                    held_ref[slot, 0, :, head * HEAD_DIM : (head + 1) * HEAD_DIM],
                )
                for head in range(KV_HEADS)
            ],
            0,
        )
        inside = lax.broadcasted_iota(jnp.int32, (HEADS, PAGE), 1) < count
        scores = jnp.where(inside, scores * inv_root, NEG_FILL)
        peak = jnp.max(scores, axis=1, keepdims=True)
        weights = jnp.where(inside, jnp.exp(scores - peak), 0.0)
        coarse = weights.astype(BF16)
        fine = (weights - coarse.astype(F32)).astype(BF16)
        gains = []
        for head in range(KV_HEADS):
            rows = slice(group * head, group * (head + 1))
            both = dot(
                jnp.concatenate([coarse[rows], fine[rows]], 0),
                held_ref[slot, 1, :, head * HEAD_DIM : (head + 1) * HEAD_DIM],
            )
            gains.append(both[:group] + both[group:])
        return start, peak, jnp.sum(weights, axis=1, keepdims=True), jnp.concatenate(gains, 0)

    def add_terms(start, peak, amount, gain):
        span = pl.ds(start, HEADS)
        old_best = best_ref[span, :]
        best = jnp.maximum(old_best, peak)
        keep = jnp.exp(old_best - best)
        take = jnp.exp(peak - best)
        best_ref[span, :] = best
        total_ref[span, :] = total_ref[span, :] * keep + amount * take
        value_ref[span, :] = value_ref[span, :] * keep + gain * take

    def visit(pair, carry):
        first = 2 * pair
        second = jnp.minimum(first + 1, used - 1)
        for slot in (first, first + 1):

            @pl.when(slot + ahead < used)
            def _(slot=slot):
                page_copy(slot + ahead).start(priority=1)

        page_copy(first).wait()

        @pl.when(first + 1 < used)
        def _():
            page_copy(second).wait()

        terms = [
            page_terms(first, filled_ref[first]),
            page_terms(second, jnp.where(first + 1 < used, filled_ref[second], 0)),
        ]
        for term in terms:
            add_terms(*term)
        return carry

    lax.fori_loop(0, (used + 1) // 2, visit, 0)
    for slot in range(ahead):

        @pl.when(slot >= used)
        def _(slot=slot):
            page_copy(slot).wait()


    def close():
        eye = lax.broadcasted_iota(jnp.int32, (HEADS, HEAD_DIM), 0) == lax.broadcasted_iota(
            jnp.int32, (HEADS, HEAD_DIM), 1
        )
        lines = []
        for source in (best_ref, total_ref):
            for row in range(row_count):
                block = source[row * HEADS : (row + 1) * HEADS, :]
                lines.append(jnp.sum(jnp.where(eye, block, 0.0), axis=0, keepdims=True))
        scalars = jnp.concatenate(lines, 0)
        for target in range(devices):
            for row in range(row_count):
                begin = row * HEADS + target * per_target
                send_ref[target, row * per_target : (row + 1) * per_target, :] = value_ref[
                    begin : begin + per_target, :
                ]
            send_ref[target, row_count * per_target :, :] = scalars

    close()


def merge_kernel(row_count, per_target, info_ref, parts_ref, out_ref):
    offset = info_ref[0] * per_target
    values = parts_ref[:, : row_count * per_target, :]
    scalars = parts_ref[:, row_count * per_target :, :]
    lane = lax.broadcasted_iota(jnp.int32, scalars.shape, 2)
    for row in range(row_count):
        for head in range(per_target):
            chosen = jnp.sum(jnp.where(lane == offset + head, scalars, 0.0), axis=2, keepdims=True)
            best = chosen[:, row : row + 1, :]
            total = chosen[:, row_count + row : row_count + row + 1, :]
            factor = jnp.exp(best - jnp.max(best, axis=0, keepdims=True))
            line = row * per_target + head
            top = jnp.sum(values[:, line : line + 1, :] * factor, axis=0)
            bottom = jnp.sum(total * factor, axis=0)
            ratio = (top / bottom).astype(BF16)
            for target in range(out_ref.shape[0]):
                out_ref[target, row : row + 1, head * HEAD_DIM : (head + 1) * HEAD_DIM] = ratio


def output_kernel(
    row_count,
    size_x,
    tile_counts,
    tenant_hbm,
    attended_hbm,
    join_hbm,
    down_ref,
    *refs,
):
    parts = len(tile_counts)
    norms_hbm = refs[:parts]
    ups_hbm = refs[parts : 2 * parts]
    weights = refs[2 * parts : 3 * parts]
    outs = refs[3 * parts : 3 * parts + size_x]
    refs = refs[3 * parts + size_x :]
    norms = refs[:parts]
    splits = refs[parts : 2 * parts]
    (
        attended_ref,
        join_ref,
        left_ref,
        low_ref,
        total_ref,
        chunk_ref,
        held_ref,
        down_sems,
        held_sems,
        small_sems,
        scalar_ref,
        scalar_sem,
    ) = refs[2 * parts :]
    tiles = sum(tile_counts)
    own = row_count // size_x
    scalars = read_scalars(tenant_hbm, scalar_ref, scalar_sem.at[0])
    smalls = fetch(
        [attended_hbm, join_hbm] + list(norms_hbm) + list(ups_hbm),
        [attended_ref, join_ref] + list(norms) + list(splits),
        small_sems,
    )
    loads = [
        pltpu.make_async_copy(
            weights[part].at[tile],
            held_ref.at[sum(tile_counts[:part]) + tile],
            held_sems.at[sum(tile_counts[:part]) + tile],
        )
        for part in range(parts)
        for tile in range(tile_counts[part])
    ]
    scalars.wait()
    downs = tenant_fetch(scalar_ref, row_count, down_ref, low_ref, 0, down_sems)
    for load in loads:
        load.start(priority=1)
    smalls[0].wait()
    width = attended_ref.shape[2]
    for part in range(attended_ref.shape[0]):
        block = attended_ref[part].astype(F32)
        left_ref[:, part * width : (part + 1) * width] = jnp.concatenate(
            [block, jnp.zeros((PAD_ROWS - row_count, width), F32)], 0
        ).astype(BF16)
    finish_all(downs)
    finish_all(smalls[1:])
    middle = dot_rows(left_ref[...], low_ref[...])
    middle = jnp.where(block_mask(*middle.shape, PAD_ROWS), middle, 0.0)
    extras = [wide_dot(middle, up[...]) for up in splits]
    numbers = []
    for part in range(parts):
        for tile in range(tile_counts[part]):
            spot = len(numbers)
            loads[spot].wait()
            total_ref[spot] = dot(left_ref[...], held_ref[spot]) + extras[part][
                :, COLS * tile : COLS * (tile + 1)
            ]
            numbers.append(total_ref[spot, 0:row_count])
    joined = wide_dot(jnp.concatenate(numbers, 0), join_ref[...])
    for owner in range(size_x):
        for spot in range(tiles):
            begin = row_count * spot + owner * own
            chunk_ref[owner, 0:own, COLS * spot : COLS * (spot + 1)] = joined[begin : begin + own]
        for part in range(parts):
            begin = COLS * sum(tile_counts[:part])
            chunk_ref[owner, own : 2 * own, begin : begin + COLS * tile_counts[part]] = norms[
                part
            ][owner * own : (owner + 1) * own, :]
    here = lax.axis_index("gx")
    for shift in range(size_x):
        outs[shift][...] = chunk_ref[lax.rem(here + shift, size_x)]


def finish_kernel(row_count, size_x, scalar_ref, hidden_ref, magnitude_ref, *refs):
    parts = refs[:size_x]
    out_ref = refs[size_x]
    own = row_count // size_x
    total = parts[0][...]
    for part in parts[1:]:
        total = total + part[...]
    here = lax.axis_index("gx")
    states = hidden_ref[...].astype(F32)
    row_id = lax.broadcasted_iota(jnp.int32, states.shape, 0)
    for line in range(own):
        row = here * own + line
        state = jnp.sum(jnp.where(row_id == row, states, 0.0), axis=0, keepdims=True)
        magnitude = magnitude_ref[pl.ds(scalar_ref[row], 1), :]
        scale = magnitude * lax.rsqrt(total[own + line : own + line + 1])
        out_ref[line : line + 1, :] = (state + total[line : line + 1] * scale).astype(BF16)


def slot_info(page_table, lengths, device, slot_count):
    row_count, page_limit = page_table.shape
    page_need = (lengths + PAGE - 1) // PAGE
    page_numbers = jnp.arange(page_limit, dtype=jnp.int32)
    live_mask = page_numbers[None, :] < page_need[:, None]
    wanted = device * slot_count + jnp.arange(slot_count, dtype=jnp.int32)
    hits = ((page_table[None, :, :] == wanted[:, None, None]) & live_mask[None, :, :]).astype(
        jnp.int32
    )
    owner_row = jnp.sum(hits * jnp.arange(row_count, dtype=jnp.int32)[None, :, None], axis=(1, 2))
    remaining = jnp.clip(lengths[:, None] - page_numbers[None, :] * PAGE, 0, PAGE)
    filled = jnp.sum(hits * remaining[None, :, :], axis=(1, 2))
    return owner_row, filled


def exchange(parts, axis, size):
    received = [parts[0]]
    for shift in range(1, size):
        received.append(
            lax.ppermute(parts[shift], axis, [(spot, (spot + shift) % size) for spot in range(size)])
        )
    return received


def whole(shape):
    return pl.BlockSpec(shape, lambda *_: (0,) * len(shape))


def local(
    hidden,
    norm_gain,
    q_codes,
    q_absmax,
    kv_codes,
    kv_absmax,
    o_codes,
    o_absmax,
    q_down,
    q_up,
    q_magnitude,
    o_down,
    o_up,
    o_magnitude,
    tenant,
    lengths,
    page_table,
    kv_cache,
):
    row_count, width = hidden.shape
    row_x = lax.axis_index("gx").astype(jnp.int32)
    col_y = lax.axis_index("gy").astype(jnp.int32)
    size_x = lax.axis_size("gx")
    size_y = lax.axis_size("gy")
    devices = size_x * size_y
    device = row_x * size_y + col_y
    in_rows, q_words = q_codes.shape
    q_cols = 2 * q_words
    share = q_cols // size_x
    kv_cols = 2 * kv_codes.shape[1]
    if kv_cols < COLS:
        kv_codes = jnp.pad(kv_codes, ((0, 0), (0, WORDS - kv_codes.shape[1])))
        kv_absmax = jnp.pad(kv_absmax, ((0, 0), (0, COLS - kv_cols)))
    low_rank = row_count * RANK
    level = jnp.asarray(level_table())
    split_matrix = split_columns()
    split = jnp.asarray(split_matrix, BF16)
    join = jnp.asarray(split_matrix.T, BF16)
    order = keyval_order(kv_cols, size_x)
    kv_join = jnp.asarray(split_matrix.T @ order, BF16)
    kv_order = jnp.asarray(order, BF16)
    scalars = tenant
    q_down = jnp.swapaxes(q_down, 1, 2)
    o_down = jnp.swapaxes(o_down, 1, 2)
    q_tiles = q_words // WORDS
    scale_rows = in_rows // QBLOCK

    smem = pl.BlockSpec(memory_space=pltpu.SMEM)
    vmem = pl.BlockSpec(memory_space=pltpu.VMEM)
    anywhere = pl.BlockSpec(memory_space=pltpu.HBM)
    chunk_shape = (2 * row_count, share + HEAD_DIM)
    scalar_scratch = [pltpu.SMEM((row_count,), jnp.int32), pltpu.SemaphoreType.DMA((1,))]
    small = [
        pltpu.VMEM((scale_rows, q_cols), F32),
        pltpu.VMEM((scale_rows, COLS), F32),
        pltpu.VMEM(level.shape, F32),
        pltpu.VMEM(split.shape, BF16),
        pltpu.VMEM(join.shape, BF16),
    ]
    q_parts = pl.pallas_call(
        functools.partial(query_kernel, row_count, size_x),
        in_specs=[anywhere] * 13,
        out_specs=[vmem] * size_x,
        scratch_shapes=[
            pltpu.VMEM((row_count, width), BF16),
            pltpu.VMEM((1, width), F32),
            *small,
            pltpu.VMEM(kv_join.shape, BF16),
            pltpu.VMEM((PAD_ROWS + low_rank, in_rows), BF16),
            pltpu.VMEM((q_tiles + 1, scale_rows, COLS), F32),
            pltpu.VMEM((q_tiles, PAD_ROWS + low_rank, COLS), F32),
            pltpu.VMEM((q_tiles, 8, COLS), F32),
            pltpu.VMEM((size_x,) + chunk_shape, F32),
            pltpu.VMEM((DEPTH, in_rows, WORDS), jnp.int32),
            pltpu.VMEM((in_rows, WORDS), jnp.int32),
            pltpu.VMEM((low_rank, q_cols), BF16),
            pltpu.SemaphoreType.DMA((DEPTH,)),
            pltpu.SemaphoreType.DMA((1,)),
            pltpu.SemaphoreType.DMA((row_count,)),
            pltpu.SemaphoreType.DMA((row_count,)),
            pltpu.SemaphoreType.DMA((8,)),
            *scalar_scratch,
        ],
        out_shape=[jax.ShapeDtypeStruct(chunk_shape, F32)] * size_x,
        name="query",
    )(
        tenant,
        hidden,
        norm_gain[None, :],
        q_absmax,
        kv_absmax,
        level,
        split,
        join,
        kv_join,
        q_codes,
        kv_codes,
        q_down,
        q_up,
    )
    q_parts = exchange(q_parts, "gx", size_x)

    def output_scales(first, tiles, after):
        owners, _ = lax.optimization_barrier((tenant, after))
        return pl.pallas_call(
            functools.partial(output_scale_kernel, row_count, first),
            in_specs=[anywhere] * 8,
            out_specs=[vmem, vmem, anywhere],
            scratch_shapes=[
                pltpu.VMEM((scale_rows, tiles * COLS), F32),
                *small[2:],
                pltpu.VMEM((2, in_rows, COLS), BF16),
                pltpu.VMEM((low_rank, in_rows), BF16),
                pltpu.VMEM((tiles, scale_rows, COLS), F32),
                pltpu.VMEM((tiles, low_rank, COLS), F32),
                pltpu.VMEM((tiles, 8, COLS), F32),
                pltpu.VMEM((DEPTH, in_rows, WORDS), jnp.int32),
                pltpu.VMEM((low_rank, tiles * COLS), BF16),
                pltpu.SemaphoreType.DMA((DEPTH,)),
                pltpu.SemaphoreType.DMA((row_count,)),
                pltpu.SemaphoreType.DMA((row_count,)),
                pltpu.SemaphoreType.DMA((2,)),
                pltpu.SemaphoreType.DMA((4,)),
                *scalar_scratch,
            ],
            out_shape=[
                jax.ShapeDtypeStruct((row_count, tiles * COLS), F32),
                jax.ShapeDtypeStruct((low_rank, tiles * COLS), BF16),
                pltpu.HBM((tiles, in_rows, COLS), BF16),
            ],
            compiler_params=pltpu.CompilerParams(vmem_limit_bytes=56 * 2**20),
            cost_estimate=pl.CostEstimate(
                flops=tiles * 5_000_000 * 256,
                bytes_accessed=tiles * 8 * in_rows * WORDS,
                transcendentals=0,
            ),
            name="output_scale",
        )(owners, o_absmax, level, split, join, o_codes, o_down, o_up)

    tile_counts = [3 * q_tiles // 8, q_tiles - 3 * q_tiles // 8]

    half = HEAD_DIM // 2
    step = half // size_x
    lane = jnp.arange(share + HEAD_DIM, dtype=jnp.int32)
    in_query = lane < share
    turn = jnp.where(in_query, lane % half, row_x * step + lane % step)
    second = jnp.where(in_query, lane % HEAD_DIM // half, lane % (2 * step) // step)
    frequency = ROPE_BASE ** (-2.0 * turn.astype(F32) / HEAD_DIM)
    angles = lengths.astype(F32)[:, None] * frequency[None, :]
    plain = jnp.logical_and(~in_query, col_y * kv_cols >= KV_HEADS * HEAD_DIM)[None, :]
    cosine = jnp.where(plain, 1.0, jnp.cos(angles))
    sine = jnp.sin(angles)
    sine = jnp.where(plain, 0.0, jnp.where(second[None, :] == 1, sine, -sine))

    query_all = pl.pallas_call(
        functools.partial(rotate_kernel, row_count, size_x, step),
        grid_spec=pltpu.PrefetchScalarGridSpec(
            num_scalar_prefetch=1,
            grid=(1,),
            in_specs=[
                pl.BlockSpec((TENANTS, share), lambda tile, ref: (0, lax.axis_index("gx"))),
                whole(cosine.shape),
                whole(sine.shape),
            ]
            + [whole(chunk_shape)] * size_x,
            out_specs=whole((devices, row_count, share + HEAD_DIM)),
        ),
        out_shape=jax.ShapeDtypeStruct((devices, row_count, share + HEAD_DIM), BF16),
        compiler_params=pltpu.CompilerParams(vmem_limit_bytes=8 * 2**20),
        name="rotate",
    )(scalars, q_magnitude, cosine, sine, *q_parts)
    gathered = lax.all_to_all(query_all, ("gx", "gy"), split_axis=0, concat_axis=0, tiled=True)
    scale_parts = [output_scales(0, tile_counts[0], query_all)]
    gathered, scale_parts[0] = lax.optimization_barrier((gathered, scale_parts[0]))

    slots = kv_cache.shape[0]
    owner_row, filled = slot_info(page_table, lengths, device, slots)
    per_target = HEADS // devices
    send_shape = (devices, row_count * per_target + 2 * row_count, HEAD_DIM)
    sent = pl.pallas_call(
        functools.partial(attend_kernel, row_count, size_x, size_y),
        in_specs=[anywhere] * 5,
        out_specs=vmem,
        scratch_shapes=[
            pltpu.VMEM((row_count * HEADS, HEAD_DIM), F32),
            pltpu.VMEM((size_x, size_y * row_count, HEAD_DIM), F32),
            pltpu.VMEM((row_count * HEADS, HEAD_DIM), F32),
            pltpu.VMEM((row_count * HEADS, HEAD_DIM), F32),
            pltpu.VMEM((row_count * HEADS, HEAD_DIM), F32),
            pltpu.VMEM(kv_cache.shape, BF16),
            pltpu.VMEM(gathered.shape, BF16),
            pltpu.VMEM((kv_cols, kv_order.shape[1]), BF16),
            pltpu.SMEM((slots,), jnp.int32),
            pltpu.SMEM((slots,), jnp.int32),
            pltpu.SemaphoreType.DMA((slots,)),
            pltpu.SemaphoreType.DMA((4,)),
        ],
        out_shape=jax.ShapeDtypeStruct(send_shape, F32),
        compiler_params=pltpu.CompilerParams(vmem_limit_bytes=58 * 2**20),
        name="attend",
    )(owner_row, filled, gathered, kv_order[:kv_cols], kv_cache)
    parts = lax.all_to_all(sent, ("gx", "gy"), split_axis=0, concat_axis=0, tiled=True)
    scale_parts.append(output_scales(tile_counts[0], tile_counts[1], sent))
    parts, scale_parts[1] = lax.optimization_barrier((parts, scale_parts[1]))

    merged = pl.pallas_call(
        functools.partial(merge_kernel, row_count, per_target),
        in_specs=[
            pl.BlockSpec(memory_space=pltpu.SMEM),
            pl.BlockSpec(memory_space=pltpu.VMEM),
        ],
        out_specs=pl.BlockSpec(memory_space=pltpu.VMEM),
        out_shape=jax.ShapeDtypeStruct((size_y, row_count, per_target * HEAD_DIM), BF16),
        compiler_params=pltpu.CompilerParams(vmem_limit_bytes=8 * 2**20),
        name="merge",
    )(device[None], parts)
    attended = lax.all_to_all(merged, "gy", split_axis=0, concat_axis=0, tiled=True)

    own = row_count // size_x
    o_parts = pl.pallas_call(
        functools.partial(output_kernel, row_count, size_x, tile_counts),
        in_specs=[anywhere] * (4 + 3 * len(scale_parts)),
        out_specs=[vmem] * size_x,
        scratch_shapes=[
            *[pltpu.VMEM((row_count, count * COLS), F32) for count in tile_counts],
            *[pltpu.VMEM((low_rank, count * COLS), BF16) for count in tile_counts],
            pltpu.VMEM(attended.shape, BF16),
            pltpu.VMEM(join.shape, BF16),
            pltpu.VMEM((PAD_ROWS, in_rows), BF16),
            pltpu.VMEM((low_rank, in_rows), BF16),
            pltpu.VMEM((q_tiles, PAD_ROWS, COLS), F32),
            pltpu.VMEM((size_x, 2 * own, q_cols), F32),
            pltpu.VMEM((q_tiles, in_rows, COLS), BF16),
            pltpu.SemaphoreType.DMA((row_count,)),
            pltpu.SemaphoreType.DMA((q_tiles,)),
            pltpu.SemaphoreType.DMA((2 + 2 * len(scale_parts),)),
            *scalar_scratch,
        ],
        out_shape=[jax.ShapeDtypeStruct((2 * own, q_cols), F32)] * size_x,
        compiler_params=pltpu.CompilerParams(vmem_limit_bytes=56 * 2**20),
        name="output",
    )(
        tenant,
        attended,
        join,
        o_down,
        *[part[0] for part in scale_parts],
        *[part[1] for part in scale_parts],
        *[part[2] for part in scale_parts],
    )
    o_parts = exchange(o_parts, "gx", size_x)
    return pl.pallas_call(
        functools.partial(finish_kernel, row_count, size_x),
        grid_spec=pltpu.PrefetchScalarGridSpec(
            num_scalar_prefetch=1,
            grid=(1,),
            in_specs=[
                pl.BlockSpec((row_count, q_cols), lambda tile, ref: (0, lax.axis_index("gy"))),
                whole(o_magnitude.shape),
            ]
            + [whole((2 * own, q_cols))] * size_x,
            out_specs=whole((own, q_cols)),
        ),
        out_shape=jax.ShapeDtypeStruct((own, q_cols), BF16),
        compiler_params=pltpu.CompilerParams(vmem_limit_bytes=4 * 2**20),
        name="finish",
    )(scalars, hidden, o_magnitude, *o_parts)


def solution(mesh):
    in_specs = (
        P(),
        P(),
        P("gx", "gy"),
        P("gx", "gy"),
        P("gx", "gy"),
        P("gx", "gy"),
        P("gx", "gy"),
        P("gx", "gy"),
        P(None, "gx", None),
        P(None, None, "gy"),
        P(None, "gy"),
        P(None, "gx", None),
        P(None, None, "gy"),
        P(None, "gy"),
        P(),
        P(),
        P(),
        P(("gx", "gy"), None, None, None),
    )
    out_specs = P("gx", "gy")
    return jax.shard_map(local, mesh=mesh, in_specs=in_specs, out_specs=out_specs, check_vma=False)
```

```python
import functools
import math

import jax
import jax.numpy as jnp
import numpy as np
from jax import lax
from jax.experimental import pallas as pl
from jax.experimental.pallas import tpu as pltpu
from jax.sharding import PartitionSpec as P

HEADS = 128
KV_HEADS = 8
HEAD_DIM = 128
TENANTS = 8
RANK = 16
QBLOCK = 64
PAGE = 256

NF4_LEVELS = (
    -1.0,
    -0.6961928009986877,
    -0.5250730514526367,
    -0.39491748809814453,
    -0.28444138169288635,
    -0.18477343022833234,
    -0.09105003625154495,
    0.0,
    0.07958029955625534,
    0.16093020141124725,
    0.24611230194568634,
    0.33791524171829224,
    0.44070982933044434,
    0.5626170039176941,
    0.7229568362236023,
    1.0,
)
NORM_EPS = 1e-05
NEG_FILL = -1e30
ROPE_BASE = 500000.0
WORDS = 128
COLS = 2 * WORDS
CHUNK = 2048
PAD_ROWS = 16
DEPTH = 3
LANE_VECTORS = 2
F32 = jnp.float32
BF16 = jnp.bfloat16
GATHER_ROWS = lax.GatherDimensionNumbers(
    offset_dims=(),
    collapsed_slice_dims=(0,),
    start_index_map=(0,),
    operand_batching_dims=(1,),
    start_indices_batching_dims=(1,),
)


def level_table():
    levels = np.asarray(NF4_LEVELS, np.float32)
    down = np.broadcast_to(levels[:, None], (16, WORDS))
    across = np.broadcast_to(np.tile(levels, WORDS // 16)[None, :], (8, WORDS))
    return np.concatenate([down, across], 0)


def split_columns():
    matrix = np.zeros((COLS, COLS), np.float32)
    for column in range(COLS):
        matrix[column, column // 2 + WORDS * (column % 2)] = 1.0
    return matrix


def keyval_order(kv_columns, size_x):
    step = HEAD_DIM // 2 // size_x
    matrix = np.zeros((COLS, size_x * HEAD_DIM), np.float32)
    for column in range(kv_columns):
        head, inner = divmod(column, HEAD_DIM)
        half, turn = divmod(inner, HEAD_DIM // 2)
        piece, spot = divmod(turn, step)
        place = piece * HEAD_DIM + head * 2 * step + half * step + spot
        matrix[column, place] = 1.0
    return matrix


def dot(left, right):
    return jnp.dot(left, right, preferred_element_type=F32)


def dot_rows(left, right):
    return lax.dot_general(left, right, (((1,), (1,)), ((), ())), preferred_element_type=F32)


def three_parts(values):
    first = values.astype(BF16)
    rest = values - first.astype(F32)
    second = rest.astype(BF16)
    third = (rest - second.astype(F32)).astype(BF16)
    return first, second, third


def wide_dot(left, right):
    rows = left.shape[0]
    both = dot(jnp.concatenate(three_parts(left), 0), right)
    return (both[:rows] + both[rows : 2 * rows]) + both[2 * rows :]


def split_scales(absmax_ref, split_ref, scale_ref, first, tiles):
    rows = absmax_ref.shape[0]
    stacked = jnp.concatenate(
        [absmax_ref[:, COLS * tile : COLS * (tile + 1)] for tile in range(tiles)], 0
    )
    both = wide_dot(stacked, split_ref[...])
    for tile in range(tiles):
        scale_ref[first + tile] = both[rows * tile : rows * (tile + 1)]


def stack_tiles(array):
    return jnp.concatenate(
        [array[:, COLS * tile : COLS * (tile + 1)] for tile in range(array.shape[1] // COLS)], 0
    )


GATHER_LANES = lax.GatherDimensionNumbers(
    offset_dims=(),
    collapsed_slice_dims=(1,),
    start_index_map=(1,),
    operand_batching_dims=(0,),
    start_indices_batching_dims=(0,),
)


def pick_lanes(table, index):
    return lax.gather(
        table,
        index[..., None],
        GATHER_LANES,
        slice_sizes=(1, 1),
        mode=lax.GatherScatterMode.PROMISE_IN_BOUNDS,
    )


def pick_rows(table, index):
    return lax.gather(
        table,
        index[..., None],
        GATHER_ROWS,
        slice_sizes=(1, 1),
        mode=lax.GatherScatterMode.PROMISE_IN_BOUNDS,
    )


def weight_tile(codes_ref, scale_ref, level_ref, left_ref, store_ref, squared=True):
    in_rows = codes_ref.shape[0]
    chunk = min(CHUNK, in_rows)
    blocks = chunk // QBLOCK

    def visit(step, carry):
        total, squares = carry
        even_list = []
        odd_list = []
        for block in range(blocks):
            scale_row = scale_ref[pl.ds(step * blocks + block, 1), :]
            tables = [
                level_ref[8 * half : 8 * half + 8, :]
                * scale_row[:, WORDS * side : WORDS * side + WORDS]
                for side in range(2)
                for half in range(2)
            ]
            for row in range(0, QBLOCK, 8):
                word = codes_ref[pl.ds(step * chunk + block * QBLOCK + row, 8), :]
                if row < 8 * LANE_VECTORS:
                    across = level_ref[16:24, :]
                    even = pick_lanes(across, word & 15) * scale_row[:, :WORDS]
                    odd = pick_lanes(across, lax.shift_right_logical(word, 4)) * scale_row[:, WORDS:]
                else:
                    low = word & 7
                    even = jnp.where(
                        (word & 8) != 0, pick_rows(tables[1], low), pick_rows(tables[0], low)
                    )
                    high = lax.shift_right_logical(word, 4) & 7
                    odd = jnp.where(
                        word >= 128, pick_rows(tables[3], high), pick_rows(tables[2], high)
                    )
                even_list.append(even)
                odd_list.append(odd)
        weight = jnp.concatenate(
            [jnp.concatenate(even_list, 0), jnp.concatenate(odd_list, 0)], 1
        ).astype(BF16)
        start = pl.multiple_of(step * chunk, chunk)
        if store_ref is not None:
            store_ref[pl.ds(start, chunk), :] = weight
        total = total + dot(left_ref[:, pl.ds(start, chunk)], weight)
        if squared:
            squares = squares + dot(jnp.ones((PAD_ROWS, chunk), BF16), weight * weight)
        return (total, squares)

    return lax.fori_loop(
        0,
        in_rows // chunk,
        visit,
        (jnp.zeros((left_ref.shape[0], COLS), F32), jnp.zeros((PAD_ROWS, COLS), F32)),
    )


def block_mask(rows, columns, lead):
    row_id = lax.broadcasted_iota(jnp.int32, (rows, columns), 0)
    column_id = lax.broadcasted_iota(jnp.int32, (rows, columns), 1)
    owner = jnp.where(row_id < lead, row_id, lax.shift_right_logical(row_id - lead, 4))
    return owner == lax.shift_right_logical(column_id, 4)


def norm_terms(cross, gram, up_split, squares, row_count):
    inner = up_split * (2.0 * cross + gram)
    return squares + jnp.sum(
        inner.reshape(row_count, RANK, COLS), axis=1
    )


def code_copy(codes_ref, first, tile, buffer_ref, sems):
    columns = pl.ds(pl.multiple_of((first + tile) * WORDS, WORDS), WORDS)
    slot = tile % DEPTH if isinstance(tile, int) else lax.rem(tile, DEPTH)
    return pltpu.make_async_copy(codes_ref.at[:, columns], buffer_ref.at[slot], sems.at[slot])


def code_tile(codes_ref, first, tile, tiles, buffer_ref, sems):
    @pl.when(tile + DEPTH - 1 < tiles)
    def _():
        code_copy(codes_ref, first, tile + DEPTH - 1, buffer_ref, sems).start(priority=1)

    code_copy(codes_ref, first, tile, buffer_ref, sems).wait()
    return buffer_ref.at[lax.rem(tile, DEPTH)]


def fetch(sources, buffers, sems):
    copies = [
        pltpu.make_async_copy(source, buffer, sems.at[spot])
        for spot, (source, buffer) in enumerate(zip(sources, buffers))
    ]
    for copy in copies:
        copy.start(priority=0)
    return copies


def finish_all(copies):
    for copy in copies:
        copy.wait()


def read_scalars(source, buffer, sem):
    copy = pltpu.make_async_copy(source, buffer, sem)
    copy.start()
    return copy


def tenant_fetch(scalar_ref, row_count, source_ref, buffer_ref, lead, sems):
    return fetch(
        [source_ref.at[scalar_ref[row]] for row in range(row_count)],
        [
            buffer_ref.at[lead + RANK * row : lead + RANK * (row + 1), :]
            for row in range(row_count)
        ],
        sems,
    )


def query_kernel(
    row_count,
    size_x,
    tenant_hbm,
    hidden_hbm,
    gain_hbm,
    absmax_hbm,
    kv_absmax_hbm,
    level_hbm,
    split_hbm,
    join_hbm,
    kv_join_hbm,
    codes_ref,
    kv_codes_ref,
    down_ref,
    up_ref,
    *refs,
):
    outs = refs[:size_x]
    (
        hidden_ref,
        gain_ref,
        absmax_ref,
        kv_absmax_ref,
        level_ref,
        split_ref,
        join_ref,
        kv_join_ref,
        left_ref,
        scale_ref,
        total_ref,
        square_ref,
        chunk_ref,
        buffer_ref,
        kv_buffer_ref,
        ups_ref,
        code_sems,
        kv_sem,
        down_sems,
        up_sems,
        small_sems,
        scalar_ref,
        scalar_sem,
    ) = refs[size_x:]
    tiles = absmax_ref.shape[1] // COLS
    share = chunk_ref.shape[2] - HEAD_DIM
    low_rank = row_count * RANK
    here = lax.axis_index("gx")
    kv_copy = pltpu.make_async_copy(kv_codes_ref, kv_buffer_ref, kv_sem.at[0])
    scalars = read_scalars(tenant_hbm, scalar_ref, scalar_sem.at[0])
    kv_copy.start(priority=1)
    smalls = fetch(
        [
            split_hbm,
            kv_absmax_hbm,
            level_hbm,
            hidden_hbm,
            gain_hbm,
            absmax_hbm,
            kv_join_hbm,
            join_hbm,
        ],
        [
            split_ref,
            kv_absmax_ref,
            level_ref,
            hidden_ref,
            gain_ref,
            absmax_ref,
            kv_join_ref,
            join_ref,
        ],
        small_sems,
    )
    code_copy(codes_ref, 0, 0, buffer_ref, code_sems).start(priority=1)
    scalars.wait()
    downs = tenant_fetch(scalar_ref, row_count, down_ref, left_ref, PAD_ROWS, down_sems)
    finish_all(smalls[:5])
    states = hidden_ref[...].astype(F32)
    mean_square = jnp.mean(states * states, axis=1, keepdims=True)
    in_rows = left_ref.shape[1]
    own = pl.ds(pl.multiple_of(here * in_rows, in_rows), in_rows)
    normed = hidden_ref[:, own].astype(F32) * lax.rsqrt(mean_square + NORM_EPS) * gain_ref[:, own]
    left_ref[0:PAD_ROWS, :] = jnp.concatenate(
        [normed, jnp.zeros((PAD_ROWS - row_count, normed.shape[1]), F32)], 0
    ).astype(BF16)
    split_scales(kv_absmax_ref, split_ref, scale_ref, 0, 1)
    kv_copy.wait()
    for tile in range(1, min(DEPTH - 1, tiles)):
        code_copy(codes_ref, 0, tile, buffer_ref, code_sems).start(priority=1)
    total, _ = weight_tile(
        kv_buffer_ref, scale_ref.at[0], level_ref, left_ref.at[0:PAD_ROWS, :], None, False
    )
    finish_all(smalls[5:])
    split_scales(absmax_ref, split_ref, scale_ref, 1, tiles)
    joined = wide_dot(total, kv_join_ref[...])
    for owner in range(size_x):
        chunk_ref[owner, :, share:] = joined[
            : 2 * row_count, owner * HEAD_DIM : (owner + 1) * HEAD_DIM
        ]
    ups = tenant_fetch(scalar_ref, row_count, up_ref, ups_ref, 0, up_sems)
    finish_all(downs)

    def visit(tile, carry):
        codes = code_tile(codes_ref, 0, tile, tiles, buffer_ref, code_sems)
        total, squares = weight_tile(codes, scale_ref.at[tile + 1], level_ref, left_ref, None)
        total_ref[tile] = total
        square_ref[tile] = squares[0:8]
        return carry

    lax.fori_loop(0, tiles, visit, 0)
    finish_all(ups)
    gram = dot_rows(left_ref[...], left_ref[PAD_ROWS:, :])
    gram = jnp.where(block_mask(*gram.shape, PAD_ROWS), gram, 0.0)
    up_split = dot(stack_tiles(ups_ref[...]), split_ref[...])
    lines = []
    for tile in range(tiles):
        up_tile = up_split[low_rank * tile : low_rank * (tile + 1)]
        extra = wide_dot(gram, up_tile.astype(BF16))
        total = total_ref[tile]
        lines.append(total[:row_count] + extra[:row_count])
        lines.append(
            norm_terms(
                total[PAD_ROWS:], extra[PAD_ROWS:], up_tile, square_ref[tile, 0:1], row_count
            )
        )
    joined = wide_dot(jnp.concatenate(lines, 0), join_ref[...])
    piece = min(COLS, share)
    for tile in range(tiles):
        for part in range(COLS // piece):
            owner, place = divmod(tile * COLS + part * piece, share)
            chunk_ref[owner, :, place : place + piece] = joined[
                2 * row_count * tile : 2 * row_count * (tile + 1),
                part * piece : (part + 1) * piece,
            ]
    for shift in range(size_x):
        outs[shift][...] = chunk_ref[lax.rem(here + shift, size_x)]


def store_copy(store_ref, slot, weight_ref, tile, sems):
    return pltpu.make_async_copy(store_ref.at[slot], weight_ref.at[tile], sems.at[slot])


def output_scale_kernel(
    row_count,
    first,
    tenant_hbm,
    absmax_hbm,
    level_hbm,
    split_hbm,
    join_hbm,
    codes_ref,
    down_ref,
    up_ref,
    norm_ref,
    up_split_ref,
    weight_ref,
    absmax_ref,
    level_ref,
    split_ref,
    join_ref,
    store_ref,
    left_ref,
    scale_ref,
    total_ref,
    square_ref,
    buffer_ref,
    ups_ref,
    code_sems,
    down_sems,
    up_sems,
    store_sems,
    small_sems,
    scalar_ref,
    scalar_sem,
):
    scalars = read_scalars(tenant_hbm, scalar_ref, scalar_sem.at[0])
    tiles = weight_ref.shape[0]
    low_rank = row_count * RANK
    columns = slice(first * COLS, (first + tiles) * COLS)
    code_copy(codes_ref, first, 0, buffer_ref, code_sems).start(priority=1)
    smalls = fetch(
        [split_hbm, absmax_hbm.at[:, columns], level_hbm, join_hbm],
        [split_ref, absmax_ref, level_ref, join_ref],
        small_sems,
    )
    scalars.wait()
    downs = tenant_fetch(scalar_ref, row_count, down_ref, left_ref, 0, down_sems)
    for tile in range(1, min(DEPTH - 1, tiles)):
        code_copy(codes_ref, first, tile, buffer_ref, code_sems).start(priority=1)
    ups = tenant_fetch(
        scalar_ref, row_count, up_ref.at[:, :, columns], ups_ref, 0, up_sems
    )
    finish_all(smalls)
    split_scales(absmax_ref, split_ref, scale_ref, 0, tiles)
    finish_all(downs)

    def visit(tile, carry):
        codes = code_tile(codes_ref, first, tile, tiles, buffer_ref, code_sems)
        slot = lax.rem(tile, 2)

        @pl.when(tile >= 2)
        def _():
            store_copy(store_ref, slot, weight_ref, tile - 2, store_sems).wait()

        total, squares = weight_tile(
            codes, scale_ref.at[tile], level_ref, left_ref, store_ref.at[slot]
        )
        store_copy(store_ref, slot, weight_ref, tile, store_sems).start()
        total_ref[tile] = total
        square_ref[tile] = squares[0:8]
        return carry

    lax.fori_loop(0, tiles, visit, 0)
    finish_all(ups)
    gram = dot_rows(left_ref[...], left_ref[...])
    gram = jnp.where(block_mask(*gram.shape, 0), gram, 0.0)
    up_split = dot(stack_tiles(ups_ref[...]), split_ref[...])
    lines = []
    for tile in range(tiles):
        up_tile = up_split[low_rank * tile : low_rank * (tile + 1)]
        narrow = up_tile.astype(BF16)
        up_split_ref[:, COLS * tile : COLS * (tile + 1)] = narrow
        extra = wide_dot(gram, narrow)
        lines.append(norm_terms(total_ref[tile], extra, up_tile, square_ref[tile, 0:1], row_count))
    joined = wide_dot(jnp.concatenate(lines, 0), join_ref[...])
    for tile in range(tiles):
        norm_ref[:, COLS * tile : COLS * (tile + 1)] = joined[
            row_count * tile : row_count * (tile + 1)
        ]
    for tile in range(max(tiles - 2, 0), tiles):
        store_copy(store_ref, tile % 2, weight_ref, tile, store_sems).wait()


def rotate_kernel(row_count, size_x, step, scalar_ref, magnitude_ref, cos_ref, sin_ref, *refs):
    parts = refs[:size_x]
    out_ref = refs[size_x]
    share = cos_ref.shape[1] - HEAD_DIM
    total = parts[0][...]
    for part in parts[1:]:
        total = total + part[...]
    magnitude = jnp.concatenate(
        [
            magnitude_ref[pl.ds(scalar_ref[row], 1), :]
            for row in range(row_count)
        ],
        0,
    )
    query = total[:row_count, :share] * (
        magnitude * lax.rsqrt(total[row_count:, :share])
    )
    keyval = total[:row_count, share:]
    half = HEAD_DIM // 2
    pieces = []
    for head in range(share // HEAD_DIM):
        block = query[:, head * HEAD_DIM : (head + 1) * HEAD_DIM]
        pieces.append(pltpu.roll(block, half, 1))
    lane = lax.broadcasted_iota(jnp.int32, keyval.shape, 1)
    other = jnp.where(
        (lane & step) != 0, pltpu.roll(keyval, step, 1), pltpu.roll(keyval, HEAD_DIM - step, 1)
    )
    values = jnp.concatenate([query, keyval], 1)
    partner = jnp.concatenate(pieces + [other], 1)
    turned = (values * cos_ref[...] + partner * sin_ref[...]).astype(BF16)
    for target in range(out_ref.shape[0]):
        out_ref[target] = turned


def attend_kernel(
    row_count,
    size_x,
    size_y,
    owner_hbm,
    filled_hbm,
    gathered_hbm,
    kv_order_hbm,
    pages_ref,
    send_ref,
    query_ref,
    mixed_ref,
    best_ref,
    total_ref,
    value_ref,
    held_ref,
    gathered_ref,
    kv_order_ref,
    owner_ref,
    filled_ref,
    table_ref,
    page_sems,
    small_sems,
):
    slots = pages_ref.shape[0]

    def page_copy(slot):
        return pltpu.make_async_copy(pages_ref.at[slot], held_ref.at[slot], page_sems.at[slot])

    smalls = fetch(
        [owner_hbm, filled_hbm, gathered_hbm, kv_order_hbm],
        [owner_ref, filled_ref, gathered_ref, kv_order_ref],
        small_sems,
    )
    ahead = min(4, slots)
    for slot in range(ahead):
        page_copy(slot).start(priority=1)
    finish_all(smalls)
    devices = size_x * size_y
    per_target = HEADS // devices
    group = HEADS // KV_HEADS
    inv_root = 1.0 / math.sqrt(HEAD_DIM)
    used = sum((filled_ref[slot] > 0).astype(jnp.int32) for slot in range(slots))
    device = lax.axis_index("gx") * size_y + lax.axis_index("gy")
    share = gathered_ref.shape[2] - HEAD_DIM

    def setup():
        heads_here = share // HEAD_DIM
        for place_x in range(size_x):
            for place_y in range(size_y):
                block = gathered_ref[place_x * size_y + place_y].astype(F32)
                for head in range(heads_here):
                    first = (place_y * size_x + place_x) * heads_here + head
                    query_ref[pl.ds(first, row_count, stride=HEADS), :] = block[
                        :, head * HEAD_DIM : (head + 1) * HEAD_DIM
                    ]
                mixed_ref[place_x, place_y * row_count : (place_y + 1) * row_count, :] = block[
                    :, share:
                ]
        best_ref[...] = jnp.full(best_ref.shape, NEG_FILL, F32)
        total_ref[...] = jnp.zeros(total_ref.shape, F32)
        value_ref[...] = jnp.zeros(value_ref.shape, F32)

        @pl.when(device < row_count)
        def _():
            columns = kv_order_ref.shape[0]
            plain = jnp.zeros((size_y * row_count, columns), F32)
            for place_x in range(size_x):
                plain = plain + dot_rows(
                    mixed_ref[place_x].astype(BF16),
                    kv_order_ref[:, place_x * HEAD_DIM : (place_x + 1) * HEAD_DIM],
                )
            heads_each = 2 * KV_HEADS // size_y
            for row in range(row_count):

                @pl.when(device == row)
                def _():
                    rows = []
                    for head in range(2 * KV_HEADS):
                        place_y, inner = divmod(head, heads_each)
                        line = place_y * row_count + row
                        one = plain[line : line + 1, inner * HEAD_DIM : (inner + 1) * HEAD_DIM]
                        rows.append(jnp.broadcast_to(one, (group, HEAD_DIM)))
                    new_keys = jnp.concatenate(rows[:KV_HEADS], 0)
                    new_values = jnp.concatenate(rows[KV_HEADS:], 0)
                    span = slice(row * HEADS, (row + 1) * HEADS)
                    score = jnp.sum(query_ref[span, :] * new_keys, 1, keepdims=True) * inv_root
                    best_ref[span, :] = jnp.broadcast_to(score, (HEADS, HEAD_DIM))
                    total_ref[span, :] = jnp.ones((HEADS, HEAD_DIM), F32)
                    value_ref[span, :] = new_values

    setup()

    def page_terms(slot, count):
        start = pl.multiple_of(owner_ref[slot] * HEADS, HEADS)
        query = query_ref[pl.ds(start, HEADS), :].astype(BF16)
        scores = jnp.concatenate(
            [
                dot_rows(
                    query[group * head : group * (head + 1), :],
                    held_ref[slot, 0, :, head * HEAD_DIM : (head + 1) * HEAD_DIM],
                )
                for head in range(KV_HEADS)
            ],
            0,
        )
        inside = lax.broadcasted_iota(jnp.int32, (HEADS, PAGE), 1) < count
        scores = jnp.where(inside, scores * inv_root, NEG_FILL)
        peak = jnp.max(scores, axis=1, keepdims=True)
        weights = jnp.where(inside, jnp.exp(scores - peak), 0.0)
        coarse = weights.astype(BF16)
        fine = (weights - coarse.astype(F32)).astype(BF16)
        gains = []
        for head in range(KV_HEADS):
            rows = slice(group * head, group * (head + 1))
            both = dot(
                jnp.concatenate([coarse[rows], fine[rows]], 0),
                held_ref[slot, 1, :, head * HEAD_DIM : (head + 1) * HEAD_DIM],
            )
            gains.append(both[:group] + both[group:])
        return start, peak, jnp.sum(weights, axis=1, keepdims=True), jnp.concatenate(gains, 0)

    def add_terms(start, peak, amount, gain):
        span = pl.ds(start, HEADS)
        old_best = best_ref[span, :]
        best = jnp.maximum(old_best, peak)
        keep = jnp.exp(old_best - best)
        take = jnp.exp(peak - best)
        best_ref[span, :] = best
        total_ref[span, :] = total_ref[span, :] * keep + amount * take
        value_ref[span, :] = value_ref[span, :] * keep + gain * take

    def visit(pair, carry):
        first = 2 * pair
        second = jnp.minimum(first + 1, used - 1)
        for slot in (first, first + 1):

            @pl.when(slot + ahead < used)
            def _(slot=slot):
                page_copy(slot + ahead).start(priority=1)

        page_copy(first).wait()

        @pl.when(first + 1 < used)
        def _():
            page_copy(second).wait()

        terms = [
            page_terms(first, filled_ref[first]),
            page_terms(second, jnp.where(first + 1 < used, filled_ref[second], 0)),
        ]
        for term in terms:
            add_terms(*term)
        return carry

    lax.fori_loop(0, (used + 1) // 2, visit, 0)
    for slot in range(ahead):

        @pl.when(slot >= used)
        def _(slot=slot):
            page_copy(slot).wait()


    def close():
        lane = lax.broadcasted_iota(jnp.int32, (HEADS, HEAD_DIM), 1)
        kinds = 2 * row_count
        table = jnp.zeros((HEADS, HEAD_DIM), F32)
        for kind, source in enumerate((best_ref, total_ref)):
            for row in range(row_count):
                block = source[row * HEADS : (row + 1) * HEADS, :]
                for part, values in enumerate(three_parts(block)):
                    spot = part * kinds + kind * row_count + row
                    table = jnp.where(lane == spot, values.astype(F32), table)
        table_ref[...] = table
        packed = table_ref[pl.ds(0, devices, stride=per_target), :]
        for head in range(1, per_target):
            line = table_ref[pl.ds(head, devices, stride=per_target), :]
            packed = packed + pltpu.roll(line, 3 * kinds * head, 1)
        rows = row_count * per_target
        for target in range(devices):
            block = jnp.concatenate(
                [
                    value_ref[
                        row * HEADS + target * per_target : row * HEADS
                        + (target + 1) * per_target,
                        :,
                    ]
                    for row in range(row_count)
                ],
                0,
            )
            send_ref[target, 0:rows, :] = block.astype(BF16)
            send_ref[target, rows : rows + 8, :] = jnp.broadcast_to(
                packed[target : target + 1, :], (8, HEAD_DIM)
            ).astype(BF16)

    close()


def merge_kernel(row_count, per_target, parts_ref, out_ref):
    rows = row_count * per_target
    kinds = 2 * row_count
    values = parts_ref[:, 0:rows, :].astype(F32)
    packed = parts_ref[:, rows : rows + 8, :].astype(F32)[:, 0:1, :]

    def scalar(head, kind):
        lanes = [3 * kinds * head + part * kinds + kind for part in range(3)]
        first, second, third = [packed[:, :, lane : lane + 1] for lane in lanes]
        return (first + second) + third

    for row in range(row_count):
        for head in range(per_target):
            best = scalar(head, row)
            factor = jnp.exp(best - jnp.max(best, axis=0, keepdims=True))
            line = row * per_target + head
            top = jnp.sum(values[:, line : line + 1, :] * factor, axis=0)
            bottom = jnp.sum(scalar(head, row_count + row) * factor, axis=0)
            ratio = (top / bottom).astype(BF16)
            for target in range(out_ref.shape[0]):
                out_ref[target, row : row + 1, head * HEAD_DIM : (head + 1) * HEAD_DIM] = ratio


def output_kernel(
    row_count,
    size_x,
    tile_counts,
    tenant_hbm,
    attended_hbm,
    join_hbm,
    down_ref,
    *refs,
):
    parts = len(tile_counts)
    norms_hbm = refs[:parts]
    ups_hbm = refs[parts : 2 * parts]
    weights = refs[2 * parts : 3 * parts]
    outs = refs[3 * parts : 3 * parts + size_x]
    refs = refs[3 * parts + size_x :]
    norms = refs[:parts]
    splits = refs[parts : 2 * parts]
    (
        attended_ref,
        join_ref,
        left_ref,
        low_ref,
        total_ref,
        chunk_ref,
        held_ref,
        down_sems,
        held_sems,
        small_sems,
        scalar_ref,
        scalar_sem,
    ) = refs[2 * parts :]
    tiles = sum(tile_counts)
    own = row_count // size_x
    scalars = read_scalars(tenant_hbm, scalar_ref, scalar_sem.at[0])
    smalls = fetch(
        [attended_hbm, join_hbm] + list(norms_hbm) + list(ups_hbm),
        [attended_ref, join_ref] + list(norms) + list(splits),
        small_sems,
    )
    loads = [
        pltpu.make_async_copy(
            weights[part].at[tile],
            held_ref.at[sum(tile_counts[:part]) + tile],
            held_sems.at[sum(tile_counts[:part]) + tile],
        )
        for part in range(parts)
        for tile in range(tile_counts[part])
    ]
    scalars.wait()
    downs = tenant_fetch(scalar_ref, row_count, down_ref, low_ref, 0, down_sems)
    for load in loads:
        load.start(priority=1)
    smalls[0].wait()
    width = attended_ref.shape[2]
    for part in range(attended_ref.shape[0]):
        block = attended_ref[part].astype(F32)
        left_ref[:, part * width : (part + 1) * width] = jnp.concatenate(
            [block, jnp.zeros((PAD_ROWS - row_count, width), F32)], 0
        ).astype(BF16)
    finish_all(downs)
    finish_all(smalls[1:])
    middle = dot_rows(left_ref[...], low_ref[...])
    middle = jnp.where(block_mask(*middle.shape, PAD_ROWS), middle, 0.0)
    extras = [wide_dot(middle, up[...]) for up in splits]
    numbers = []
    for part in range(parts):
        for tile in range(tile_counts[part]):
            spot = len(numbers)
            loads[spot].wait()
            total_ref[spot] = dot(left_ref[...], held_ref[spot]) + extras[part][
                :, COLS * tile : COLS * (tile + 1)
            ]
            numbers.append(total_ref[spot, 0:row_count])
    joined = wide_dot(jnp.concatenate(numbers, 0), join_ref[...])
    for owner in range(size_x):
        for spot in range(tiles):
            begin = row_count * spot + owner * own
            chunk_ref[owner, 0:own, COLS * spot : COLS * (spot + 1)] = joined[begin : begin + own]
        for part in range(parts):
            begin = COLS * sum(tile_counts[:part])
            chunk_ref[owner, own : 2 * own, begin : begin + COLS * tile_counts[part]] = norms[
                part
            ][owner * own : (owner + 1) * own, :]
    here = lax.axis_index("gx")
    for shift in range(size_x):
        outs[shift][...] = chunk_ref[lax.rem(here + shift, size_x)]


def finish_kernel(row_count, size_x, scalar_ref, hidden_ref, magnitude_ref, *refs):
    parts = refs[:size_x]
    out_ref = refs[size_x]
    own = row_count // size_x
    total = parts[0][...]
    for part in parts[1:]:
        total = total + part[...]
    here = lax.axis_index("gx")
    states = hidden_ref[...].astype(F32)
    row_id = lax.broadcasted_iota(jnp.int32, states.shape, 0)
    for line in range(own):
        row = here * own + line
        state = jnp.sum(jnp.where(row_id == row, states, 0.0), axis=0, keepdims=True)
        magnitude = magnitude_ref[pl.ds(scalar_ref[row], 1), :]
        scale = magnitude * lax.rsqrt(total[own + line : own + line + 1])
        out_ref[line : line + 1, :] = (state + total[line : line + 1] * scale).astype(BF16)


def slot_info(page_table, lengths, device, slot_count):
    row_count, page_limit = page_table.shape
    page_need = (lengths + PAGE - 1) // PAGE
    page_numbers = jnp.arange(page_limit, dtype=jnp.int32)
    live_mask = page_numbers[None, :] < page_need[:, None]
    wanted = device * slot_count + jnp.arange(slot_count, dtype=jnp.int32)
    hits = ((page_table[None, :, :] == wanted[:, None, None]) & live_mask[None, :, :]).astype(
        jnp.int32
    )
    owner_row = jnp.sum(hits * jnp.arange(row_count, dtype=jnp.int32)[None, :, None], axis=(1, 2))
    remaining = jnp.clip(lengths[:, None] - page_numbers[None, :] * PAGE, 0, PAGE)
    filled = jnp.sum(hits * remaining[None, :, :], axis=(1, 2))
    return owner_row, filled


def exchange(parts, axis, size):
    received = [parts[0]]
    for shift in range(1, size):
        received.append(
            lax.ppermute(parts[shift], axis, [(spot, (spot + shift) % size) for spot in range(size)])
        )
    return received


def whole(shape):
    return pl.BlockSpec(shape, lambda *_: (0,) * len(shape))


def local(
    hidden,
    norm_gain,
    q_codes,
    q_absmax,
    kv_codes,
    kv_absmax,
    o_codes,
    o_absmax,
    q_down,
    q_up,
    q_magnitude,
    o_down,
    o_up,
    o_magnitude,
    tenant,
    lengths,
    page_table,
    kv_cache,
):
    row_count, width = hidden.shape
    row_x = lax.axis_index("gx").astype(jnp.int32)
    col_y = lax.axis_index("gy").astype(jnp.int32)
    size_x = lax.axis_size("gx")
    size_y = lax.axis_size("gy")
    devices = size_x * size_y
    device = row_x * size_y + col_y
    in_rows, q_words = q_codes.shape
    q_cols = 2 * q_words
    share = q_cols // size_x
    kv_cols = 2 * kv_codes.shape[1]
    if kv_cols < COLS:
        kv_codes = jnp.pad(kv_codes, ((0, 0), (0, WORDS - kv_codes.shape[1])))
        kv_absmax = jnp.pad(kv_absmax, ((0, 0), (0, COLS - kv_cols)))
    low_rank = row_count * RANK
    level = jnp.asarray(level_table())
    split_matrix = split_columns()
    split = jnp.asarray(split_matrix, BF16)
    join = jnp.asarray(split_matrix.T, BF16)
    order = keyval_order(kv_cols, size_x)
    kv_join = jnp.asarray(split_matrix.T @ order, BF16)
    kv_order = jnp.asarray(order, BF16)
    scalars = tenant
    q_down = jnp.swapaxes(q_down, 1, 2)
    o_down = jnp.swapaxes(o_down, 1, 2)
    q_tiles = q_words // WORDS
    scale_rows = in_rows // QBLOCK

    smem = pl.BlockSpec(memory_space=pltpu.SMEM)
    vmem = pl.BlockSpec(memory_space=pltpu.VMEM)
    anywhere = pl.BlockSpec(memory_space=pltpu.HBM)
    chunk_shape = (2 * row_count, share + HEAD_DIM)
    scalar_scratch = [pltpu.SMEM((row_count,), jnp.int32), pltpu.SemaphoreType.DMA((1,))]
    small = [
        pltpu.VMEM((scale_rows, q_cols), F32),
        pltpu.VMEM((scale_rows, COLS), F32),
        pltpu.VMEM(level.shape, F32),
        pltpu.VMEM(split.shape, BF16),
        pltpu.VMEM(join.shape, BF16),
    ]
    q_parts = pl.pallas_call(
        functools.partial(query_kernel, row_count, size_x),
        in_specs=[anywhere] * 13,
        out_specs=[vmem] * size_x,
        scratch_shapes=[
            pltpu.VMEM((row_count, width), BF16),
            pltpu.VMEM((1, width), F32),
            *small,
            pltpu.VMEM(kv_join.shape, BF16),
            pltpu.VMEM((PAD_ROWS + low_rank, in_rows), BF16),
            pltpu.VMEM((q_tiles + 1, scale_rows, COLS), F32),
            pltpu.VMEM((q_tiles, PAD_ROWS + low_rank, COLS), F32),
            pltpu.VMEM((q_tiles, 8, COLS), F32),
            pltpu.VMEM((size_x,) + chunk_shape, F32),
            pltpu.VMEM((DEPTH, in_rows, WORDS), jnp.int32),
            pltpu.VMEM((in_rows, WORDS), jnp.int32),
            pltpu.VMEM((low_rank, q_cols), BF16),
            pltpu.SemaphoreType.DMA((DEPTH,)),
            pltpu.SemaphoreType.DMA((1,)),
            pltpu.SemaphoreType.DMA((row_count,)),
            pltpu.SemaphoreType.DMA((row_count,)),
            pltpu.SemaphoreType.DMA((8,)),
            *scalar_scratch,
        ],
        out_shape=[jax.ShapeDtypeStruct(chunk_shape, F32)] * size_x,
        name="query",
    )(
        tenant,
        hidden,
        norm_gain[None, :],
        q_absmax,
        kv_absmax,
        level,
        split,
        join,
        kv_join,
        q_codes,
        kv_codes,
        q_down,
        q_up,
    )
    q_parts = exchange(q_parts, "gx", size_x)

    def output_scales(first, tiles, after):
        owners, _ = lax.optimization_barrier((tenant, after))
        return pl.pallas_call(
            functools.partial(output_scale_kernel, row_count, first),
            in_specs=[anywhere] * 8,
            out_specs=[vmem, vmem, anywhere],
            scratch_shapes=[
                pltpu.VMEM((scale_rows, tiles * COLS), F32),
                *small[2:],
                pltpu.VMEM((2, in_rows, COLS), BF16),
                pltpu.VMEM((low_rank, in_rows), BF16),
                pltpu.VMEM((tiles, scale_rows, COLS), F32),
                pltpu.VMEM((tiles, low_rank, COLS), F32),
                pltpu.VMEM((tiles, 8, COLS), F32),
                pltpu.VMEM((DEPTH, in_rows, WORDS), jnp.int32),
                pltpu.VMEM((low_rank, tiles * COLS), BF16),
                pltpu.SemaphoreType.DMA((DEPTH,)),
                pltpu.SemaphoreType.DMA((row_count,)),
                pltpu.SemaphoreType.DMA((row_count,)),
                pltpu.SemaphoreType.DMA((2,)),
                pltpu.SemaphoreType.DMA((4,)),
                *scalar_scratch,
            ],
            out_shape=[
                jax.ShapeDtypeStruct((row_count, tiles * COLS), F32),
                jax.ShapeDtypeStruct((low_rank, tiles * COLS), BF16),
                pltpu.HBM((tiles, in_rows, COLS), BF16),
            ],
            compiler_params=pltpu.CompilerParams(vmem_limit_bytes=56 * 2**20),
            cost_estimate=pl.CostEstimate(
                flops=tiles * 5_000_000 * 256,
                bytes_accessed=tiles * 8 * in_rows * WORDS,
                transcendentals=0,
            ),
            name="output_scale",
        )(owners, o_absmax, level, split, join, o_codes, o_down, o_up)

    tile_counts = [3 * q_tiles // 8, q_tiles - 3 * q_tiles // 8]

    half = HEAD_DIM // 2
    step = half // size_x
    lane = jnp.arange(share + HEAD_DIM, dtype=jnp.int32)
    in_query = lane < share
    turn = jnp.where(in_query, lane % half, row_x * step + lane % step)
    second = jnp.where(in_query, lane % HEAD_DIM // half, lane % (2 * step) // step)
    frequency = ROPE_BASE ** (-2.0 * turn.astype(F32) / HEAD_DIM)
    angles = lengths.astype(F32)[:, None] * frequency[None, :]
    plain = jnp.logical_and(~in_query, col_y * kv_cols >= KV_HEADS * HEAD_DIM)[None, :]
    cosine = jnp.where(plain, 1.0, jnp.cos(angles))
    sine = jnp.sin(angles)
    sine = jnp.where(plain, 0.0, jnp.where(second[None, :] == 1, sine, -sine))

    query_all = pl.pallas_call(
        functools.partial(rotate_kernel, row_count, size_x, step),
        grid_spec=pltpu.PrefetchScalarGridSpec(
            num_scalar_prefetch=1,
            grid=(1,),
            in_specs=[
                pl.BlockSpec((TENANTS, share), lambda tile, ref: (0, lax.axis_index("gx"))),
                whole(cosine.shape),
                whole(sine.shape),
            ]
            + [whole(chunk_shape)] * size_x,
            out_specs=whole((devices, row_count, share + HEAD_DIM)),
        ),
        out_shape=jax.ShapeDtypeStruct((devices, row_count, share + HEAD_DIM), BF16),
        compiler_params=pltpu.CompilerParams(vmem_limit_bytes=8 * 2**20),
        name="rotate",
    )(scalars, q_magnitude, cosine, sine, *q_parts)
    gathered = lax.all_to_all(query_all, ("gx", "gy"), split_axis=0, concat_axis=0, tiled=True)
    scale_parts = [output_scales(0, tile_counts[0], query_all)]
    gathered, scale_parts[0] = lax.optimization_barrier((gathered, scale_parts[0]))

    slots = kv_cache.shape[0]
    owner_row, filled = slot_info(page_table, lengths, device, slots)
    per_target = HEADS // devices
    send_shape = (devices, row_count * per_target + 8, HEAD_DIM)
    sent = pl.pallas_call(
        functools.partial(attend_kernel, row_count, size_x, size_y),
        in_specs=[anywhere] * 5,
        out_specs=vmem,
        scratch_shapes=[
            pltpu.VMEM((row_count * HEADS, HEAD_DIM), F32),
            pltpu.VMEM((size_x, size_y * row_count, HEAD_DIM), F32),
            pltpu.VMEM((row_count * HEADS, HEAD_DIM), F32),
            pltpu.VMEM((row_count * HEADS, HEAD_DIM), F32),
            pltpu.VMEM((row_count * HEADS, HEAD_DIM), F32),
            pltpu.VMEM(kv_cache.shape, BF16),
            pltpu.VMEM(gathered.shape, BF16),
            pltpu.VMEM((kv_cols, kv_order.shape[1]), BF16),
            pltpu.SMEM((slots,), jnp.int32),
            pltpu.SMEM((slots,), jnp.int32),
            pltpu.VMEM((HEADS, HEAD_DIM), F32),
            pltpu.SemaphoreType.DMA((slots,)),
            pltpu.SemaphoreType.DMA((4,)),
        ],
        out_shape=jax.ShapeDtypeStruct(send_shape, BF16),
        compiler_params=pltpu.CompilerParams(vmem_limit_bytes=58 * 2**20),
        name="attend",
    )(owner_row, filled, gathered, kv_order[:kv_cols], kv_cache)
    parts = lax.all_to_all(sent, ("gx", "gy"), split_axis=0, concat_axis=0, tiled=True)
    scale_parts.append(output_scales(tile_counts[0], tile_counts[1], sent))
    parts, scale_parts[1] = lax.optimization_barrier((parts, scale_parts[1]))

    merged = pl.pallas_call(
        functools.partial(merge_kernel, row_count, per_target),
        in_specs=[pl.BlockSpec(memory_space=pltpu.VMEM)],
        out_specs=pl.BlockSpec(memory_space=pltpu.VMEM),
        out_shape=jax.ShapeDtypeStruct((size_y, row_count, per_target * HEAD_DIM), BF16),
        compiler_params=pltpu.CompilerParams(vmem_limit_bytes=8 * 2**20),
        name="merge",
    )(parts)
    attended = lax.all_to_all(merged, "gy", split_axis=0, concat_axis=0, tiled=True)

    own = row_count // size_x
    o_parts = pl.pallas_call(
        functools.partial(output_kernel, row_count, size_x, tile_counts),
        in_specs=[anywhere] * (4 + 3 * len(scale_parts)),
        out_specs=[vmem] * size_x,
        scratch_shapes=[
            *[pltpu.VMEM((row_count, count * COLS), F32) for count in tile_counts],
            *[pltpu.VMEM((low_rank, count * COLS), BF16) for count in tile_counts],
            pltpu.VMEM(attended.shape, BF16),
            pltpu.VMEM(join.shape, BF16),
            pltpu.VMEM((PAD_ROWS, in_rows), BF16),
            pltpu.VMEM((low_rank, in_rows), BF16),
            pltpu.VMEM((q_tiles, PAD_ROWS, COLS), F32),
            pltpu.VMEM((size_x, 2 * own, q_cols), F32),
            pltpu.VMEM((q_tiles, in_rows, COLS), BF16),
            pltpu.SemaphoreType.DMA((row_count,)),
            pltpu.SemaphoreType.DMA((q_tiles,)),
            pltpu.SemaphoreType.DMA((2 + 2 * len(scale_parts),)),
            *scalar_scratch,
        ],
        out_shape=[jax.ShapeDtypeStruct((2 * own, q_cols), F32)] * size_x,
        compiler_params=pltpu.CompilerParams(vmem_limit_bytes=56 * 2**20),
        name="output",
    )(
        tenant,
        attended,
        join,
        o_down,
        *[part[0] for part in scale_parts],
        *[part[1] for part in scale_parts],
        *[part[2] for part in scale_parts],
    )
    o_parts = exchange(o_parts, "gx", size_x)
    return pl.pallas_call(
        functools.partial(finish_kernel, row_count, size_x),
        grid_spec=pltpu.PrefetchScalarGridSpec(
            num_scalar_prefetch=1,
            grid=(1,),
            in_specs=[
                pl.BlockSpec((row_count, q_cols), lambda tile, ref: (0, lax.axis_index("gy"))),
                whole(o_magnitude.shape),
            ]
            + [whole((2 * own, q_cols))] * size_x,
            out_specs=whole((own, q_cols)),
        ),
        out_shape=jax.ShapeDtypeStruct((own, q_cols), BF16),
        compiler_params=pltpu.CompilerParams(vmem_limit_bytes=4 * 2**20),
        name="finish",
    )(scalars, hidden, o_magnitude, *o_parts)


def solution(mesh):
    in_specs = (
        P(),
        P(),
        P("gx", "gy"),
        P("gx", "gy"),
        P("gx", "gy"),
        P("gx", "gy"),
        P("gx", "gy"),
        P("gx", "gy"),
        P(None, "gx", None),
        P(None, None, "gy"),
        P(None, "gy"),
        P(None, "gx", None),
        P(None, None, "gy"),
        P(None, "gy"),
        P(),
        P(),
        P(),
        P(("gx", "gy"), None, None, None),
    )
    out_specs = P("gx", "gy")
    return jax.shard_map(local, mesh=mesh, in_specs=in_specs, out_specs=out_specs, check_vma=False)
```

```python
import functools
import math

import jax
import jax.numpy as jnp
import numpy as np
from jax import lax
from jax.experimental import pallas as pl
from jax.experimental.pallas import tpu as pltpu
from jax.sharding import PartitionSpec as P

HEADS = 128
KV_HEADS = 8
HEAD_DIM = 128
TENANTS = 8
RANK = 16
QBLOCK = 64
PAGE = 256

NF4_LEVELS = (
    -1.0,
    -0.6961928009986877,
    -0.5250730514526367,
    -0.39491748809814453,
    -0.28444138169288635,
    -0.18477343022833234,
    -0.09105003625154495,
    0.0,
    0.07958029955625534,
    0.16093020141124725,
    0.24611230194568634,
    0.33791524171829224,
    0.44070982933044434,
    0.5626170039176941,
    0.7229568362236023,
    1.0,
)
NORM_EPS = 1e-05
NEG_FILL = -1e30
ROPE_BASE = 500000.0
WORDS = 128
COLS = 2 * WORDS
CHUNK = 2048
PAD_ROWS = 16
DEPTH = 3
LANE_VECTORS = 2
F32 = jnp.float32
BF16 = jnp.bfloat16
GATHER_ROWS = lax.GatherDimensionNumbers(
    offset_dims=(),
    collapsed_slice_dims=(0,),
    start_index_map=(0,),
    operand_batching_dims=(1,),
    start_indices_batching_dims=(1,),
)


def level_table():
    levels = np.asarray(NF4_LEVELS, np.float32)
    down = np.broadcast_to(levels[:, None], (16, WORDS))
    across = np.broadcast_to(np.tile(levels, WORDS // 16)[None, :], (8, WORDS))
    return np.concatenate([down, across], 0)


def split_columns():
    matrix = np.zeros((COLS, COLS), np.float32)
    for column in range(COLS):
        matrix[column, column // 2 + WORDS * (column % 2)] = 1.0
    return matrix


def keyval_order(kv_columns, size_x):
    step = HEAD_DIM // 2 // size_x
    matrix = np.zeros((COLS, size_x * HEAD_DIM), np.float32)
    for column in range(kv_columns):
        head, inner = divmod(column, HEAD_DIM)
        half, turn = divmod(inner, HEAD_DIM // 2)
        piece, spot = divmod(turn, step)
        place = piece * HEAD_DIM + head * 2 * step + half * step + spot
        matrix[column, place] = 1.0
    return matrix


def dot(left, right):
    return jnp.dot(left, right, preferred_element_type=F32)


def dot_rows(left, right):
    return lax.dot_general(left, right, (((1,), (1,)), ((), ())), preferred_element_type=F32)


def three_parts(values):
    first = values.astype(BF16)
    rest = values - first.astype(F32)
    second = rest.astype(BF16)
    third = (rest - second.astype(F32)).astype(BF16)
    return first, second, third


def wide_dot(left, right):
    rows = left.shape[0]
    both = dot(jnp.concatenate(three_parts(left), 0), right)
    return (both[:rows] + both[rows : 2 * rows]) + both[2 * rows :]


def split_scales(absmax_ref, split_ref, scale_ref, first, tiles):
    rows = absmax_ref.shape[0]
    stacked = jnp.concatenate(
        [absmax_ref[:, COLS * tile : COLS * (tile + 1)] for tile in range(tiles)], 0
    )
    both = wide_dot(stacked, split_ref[...])
    for tile in range(tiles):
        scale_ref[first + tile] = both[rows * tile : rows * (tile + 1)]


def stack_tiles(array):
    return jnp.concatenate(
        [array[:, COLS * tile : COLS * (tile + 1)] for tile in range(array.shape[1] // COLS)], 0
    )


GATHER_LANES = lax.GatherDimensionNumbers(
    offset_dims=(),
    collapsed_slice_dims=(1,),
    start_index_map=(1,),
    operand_batching_dims=(0,),
    start_indices_batching_dims=(0,),
)


def pick_lanes(table, index):
    return lax.gather(
        table,
        index[..., None],
        GATHER_LANES,
        slice_sizes=(1, 1),
        mode=lax.GatherScatterMode.PROMISE_IN_BOUNDS,
    )


def pick_rows(table, index):
    return lax.gather(
        table,
        index[..., None],
        GATHER_ROWS,
        slice_sizes=(1, 1),
        mode=lax.GatherScatterMode.PROMISE_IN_BOUNDS,
    )


def weight_tile(codes_ref, scale_ref, level_ref, left_ref, store_ref, squared=True):
    in_rows = codes_ref.shape[0]
    chunk = min(CHUNK, in_rows)
    blocks = chunk // QBLOCK

    def visit(step, carry):
        total, squares = carry
        even_list = []
        odd_list = []
        for block in range(blocks):
            scale_row = scale_ref[pl.ds(step * blocks + block, 1), :]
            tables = [
                level_ref[8 * half : 8 * half + 8, :]
                * scale_row[:, WORDS * side : WORDS * side + WORDS]
                for side in range(2)
                for half in range(2)
            ]
            for row in range(0, QBLOCK, 8):
                word = codes_ref[pl.ds(step * chunk + block * QBLOCK + row, 8), :]
                if row < 8 * LANE_VECTORS:
                    across = level_ref[16:24, :]
                    even = pick_lanes(across, word & 15) * scale_row[:, :WORDS]
                    odd = pick_lanes(across, lax.shift_right_logical(word, 4)) * scale_row[:, WORDS:]
                else:
                    low = word & 7
                    even = jnp.where(
                        (word & 8) != 0, pick_rows(tables[1], low), pick_rows(tables[0], low)
                    )
                    high = lax.shift_right_logical(word, 4) & 7
                    odd = jnp.where(
                        word >= 128, pick_rows(tables[3], high), pick_rows(tables[2], high)
                    )
                even_list.append(even)
                odd_list.append(odd)
        weight = jnp.concatenate(
            [jnp.concatenate(even_list, 0), jnp.concatenate(odd_list, 0)], 1
        ).astype(BF16)
        start = pl.multiple_of(step * chunk, chunk)
        if store_ref is not None:
            store_ref[pl.ds(start, chunk), :] = weight
        total = total + dot(left_ref[:, pl.ds(start, chunk)], weight)
        if squared:
            squares = squares + dot(jnp.ones((PAD_ROWS, chunk), BF16), weight * weight)
        return (total, squares)

    return lax.fori_loop(
        0,
        in_rows // chunk,
        visit,
        (jnp.zeros((left_ref.shape[0], COLS), F32), jnp.zeros((PAD_ROWS, COLS), F32)),
    )


def block_mask(rows, columns, lead):
    row_id = lax.broadcasted_iota(jnp.int32, (rows, columns), 0)
    column_id = lax.broadcasted_iota(jnp.int32, (rows, columns), 1)
    owner = jnp.where(row_id < lead, row_id, lax.shift_right_logical(row_id - lead, 4))
    return owner == lax.shift_right_logical(column_id, 4)


def norm_terms(cross, gram, up_split, squares, row_count):
    inner = up_split * (2.0 * cross + gram)
    return squares + jnp.sum(
        inner.reshape(row_count, RANK, COLS), axis=1
    )


def code_copy(codes_ref, first, tile, buffer_ref, sems):
    columns = pl.ds(pl.multiple_of((first + tile) * WORDS, WORDS), WORDS)
    slot = tile % DEPTH if isinstance(tile, int) else lax.rem(tile, DEPTH)
    return pltpu.make_async_copy(codes_ref.at[:, columns], buffer_ref.at[slot], sems.at[slot])


def code_tile(codes_ref, first, tile, tiles, buffer_ref, sems):
    @pl.when(tile + DEPTH - 1 < tiles)
    def _():
        code_copy(codes_ref, first, tile + DEPTH - 1, buffer_ref, sems).start(priority=1)

    code_copy(codes_ref, first, tile, buffer_ref, sems).wait()
    return buffer_ref.at[lax.rem(tile, DEPTH)]


def fetch(sources, buffers, sems):
    copies = [
        pltpu.make_async_copy(source, buffer, sems.at[spot])
        for spot, (source, buffer) in enumerate(zip(sources, buffers))
    ]
    for copy in copies:
        copy.start(priority=0)
    return copies


def finish_all(copies):
    for copy in copies:
        copy.wait()


def read_scalars(source, buffer, sem):
    copy = pltpu.make_async_copy(source, buffer, sem)
    copy.start()
    return copy


def tenant_fetch(scalar_ref, row_count, source_ref, buffer_ref, lead, sems):
    return fetch(
        [source_ref.at[scalar_ref[row]] for row in range(row_count)],
        [
            buffer_ref.at[lead + RANK * row : lead + RANK * (row + 1), :]
            for row in range(row_count)
        ],
        sems,
    )


def query_kernel(
    row_count,
    size_x,
    tenant_hbm,
    hidden_hbm,
    gain_hbm,
    absmax_hbm,
    kv_absmax_hbm,
    level_hbm,
    split_hbm,
    join_hbm,
    kv_join_hbm,
    codes_ref,
    kv_codes_ref,
    down_ref,
    up_ref,
    *refs,
):
    outs = refs[:size_x]
    (
        hidden_ref,
        gain_ref,
        absmax_ref,
        kv_absmax_ref,
        level_ref,
        split_ref,
        join_ref,
        kv_join_ref,
        left_ref,
        scale_ref,
        total_ref,
        square_ref,
        chunk_ref,
        buffer_ref,
        kv_buffer_ref,
        ups_ref,
        code_sems,
        kv_sem,
        down_sems,
        up_sems,
        small_sems,
        scalar_ref,
        scalar_sem,
    ) = refs[size_x:]
    tiles = absmax_ref.shape[1] // COLS
    share = chunk_ref.shape[2] - HEAD_DIM
    low_rank = row_count * RANK
    here = lax.axis_index("gx")
    kv_copy = pltpu.make_async_copy(kv_codes_ref, kv_buffer_ref, kv_sem.at[0])
    scalars = read_scalars(tenant_hbm, scalar_ref, scalar_sem.at[0])
    kv_copy.start(priority=1)
    smalls = fetch(
        [
            split_hbm,
            kv_absmax_hbm,
            level_hbm,
            hidden_hbm,
            gain_hbm,
            absmax_hbm,
            kv_join_hbm,
            join_hbm,
        ],
        [
            split_ref,
            kv_absmax_ref,
            level_ref,
            hidden_ref,
            gain_ref,
            absmax_ref,
            kv_join_ref,
            join_ref,
        ],
        small_sems,
    )
    code_copy(codes_ref, 0, 0, buffer_ref, code_sems).start(priority=1)
    scalars.wait()
    downs = tenant_fetch(scalar_ref, row_count, down_ref, left_ref, PAD_ROWS, down_sems)
    finish_all(smalls[:5])
    states = hidden_ref[...].astype(F32)
    mean_square = jnp.mean(states * states, axis=1, keepdims=True)
    in_rows = left_ref.shape[1]
    own = pl.ds(pl.multiple_of(here * in_rows, in_rows), in_rows)
    normed = hidden_ref[:, own].astype(F32) * lax.rsqrt(mean_square + NORM_EPS) * gain_ref[:, own]
    left_ref[0:PAD_ROWS, :] = jnp.concatenate(
        [normed, jnp.zeros((PAD_ROWS - row_count, normed.shape[1]), F32)], 0
    ).astype(BF16)
    split_scales(kv_absmax_ref, split_ref, scale_ref, 0, 1)
    kv_copy.wait()
    for tile in range(1, min(DEPTH - 1, tiles)):
        code_copy(codes_ref, 0, tile, buffer_ref, code_sems).start(priority=1)
    total, _ = weight_tile(
        kv_buffer_ref, scale_ref.at[0], level_ref, left_ref.at[0:PAD_ROWS, :], None, False
    )
    finish_all(smalls[5:])
    split_scales(absmax_ref, split_ref, scale_ref, 1, tiles)
    joined = wide_dot(total, kv_join_ref[...])
    for owner in range(size_x):
        chunk_ref[owner, :, share:] = joined[
            : 2 * row_count, owner * HEAD_DIM : (owner + 1) * HEAD_DIM
        ]
    ups = tenant_fetch(scalar_ref, row_count, up_ref, ups_ref, 0, up_sems)
    finish_all(downs)

    def visit(tile, carry):
        codes = code_tile(codes_ref, 0, tile, tiles, buffer_ref, code_sems)
        total, squares = weight_tile(codes, scale_ref.at[tile + 1], level_ref, left_ref, None)
        total_ref[tile] = total
        square_ref[tile] = squares[0:8]
        return carry

    lax.fori_loop(0, tiles, visit, 0)
    finish_all(ups)
    gram = dot_rows(left_ref[...], left_ref[PAD_ROWS:, :])
    gram = jnp.where(block_mask(*gram.shape, PAD_ROWS), gram, 0.0)
    up_split = dot(stack_tiles(ups_ref[...]), split_ref[...])
    lines = []
    for tile in range(tiles):
        up_tile = up_split[low_rank * tile : low_rank * (tile + 1)]
        extra = wide_dot(gram, up_tile.astype(BF16))
        total = total_ref[tile]
        lines.append(total[:row_count] + extra[:row_count])
        lines.append(
            norm_terms(
                total[PAD_ROWS:], extra[PAD_ROWS:], up_tile, square_ref[tile, 0:1], row_count
            )
        )
    joined = wide_dot(jnp.concatenate(lines, 0), join_ref[...])
    piece = min(COLS, share)
    for tile in range(tiles):
        for part in range(COLS // piece):
            owner, place = divmod(tile * COLS + part * piece, share)
            chunk_ref[owner, :, place : place + piece] = joined[
                2 * row_count * tile : 2 * row_count * (tile + 1),
                part * piece : (part + 1) * piece,
            ]
    for shift in range(size_x):
        outs[shift][...] = chunk_ref[lax.rem(here + shift, size_x)]


def store_copy(store_ref, slot, weight_ref, tile, sems):
    return pltpu.make_async_copy(store_ref.at[slot], weight_ref.at[tile], sems.at[slot])


def output_scale_kernel(
    row_count,
    first,
    tenant_hbm,
    absmax_hbm,
    level_hbm,
    split_hbm,
    join_hbm,
    codes_ref,
    down_ref,
    up_ref,
    norm_ref,
    up_split_ref,
    weight_ref,
    absmax_ref,
    level_ref,
    split_ref,
    join_ref,
    store_ref,
    left_ref,
    scale_ref,
    total_ref,
    square_ref,
    buffer_ref,
    ups_ref,
    code_sems,
    down_sems,
    up_sems,
    store_sems,
    small_sems,
    scalar_ref,
    scalar_sem,
):
    scalars = read_scalars(tenant_hbm, scalar_ref, scalar_sem.at[0])
    tiles = weight_ref.shape[0]
    low_rank = row_count * RANK
    columns = slice(first * COLS, (first + tiles) * COLS)
    code_copy(codes_ref, first, 0, buffer_ref, code_sems).start(priority=1)
    smalls = fetch(
        [split_hbm, absmax_hbm.at[:, columns], level_hbm, join_hbm],
        [split_ref, absmax_ref, level_ref, join_ref],
        small_sems,
    )
    scalars.wait()
    downs = tenant_fetch(scalar_ref, row_count, down_ref, left_ref, 0, down_sems)
    for tile in range(1, min(DEPTH - 1, tiles)):
        code_copy(codes_ref, first, tile, buffer_ref, code_sems).start(priority=1)
    ups = tenant_fetch(
        scalar_ref, row_count, up_ref.at[:, :, columns], ups_ref, 0, up_sems
    )
    finish_all(smalls)
    split_scales(absmax_ref, split_ref, scale_ref, 0, tiles)
    finish_all(downs)

    def visit(tile, carry):
        codes = code_tile(codes_ref, first, tile, tiles, buffer_ref, code_sems)
        slot = lax.rem(tile, 2)

        @pl.when(tile >= 2)
        def _():
            store_copy(store_ref, slot, weight_ref, tile - 2, store_sems).wait()

        total, squares = weight_tile(
            codes, scale_ref.at[tile], level_ref, left_ref, store_ref.at[slot]
        )
        store_copy(store_ref, slot, weight_ref, tile, store_sems).start()
        total_ref[tile] = total
        square_ref[tile] = squares[0:8]
        return carry

    lax.fori_loop(0, tiles, visit, 0)
    finish_all(ups)
    gram = dot_rows(left_ref[...], left_ref[...])
    gram = jnp.where(block_mask(*gram.shape, 0), gram, 0.0)
    up_split = dot(stack_tiles(ups_ref[...]), split_ref[...])
    lines = []
    for tile in range(tiles):
        up_tile = up_split[low_rank * tile : low_rank * (tile + 1)]
        narrow = up_tile.astype(BF16)
        up_split_ref[:, COLS * tile : COLS * (tile + 1)] = narrow
        extra = wide_dot(gram, narrow)
        lines.append(norm_terms(total_ref[tile], extra, up_tile, square_ref[tile, 0:1], row_count))
    joined = wide_dot(jnp.concatenate(lines, 0), join_ref[...])
    for tile in range(tiles):
        norm_ref[:, COLS * tile : COLS * (tile + 1)] = joined[
            row_count * tile : row_count * (tile + 1)
        ]
    for tile in range(max(tiles - 2, 0), tiles):
        store_copy(store_ref, tile % 2, weight_ref, tile, store_sems).wait()


def rotate_kernel(row_count, size_x, step, scalar_ref, magnitude_ref, cos_ref, sin_ref, *refs):
    parts = refs[:size_x]
    out_ref = refs[size_x]
    share = cos_ref.shape[1] - HEAD_DIM
    total = parts[0][...]
    for part in parts[1:]:
        total = total + part[...]
    magnitude = jnp.concatenate(
        [
            magnitude_ref[pl.ds(scalar_ref[row], 1), :]
            for row in range(row_count)
        ],
        0,
    )
    query = total[:row_count, :share] * (
        magnitude * lax.rsqrt(total[row_count:, :share])
    )
    keyval = total[:row_count, share:]
    half = HEAD_DIM // 2
    pieces = []
    for head in range(share // HEAD_DIM):
        block = query[:, head * HEAD_DIM : (head + 1) * HEAD_DIM]
        pieces.append(pltpu.roll(block, half, 1))
    lane = lax.broadcasted_iota(jnp.int32, keyval.shape, 1)
    other = jnp.where(
        (lane & step) != 0, pltpu.roll(keyval, step, 1), pltpu.roll(keyval, HEAD_DIM - step, 1)
    )
    values = jnp.concatenate([query, keyval], 1)
    partner = jnp.concatenate(pieces + [other], 1)
    turned = (values * cos_ref[...] + partner * sin_ref[...]).astype(BF16)
    for target in range(out_ref.shape[0]):
        out_ref[target] = turned


def attend_kernel(
    row_count,
    size_x,
    size_y,
    owner_hbm,
    filled_hbm,
    gathered_hbm,
    kv_order_hbm,
    pages_ref,
    send_ref,
    query_ref,
    mixed_ref,
    best_ref,
    total_ref,
    value_ref,
    held_ref,
    gathered_ref,
    kv_order_ref,
    owner_ref,
    filled_ref,
    page_sems,
    small_sems,
):
    slots = pages_ref.shape[0]

    def page_copy(slot):
        return pltpu.make_async_copy(pages_ref.at[slot], held_ref.at[slot], page_sems.at[slot])

    smalls = fetch(
        [owner_hbm, filled_hbm, gathered_hbm, kv_order_hbm],
        [owner_ref, filled_ref, gathered_ref, kv_order_ref],
        small_sems,
    )
    ahead = min(DEPTH, slots)
    for slot in range(ahead):
        page_copy(slot).start(priority=1)
    finish_all(smalls)
    devices = size_x * size_y
    per_target = HEADS // devices
    group = HEADS // KV_HEADS
    inv_root = 1.0 / math.sqrt(HEAD_DIM)
    used = sum((filled_ref[slot] > 0).astype(jnp.int32) for slot in range(slots))
    device = lax.axis_index("gx") * size_y + lax.axis_index("gy")
    share = gathered_ref.shape[2] - HEAD_DIM

    def setup():
        heads_here = share // HEAD_DIM
        for place_x in range(size_x):
            for place_y in range(size_y):
                block = gathered_ref[place_x * size_y + place_y].astype(F32)
                for head in range(heads_here):
                    first = (place_y * size_x + place_x) * heads_here + head
                    query_ref[pl.ds(first, row_count, stride=HEADS), :] = block[
                        :, head * HEAD_DIM : (head + 1) * HEAD_DIM
                    ]
                mixed_ref[place_x, place_y * row_count : (place_y + 1) * row_count, :] = block[
                    :, share:
                ]
        best_ref[...] = jnp.full(best_ref.shape, NEG_FILL, F32)
        total_ref[...] = jnp.zeros(total_ref.shape, F32)
        value_ref[...] = jnp.zeros(value_ref.shape, F32)

        @pl.when(device < row_count)
        def _():
            columns = kv_order_ref.shape[0]
            plain = jnp.zeros((size_y * row_count, columns), F32)
            for place_x in range(size_x):
                plain = plain + dot_rows(
                    mixed_ref[place_x].astype(BF16),
                    kv_order_ref[:, place_x * HEAD_DIM : (place_x + 1) * HEAD_DIM],
                )
            heads_each = 2 * KV_HEADS // size_y
            for row in range(row_count):

                @pl.when(device == row)
                def _():
                    rows = []
                    for head in range(2 * KV_HEADS):
                        place_y, inner = divmod(head, heads_each)
                        line = place_y * row_count + row
                        one = plain[line : line + 1, inner * HEAD_DIM : (inner + 1) * HEAD_DIM]
                        rows.append(jnp.broadcast_to(one, (group, HEAD_DIM)))
                    new_keys = jnp.concatenate(rows[:KV_HEADS], 0)
                    new_values = jnp.concatenate(rows[KV_HEADS:], 0)
                    span = slice(row * HEADS, (row + 1) * HEADS)
                    score = jnp.sum(query_ref[span, :] * new_keys, 1, keepdims=True) * inv_root
                    best_ref[span, :] = jnp.broadcast_to(score, (HEADS, HEAD_DIM))
                    total_ref[span, :] = jnp.ones((HEADS, HEAD_DIM), F32)
                    value_ref[span, :] = new_values

    setup()

    def visit(slot, carry):
        @pl.when(slot + ahead < used)
        def _():
            page_copy(slot + ahead).start(priority=1)

        page_copy(slot).wait()
        start = pl.multiple_of(owner_ref[slot] * HEADS, HEADS)
        count = filled_ref[slot]
        span = pl.ds(start, HEADS)
        query = query_ref[span, :].astype(BF16)
        scores = jnp.concatenate(
            [
                dot_rows(
                    query[group * head : group * (head + 1), :],
                    held_ref[slot, 0, :, head * HEAD_DIM : (head + 1) * HEAD_DIM],
                )
                for head in range(KV_HEADS)
            ],
            0,
        )
        inside = lax.broadcasted_iota(jnp.int32, (HEADS, PAGE), 1) < count
        scores = jnp.where(inside, scores * inv_root, NEG_FILL)
        old_best = best_ref[span, :]
        best = jnp.maximum(old_best, jnp.max(scores, axis=1, keepdims=True))
        weights = jnp.where(inside, jnp.exp(scores - best[:, :1]), 0.0)
        keep = jnp.exp(old_best - best)
        best_ref[span, :] = best
        total_ref[span, :] = total_ref[span, :] * keep + jnp.sum(weights, axis=1, keepdims=True)
        coarse = weights.astype(BF16)
        fine = (weights - coarse.astype(F32)).astype(BF16)
        gains = []
        for head in range(KV_HEADS):
            rows = slice(group * head, group * (head + 1))
            both = dot(
                jnp.concatenate([coarse[rows], fine[rows]], 0),
                held_ref[slot, 1, :, head * HEAD_DIM : (head + 1) * HEAD_DIM],
            )
            gains.append(both[:group] + both[group:])
        value_ref[span, :] = value_ref[span, :] * keep + jnp.concatenate(gains, 0)
        return carry

    lax.fori_loop(0, used, visit, 0)
    for slot in range(ahead):

        @pl.when(slot >= used)
        def _(slot=slot):
            page_copy(slot).wait()


    def close():
        eye = lax.broadcasted_iota(jnp.int32, (HEADS, HEAD_DIM), 0) == lax.broadcasted_iota(
            jnp.int32, (HEADS, HEAD_DIM), 1
        )
        lines = []
        for source in (best_ref, total_ref):
            for row in range(row_count):
                block = source[row * HEADS : (row + 1) * HEADS, :]
                lines.append(jnp.sum(jnp.where(eye, block, 0.0), axis=0, keepdims=True))
        scalars = jnp.concatenate(lines, 0)
        for target in range(devices):
            for row in range(row_count):
                begin = row * HEADS + target * per_target
                send_ref[target, row * per_target : (row + 1) * per_target, :] = value_ref[
                    begin : begin + per_target, :
                ]
            send_ref[target, row_count * per_target :, :] = scalars

    close()


def merge_kernel(row_count, per_target, info_ref, parts_ref, out_ref):
    offset = info_ref[0] * per_target
    values = parts_ref[:, : row_count * per_target, :]
    scalars = parts_ref[:, row_count * per_target :, :]
    lane = lax.broadcasted_iota(jnp.int32, scalars.shape, 2)
    for row in range(row_count):
        for head in range(per_target):
            chosen = jnp.sum(jnp.where(lane == offset + head, scalars, 0.0), axis=2, keepdims=True)
            best = chosen[:, row : row + 1, :]
            total = chosen[:, row_count + row : row_count + row + 1, :]
            factor = jnp.exp(best - jnp.max(best, axis=0, keepdims=True))
            line = row * per_target + head
            top = jnp.sum(values[:, line : line + 1, :] * factor, axis=0)
            bottom = jnp.sum(total * factor, axis=0)
            ratio = (top / bottom).astype(BF16)
            for target in range(out_ref.shape[0]):
                out_ref[target, row : row + 1, head * HEAD_DIM : (head + 1) * HEAD_DIM] = ratio


def output_kernel(
    row_count,
    size_x,
    tile_counts,
    tenant_hbm,
    attended_hbm,
    join_hbm,
    down_ref,
    *refs,
):
    parts = len(tile_counts)
    norms_hbm = refs[:parts]
    ups_hbm = refs[parts : 2 * parts]
    weights = refs[2 * parts : 3 * parts]
    outs = refs[3 * parts : 3 * parts + size_x]
    refs = refs[3 * parts + size_x :]
    norms = refs[:parts]
    splits = refs[parts : 2 * parts]
    (
        attended_ref,
        join_ref,
        left_ref,
        low_ref,
        total_ref,
        chunk_ref,
        held_ref,
        down_sems,
        held_sems,
        small_sems,
        scalar_ref,
        scalar_sem,
    ) = refs[2 * parts :]
    tiles = sum(tile_counts)
    own = row_count // size_x
    scalars = read_scalars(tenant_hbm, scalar_ref, scalar_sem.at[0])
    smalls = fetch(
        [attended_hbm, join_hbm] + list(norms_hbm) + list(ups_hbm),
        [attended_ref, join_ref] + list(norms) + list(splits),
        small_sems,
    )
    loads = [
        pltpu.make_async_copy(
            weights[part].at[tile],
            held_ref.at[sum(tile_counts[:part]) + tile],
            held_sems.at[sum(tile_counts[:part]) + tile],
        )
        for part in range(parts)
        for tile in range(tile_counts[part])
    ]
    scalars.wait()
    downs = tenant_fetch(scalar_ref, row_count, down_ref, low_ref, 0, down_sems)
    for load in loads:
        load.start(priority=1)
    smalls[0].wait()
    width = attended_ref.shape[2]
    for part in range(attended_ref.shape[0]):
        block = attended_ref[part].astype(F32)
        left_ref[:, part * width : (part + 1) * width] = jnp.concatenate(
            [block, jnp.zeros((PAD_ROWS - row_count, width), F32)], 0
        ).astype(BF16)
    finish_all(downs)
    finish_all(smalls[1:])
    middle = dot_rows(left_ref[...], low_ref[...])
    middle = jnp.where(block_mask(*middle.shape, PAD_ROWS), middle, 0.0)
    extras = [wide_dot(middle, up[...]) for up in splits]
    numbers = []
    for part in range(parts):
        for tile in range(tile_counts[part]):
            spot = len(numbers)
            loads[spot].wait()
            total_ref[spot] = dot(left_ref[...], held_ref[spot]) + extras[part][
                :, COLS * tile : COLS * (tile + 1)
            ]
            numbers.append(total_ref[spot, 0:row_count])
    joined = wide_dot(jnp.concatenate(numbers, 0), join_ref[...])
    for owner in range(size_x):
        for spot in range(tiles):
            begin = row_count * spot + owner * own
            chunk_ref[owner, 0:own, COLS * spot : COLS * (spot + 1)] = joined[begin : begin + own]
        for part in range(parts):
            begin = COLS * sum(tile_counts[:part])
            chunk_ref[owner, own : 2 * own, begin : begin + COLS * tile_counts[part]] = norms[
                part
            ][owner * own : (owner + 1) * own, :]
    here = lax.axis_index("gx")
    for shift in range(size_x):
        outs[shift][...] = chunk_ref[lax.rem(here + shift, size_x)]


def finish_kernel(row_count, size_x, scalar_ref, hidden_ref, magnitude_ref, *refs):
    parts = refs[:size_x]
    out_ref = refs[size_x]
    own = row_count // size_x
    total = parts[0][...]
    for part in parts[1:]:
        total = total + part[...]
    here = lax.axis_index("gx")
    states = hidden_ref[...].astype(F32)
    row_id = lax.broadcasted_iota(jnp.int32, states.shape, 0)
    for line in range(own):
        row = here * own + line
        state = jnp.sum(jnp.where(row_id == row, states, 0.0), axis=0, keepdims=True)
        magnitude = magnitude_ref[pl.ds(scalar_ref[row], 1), :]
        scale = magnitude * lax.rsqrt(total[own + line : own + line + 1])
        out_ref[line : line + 1, :] = (state + total[line : line + 1] * scale).astype(BF16)


def slot_info(page_table, lengths, device, slot_count):
    row_count, page_limit = page_table.shape
    page_need = (lengths + PAGE - 1) // PAGE
    page_numbers = jnp.arange(page_limit, dtype=jnp.int32)
    live_mask = page_numbers[None, :] < page_need[:, None]
    wanted = device * slot_count + jnp.arange(slot_count, dtype=jnp.int32)
    hits = ((page_table[None, :, :] == wanted[:, None, None]) & live_mask[None, :, :]).astype(
        jnp.int32
    )
    owner_row = jnp.sum(hits * jnp.arange(row_count, dtype=jnp.int32)[None, :, None], axis=(1, 2))
    remaining = jnp.clip(lengths[:, None] - page_numbers[None, :] * PAGE, 0, PAGE)
    filled = jnp.sum(hits * remaining[None, :, :], axis=(1, 2))
    return owner_row, filled


def exchange(parts, axis, size):
    received = [parts[0]]
    for shift in range(1, size):
        received.append(
            lax.ppermute(parts[shift], axis, [(spot, (spot + shift) % size) for spot in range(size)])
        )
    return received


def whole(shape):
    return pl.BlockSpec(shape, lambda *_: (0,) * len(shape))


def local(
    hidden,
    norm_gain,
    q_codes,
    q_absmax,
    kv_codes,
    kv_absmax,
    o_codes,
    o_absmax,
    q_down,
    q_up,
    q_magnitude,
    o_down,
    o_up,
    o_magnitude,
    tenant,
    lengths,
    page_table,
    kv_cache,
):
    row_count, width = hidden.shape
    row_x = lax.axis_index("gx").astype(jnp.int32)
    col_y = lax.axis_index("gy").astype(jnp.int32)
    size_x = lax.axis_size("gx")
    size_y = lax.axis_size("gy")
    devices = size_x * size_y
    device = row_x * size_y + col_y
    in_rows, q_words = q_codes.shape
    q_cols = 2 * q_words
    share = q_cols // size_x
    kv_cols = 2 * kv_codes.shape[1]
    if kv_cols < COLS:
        kv_codes = jnp.pad(kv_codes, ((0, 0), (0, WORDS - kv_codes.shape[1])))
        kv_absmax = jnp.pad(kv_absmax, ((0, 0), (0, COLS - kv_cols)))
    low_rank = row_count * RANK
    level = jnp.asarray(level_table())
    split_matrix = split_columns()
    split = jnp.asarray(split_matrix, BF16)
    join = jnp.asarray(split_matrix.T, BF16)
    order = keyval_order(kv_cols, size_x)
    kv_join = jnp.asarray(split_matrix.T @ order, BF16)
    kv_order = jnp.asarray(order, BF16)
    scalars = tenant
    q_down = jnp.swapaxes(q_down, 1, 2)
    o_down = jnp.swapaxes(o_down, 1, 2)
    q_tiles = q_words // WORDS
    scale_rows = in_rows // QBLOCK

    smem = pl.BlockSpec(memory_space=pltpu.SMEM)
    vmem = pl.BlockSpec(memory_space=pltpu.VMEM)
    anywhere = pl.BlockSpec(memory_space=pltpu.HBM)
    chunk_shape = (2 * row_count, share + HEAD_DIM)
    scalar_scratch = [pltpu.SMEM((row_count,), jnp.int32), pltpu.SemaphoreType.DMA((1,))]
    small = [
        pltpu.VMEM((scale_rows, q_cols), F32),
        pltpu.VMEM((scale_rows, COLS), F32),
        pltpu.VMEM(level.shape, F32),
        pltpu.VMEM(split.shape, BF16),
        pltpu.VMEM(join.shape, BF16),
    ]
    q_parts = pl.pallas_call(
        functools.partial(query_kernel, row_count, size_x),
        in_specs=[anywhere] * 13,
        out_specs=[vmem] * size_x,
        scratch_shapes=[
            pltpu.VMEM((row_count, width), BF16),
            pltpu.VMEM((1, width), F32),
            *small,
            pltpu.VMEM(kv_join.shape, BF16),
            pltpu.VMEM((PAD_ROWS + low_rank, in_rows), BF16),
            pltpu.VMEM((q_tiles + 1, scale_rows, COLS), F32),
            pltpu.VMEM((q_tiles, PAD_ROWS + low_rank, COLS), F32),
            pltpu.VMEM((q_tiles, 8, COLS), F32),
            pltpu.VMEM((size_x,) + chunk_shape, F32),
            pltpu.VMEM((DEPTH, in_rows, WORDS), jnp.int32),
            pltpu.VMEM((in_rows, WORDS), jnp.int32),
            pltpu.VMEM((low_rank, q_cols), BF16),
            pltpu.SemaphoreType.DMA((DEPTH,)),
            pltpu.SemaphoreType.DMA((1,)),
            pltpu.SemaphoreType.DMA((row_count,)),
            pltpu.SemaphoreType.DMA((row_count,)),
            pltpu.SemaphoreType.DMA((8,)),
            *scalar_scratch,
        ],
        out_shape=[jax.ShapeDtypeStruct(chunk_shape, F32)] * size_x,
        name="query",
    )(
        tenant,
        hidden,
        norm_gain[None, :],
        q_absmax,
        kv_absmax,
        level,
        split,
        join,
        kv_join,
        q_codes,
        kv_codes,
        q_down,
        q_up,
    )
    q_parts = exchange(q_parts, "gx", size_x)

    def output_scales(first, tiles, after):
        owners, _ = lax.optimization_barrier((tenant, after))
        return pl.pallas_call(
            functools.partial(output_scale_kernel, row_count, first),
            in_specs=[anywhere] * 8,
            out_specs=[vmem, vmem, anywhere],
            scratch_shapes=[
                pltpu.VMEM((scale_rows, tiles * COLS), F32),
                *small[2:],
                pltpu.VMEM((2, in_rows, COLS), BF16),
                pltpu.VMEM((low_rank, in_rows), BF16),
                pltpu.VMEM((tiles, scale_rows, COLS), F32),
                pltpu.VMEM((tiles, low_rank, COLS), F32),
                pltpu.VMEM((tiles, 8, COLS), F32),
                pltpu.VMEM((DEPTH, in_rows, WORDS), jnp.int32),
                pltpu.VMEM((low_rank, tiles * COLS), BF16),
                pltpu.SemaphoreType.DMA((DEPTH,)),
                pltpu.SemaphoreType.DMA((row_count,)),
                pltpu.SemaphoreType.DMA((row_count,)),
                pltpu.SemaphoreType.DMA((2,)),
                pltpu.SemaphoreType.DMA((4,)),
                *scalar_scratch,
            ],
            out_shape=[
                jax.ShapeDtypeStruct((row_count, tiles * COLS), F32),
                jax.ShapeDtypeStruct((low_rank, tiles * COLS), BF16),
                pltpu.HBM((tiles, in_rows, COLS), BF16),
            ],
            compiler_params=pltpu.CompilerParams(vmem_limit_bytes=56 * 2**20),
            cost_estimate=pl.CostEstimate(
                flops=tiles * 5_000_000 * 256,
                bytes_accessed=tiles * 8 * in_rows * WORDS,
                transcendentals=0,
            ),
            name="output_scale",
        )(owners, o_absmax, level, split, join, o_codes, o_down, o_up)

    tile_counts = [3 * q_tiles // 8, q_tiles - 3 * q_tiles // 8]

    half = HEAD_DIM // 2
    step = half // size_x
    lane = jnp.arange(share + HEAD_DIM, dtype=jnp.int32)
    in_query = lane < share
    turn = jnp.where(in_query, lane % half, row_x * step + lane % step)
    second = jnp.where(in_query, lane % HEAD_DIM // half, lane % (2 * step) // step)
    frequency = ROPE_BASE ** (-2.0 * turn.astype(F32) / HEAD_DIM)
    angles = lengths.astype(F32)[:, None] * frequency[None, :]
    plain = jnp.logical_and(~in_query, col_y * kv_cols >= KV_HEADS * HEAD_DIM)[None, :]
    cosine = jnp.where(plain, 1.0, jnp.cos(angles))
    sine = jnp.sin(angles)
    sine = jnp.where(plain, 0.0, jnp.where(second[None, :] == 1, sine, -sine))

    query_all = pl.pallas_call(
        functools.partial(rotate_kernel, row_count, size_x, step),
        grid_spec=pltpu.PrefetchScalarGridSpec(
            num_scalar_prefetch=1,
            grid=(1,),
            in_specs=[
                pl.BlockSpec((TENANTS, share), lambda tile, ref: (0, lax.axis_index("gx"))),
                whole(cosine.shape),
                whole(sine.shape),
            ]
            + [whole(chunk_shape)] * size_x,
            out_specs=whole((devices, row_count, share + HEAD_DIM)),
        ),
        out_shape=jax.ShapeDtypeStruct((devices, row_count, share + HEAD_DIM), BF16),
        compiler_params=pltpu.CompilerParams(vmem_limit_bytes=8 * 2**20),
        name="rotate",
    )(scalars, q_magnitude, cosine, sine, *q_parts)
    gathered = lax.all_to_all(query_all, ("gx", "gy"), split_axis=0, concat_axis=0, tiled=True)
    scale_parts = [output_scales(0, tile_counts[0], query_all)]
    gathered, scale_parts[0] = lax.optimization_barrier((gathered, scale_parts[0]))

    slots = kv_cache.shape[0]
    owner_row, filled = slot_info(page_table, lengths, device, slots)
    per_target = HEADS // devices
    send_shape = (devices, row_count * per_target + 2 * row_count, HEAD_DIM)
    sent = pl.pallas_call(
        functools.partial(attend_kernel, row_count, size_x, size_y),
        in_specs=[anywhere] * 5,
        out_specs=vmem,
        scratch_shapes=[
            pltpu.VMEM((row_count * HEADS, HEAD_DIM), F32),
            pltpu.VMEM((size_x, size_y * row_count, HEAD_DIM), F32),
            pltpu.VMEM((row_count * HEADS, HEAD_DIM), F32),
            pltpu.VMEM((row_count * HEADS, HEAD_DIM), F32),
            pltpu.VMEM((row_count * HEADS, HEAD_DIM), F32),
            pltpu.VMEM(kv_cache.shape, BF16),
            pltpu.VMEM(gathered.shape, BF16),
            pltpu.VMEM((kv_cols, kv_order.shape[1]), BF16),
            pltpu.SMEM((slots,), jnp.int32),
            pltpu.SMEM((slots,), jnp.int32),
            pltpu.SemaphoreType.DMA((slots,)),
            pltpu.SemaphoreType.DMA((4,)),
        ],
        out_shape=jax.ShapeDtypeStruct(send_shape, F32),
        compiler_params=pltpu.CompilerParams(vmem_limit_bytes=58 * 2**20),
        name="attend",
    )(owner_row, filled, gathered, kv_order[:kv_cols], kv_cache)
    parts = lax.all_to_all(sent, ("gx", "gy"), split_axis=0, concat_axis=0, tiled=True)
    scale_parts.append(output_scales(tile_counts[0], tile_counts[1], sent))
    parts, scale_parts[1] = lax.optimization_barrier((parts, scale_parts[1]))

    merged = pl.pallas_call(
        functools.partial(merge_kernel, row_count, per_target),
        in_specs=[
            pl.BlockSpec(memory_space=pltpu.SMEM),
            pl.BlockSpec(memory_space=pltpu.VMEM),
        ],
        out_specs=pl.BlockSpec(memory_space=pltpu.VMEM),
        out_shape=jax.ShapeDtypeStruct((size_y, row_count, per_target * HEAD_DIM), BF16),
        compiler_params=pltpu.CompilerParams(vmem_limit_bytes=8 * 2**20),
        name="merge",
    )(device[None], parts)
    attended = lax.all_to_all(merged, "gy", split_axis=0, concat_axis=0, tiled=True)

    own = row_count // size_x
    o_parts = pl.pallas_call(
        functools.partial(output_kernel, row_count, size_x, tile_counts),
        in_specs=[anywhere] * (4 + 3 * len(scale_parts)),
        out_specs=[vmem] * size_x,
        scratch_shapes=[
            *[pltpu.VMEM((row_count, count * COLS), F32) for count in tile_counts],
            *[pltpu.VMEM((low_rank, count * COLS), BF16) for count in tile_counts],
            pltpu.VMEM(attended.shape, BF16),
            pltpu.VMEM(join.shape, BF16),
            pltpu.VMEM((PAD_ROWS, in_rows), BF16),
            pltpu.VMEM((low_rank, in_rows), BF16),
            pltpu.VMEM((q_tiles, PAD_ROWS, COLS), F32),
            pltpu.VMEM((size_x, 2 * own, q_cols), F32),
            pltpu.VMEM((q_tiles, in_rows, COLS), BF16),
            pltpu.SemaphoreType.DMA((row_count,)),
            pltpu.SemaphoreType.DMA((q_tiles,)),
            pltpu.SemaphoreType.DMA((2 + 2 * len(scale_parts),)),
            *scalar_scratch,
        ],
        out_shape=[jax.ShapeDtypeStruct((2 * own, q_cols), F32)] * size_x,
        compiler_params=pltpu.CompilerParams(vmem_limit_bytes=56 * 2**20),
        name="output",
    )(
        tenant,
        attended,
        join,
        o_down,
        *[part[0] for part in scale_parts],
        *[part[1] for part in scale_parts],
        *[part[2] for part in scale_parts],
    )
    o_parts = exchange(o_parts, "gx", size_x)
    return pl.pallas_call(
        functools.partial(finish_kernel, row_count, size_x),
        grid_spec=pltpu.PrefetchScalarGridSpec(
            num_scalar_prefetch=1,
            grid=(1,),
            in_specs=[
                pl.BlockSpec((row_count, q_cols), lambda tile, ref: (0, lax.axis_index("gy"))),
                whole(o_magnitude.shape),
            ]
            + [whole((2 * own, q_cols))] * size_x,
            out_specs=whole((own, q_cols)),
        ),
        out_shape=jax.ShapeDtypeStruct((own, q_cols), BF16),
        compiler_params=pltpu.CompilerParams(vmem_limit_bytes=4 * 2**20),
        name="finish",
    )(scalars, hidden, o_magnitude, *o_parts)


def solution(mesh):
    in_specs = (
        P(),
        P(),
        P("gx", "gy"),
        P("gx", "gy"),
        P("gx", "gy"),
        P("gx", "gy"),
        P("gx", "gy"),
        P("gx", "gy"),
        P(None, "gx", None),
        P(None, None, "gy"),
        P(None, "gy"),
        P(None, "gx", None),
        P(None, None, "gy"),
        P(None, "gy"),
        P(),
        P(),
        P(),
        P(("gx", "gy"), None, None, None),
    )
    out_specs = P("gx", "gy")
    return jax.shard_map(local, mesh=mesh, in_specs=in_specs, out_specs=out_specs, check_vma=False)
```
